8 devices in a mesh: dp: 2 (over z, y), sp: 4 (over x, core).
Axes of the slice: x: 2, y: 2, z: 1, core: 2. Of those that a mesh axis runs over, the one named last changes fastest.
Arguments:
- x_special: bfloat16 [8, 5, 768], P('dp'), parts along dimension 0
- x_patch: bfloat16 [8, 1024, 768], P('dp', 'sp'), parts along dimension 0
- dy_special: bfloat16 [8, 5, 768], P('dp'), parts along dimension 0
- dy_patch: bfloat16 [8, 1024, 768], P('dp', 'sp'), parts along dimension 0
- ln_scale: float32 [768], replicated
- ln_bias: float32 [768], replicated
- w_qkv: bfloat16 [768, 2304], replicated
- b_qkv: float32 [2304], replicated
- w_proj: bfloat16 [768, 768], replicated
- b_proj: float32 [768], replicated
- layer_scale: float32 [768], replicated
Outputs:
- output 1: bfloat16 [8, 5, 768], P('dp'), parts along dimension 0
- output 2: bfloat16 [8, 1024, 768], P('dp', 'sp'), parts along dimension 0
- output 3: bfloat16 [8, 5, 768], P('dp'), parts along dimension 0
- output 4: bfloat16 [8, 1024, 768], P('dp', 'sp'), parts along dimension 0
- output 5: float32 [1536], P('dp'), parts along dimension 0
- output 6: float32 [1536], P('dp'), parts along dimension 0
- output 7: float32 [1536, 2304], P('dp'), parts along dimension 0
- output 8: float32 [4608], P('dp'), parts along dimension 0
- output 9: float32 [1536, 768], P('dp'), parts along dimension 0
- output 10: float32 [1536], P('dp'), parts along dimension 0
- output 11: float32 [1536], P('dp'), parts along dimension 0
There are 2 independent parts. The reference program is written for one: setup_inputs(seed, part) draws one part's arguments, and reference() takes and returns one part's arrays. A program takes and returns all parts, laid end to end along the dimension named above; an argument that names none is the same for every part.
All inputs are finite; a program needn't handle non-finite values.
Results may differ from the reference program's by a relative error of at most 0.0100889.
Values are sent between devices in bfloat16 or wider.
A program may use at most 1 GiB of HBM per device.

```python
import jax
import jax.numpy as jnp
from jax import lax

IMAGES = 4
PATCHES = 1024
SPECIAL = 5
D_MODEL = 768
NUM_HEADS = 12
HEAD_DIM = 64
TEXTURES = 8
TOKENS = SPECIAL + PATCHES
LN_EPS = 1e-6
ATTN_SCALE = HEAD_DIM ** -0.5


def setup_inputs(seed: int = 0, part: int = 0) -> dict:
    part_keys = jax.random.split(jax.random.fold_in(jax.random.key(seed), part), 7)
    weight_keys = jax.random.split(jax.random.key(seed + 1), 9)
    common = jax.random.normal(part_keys[0], (IMAGES, 1, D_MODEL), jnp.float32)
    texture = jax.random.normal(part_keys[1], (IMAGES, TEXTURES, D_MODEL), jnp.float32)
    tex_id = jax.random.randint(part_keys[2], (IMAGES, PATCHES), 0, TEXTURES)
    onehot = (tex_id[:, :, None] == jnp.arange(TEXTURES)[None, None, :]).astype(jnp.float32)
    patch_vals = jnp.einsum('bnt,btd->bnd', onehot, texture) + 0.7 * common + 0.5 * jax.random.normal(part_keys[3], (IMAGES, PATCHES, D_MODEL), jnp.float32)
    special_vals = 3.0 * common + 0.5 * jax.random.normal(part_keys[4], (IMAGES, SPECIAL, D_MODEL), jnp.float32)
    dy_special = jax.random.normal(part_keys[5], (IMAGES, SPECIAL, D_MODEL), jnp.float32)
    dy_patch = jax.random.normal(part_keys[6], (IMAGES, PATCHES, D_MODEL), jnp.float32)
    fan_scale = D_MODEL ** -0.5
    w_query = jax.random.normal(weight_keys[0], (D_MODEL, D_MODEL), jnp.float32)
    w_key = 0.6 * w_query + 0.8 * jax.random.normal(weight_keys[1], (D_MODEL, D_MODEL), jnp.float32)
    w_value = jax.random.normal(weight_keys[2], (D_MODEL, D_MODEL), jnp.float32)
    w_qkv = jnp.concatenate([w_query, w_key, w_value], axis=1) * fan_scale
    w_proj = jax.random.normal(weight_keys[3], (D_MODEL, D_MODEL), jnp.float32) * fan_scale
    return {
        'x_special': special_vals.astype(jnp.bfloat16),
        'x_patch': patch_vals.astype(jnp.bfloat16),
        'dy_special': dy_special.astype(jnp.bfloat16),
        'dy_patch': dy_patch.astype(jnp.bfloat16),
        'ln_scale': 1.0 + 0.2 * jax.random.normal(weight_keys[4], (D_MODEL,), jnp.float32),
        'ln_bias': 0.3 * jax.random.normal(weight_keys[5], (D_MODEL,), jnp.float32),
        'w_qkv': w_qkv.astype(jnp.bfloat16),
        'b_qkv': 0.3 * jax.random.normal(weight_keys[6], (3 * D_MODEL,), jnp.float32),
        'w_proj': w_proj.astype(jnp.bfloat16),
        'b_proj': 0.3 * jax.random.normal(weight_keys[7], (D_MODEL,), jnp.float32),
        'layer_scale': jax.random.uniform(weight_keys[8], (D_MODEL,), jnp.float32, 0.4, 1.2),
    }


def head_attention(head_qkv):
    queries = head_qkv[0].astype(jnp.float32)
    key_rows = head_qkv[1].astype(jnp.float32)
    value_rows = head_qkv[2].astype(jnp.float32)
    scores = jnp.dot(queries, key_rows.T) * ATTN_SCALE
    attn_prob = jax.nn.softmax(scores, axis=-1)
    return jnp.dot(attn_prob.astype(jnp.bfloat16).astype(jnp.float32), value_rows).astype(jnp.bfloat16)


def block_forward(x_all, ln_scale, ln_bias, w_qkv, b_qkv, w_proj, b_proj, layer_scale):
    x_float = x_all.astype(jnp.float32)
    centered = x_float - jnp.mean(x_float, axis=-1, keepdims=True)
    inv_std = lax.rsqrt(jnp.mean(centered * centered, axis=-1, keepdims=True) + LN_EPS)
    normed = (centered * inv_std * ln_scale + ln_bias).astype(jnp.bfloat16)
    qkv_rows = jnp.einsum('btd,de->bte', normed.astype(jnp.float32), w_qkv.astype(jnp.float32)) + b_qkv
    qkv_rows = qkv_rows.astype(jnp.bfloat16).reshape(IMAGES, TOKENS, 3, NUM_HEADS, HEAD_DIM)
    per_head = jnp.transpose(qkv_rows, (0, 3, 2, 1, 4)).reshape(IMAGES * NUM_HEADS, 3, TOKENS, HEAD_DIM)
    attn_out = lax.map(jax.checkpoint(head_attention), per_head)
    attn_out = jnp.transpose(attn_out.reshape(IMAGES, NUM_HEADS, TOKENS, HEAD_DIM), (0, 2, 1, 3)).reshape(IMAGES, TOKENS, D_MODEL)
    proj_out = jnp.einsum('btd,de->bte', attn_out.astype(jnp.float32), w_proj.astype(jnp.float32)) + b_proj
    return (x_float + layer_scale * proj_out).astype(jnp.bfloat16)


def reference(x_special, x_patch, dy_special, dy_patch, ln_scale, ln_bias, w_qkv, b_qkv, w_proj, b_proj, layer_scale):
    x_all = jnp.concatenate([x_special, x_patch], axis=1)
    dy_all = jnp.concatenate([dy_special, dy_patch], axis=1)
    out_all, block_vjp = jax.vjp(block_forward, x_all, ln_scale, ln_bias, w_qkv, b_qkv, w_proj, b_proj, layer_scale)
    grad_list = block_vjp(dy_all)
    dx_all = grad_list[0]
    return (out_all[:, :SPECIAL], out_all[:, SPECIAL:], dx_all[:, :SPECIAL], dx_all[:, SPECIAL:], grad_list[1], grad_list[2], grad_list[3].astype(jnp.float32), grad_list[4], grad_list[5].astype(jnp.float32), grad_list[6], grad_list[7])
```

```python
import functools

import jax
import jax.numpy as jnp
from jax import lax
from jax.experimental import pallas as pl
from jax.experimental.pallas import tpu as pltpu
from jax.sharding import PartitionSpec as P

HEAD_DIM = 64
PAIR = 2 * HEAD_DIM
LN_EPS = 1e-6
ATTN_SCALE = HEAD_DIM ** -0.5
SPEC_PAD = 16
QBLK = 256
F32 = jnp.float32
BF16 = jnp.bfloat16


def dot_nt(a, b):
    return lax.dot_general(a, b, (((1,), (1,)), ((), ())), preferred_element_type=F32)


def dot_nn(a, b):
    return lax.dot_general(a, b, (((1,), (0,)), ((), ())), preferred_element_type=F32)


def attn_kernel(n_spec, qkv_loc, qkv_rem, da_loc, da_rem, attn_loc, attn_rem, dqkv_loc, dqkv_rem,
                q_s, k_s, v_s, da_s, vt_s, kt_s, s_s, dp_s, p_s, ds_s, dv_s, dk_s, a_s, dq_s):
    loc = qkv_loc.shape[0] - SPEC_PAD
    rem = qkv_rem.shape[0]
    main = loc + rem
    total = main + SPEC_PAD
    chunk = 80

    def fill(dst, src_loc, src_rem, col, scale):
        def put(rows, vals):
            dst[rows, :] = vals if scale is None else vals * jnp.asarray(scale, BF16)
        put(pl.ds(0, loc), src_loc[0:loc, col:col + PAIR])
        put(pl.ds(loc, rem), src_rem[:, col:col + PAIR])
        put(pl.ds(main, SPEC_PAD), src_loc[loc:loc + SPEC_PAD, col:col + PAIR])

    fill(q_s, qkv_loc, qkv_rem, 0, ATTN_SCALE)
    fill(k_s, qkv_loc, qkv_rem, PAIR, None)
    fill(v_s, qkv_loc, qkv_rem, 2 * PAIR, None)
    fill(da_s, da_loc, da_rem, 0, None)
    for dst, src, scale in ((vt_s, v_s, 1.0), (kt_s, k_s, ATTN_SCALE)):
        for row in range(0, main, PAIR):
            dst[:, row:row + PAIR] = (src[row:row + PAIR, :] * jnp.asarray(scale, BF16)).T
        tail = jnp.concatenate([src[main:total, :] * jnp.asarray(scale, BF16),
                                jnp.zeros((PAIR - SPEC_PAD, PAIR), BF16)], axis=0)
        dst[:, main:main + PAIR] = tail.T
    dv_s[...] = jnp.zeros_like(dv_s)
    dk_s[...] = jnp.zeros_like(dk_s)

    def head_mask(rows, head):
        lane = lax.broadcasted_iota(jnp.int32, (rows, PAIR), 1)
        return (lane < HEAD_DIM) if head == 0 else (lane >= HEAD_DIM)

    def scores(idx, q_rows, d_rows, width):
        s_s[idx, :, 0:width] = dot_nt(k_s[...], q_rows)
        dp_s[idx, :, 0:width] = dot_nt(v_s[...], d_rows).astype(BF16)

    def softmax_back(idx, out_col, width):
        row = lax.broadcasted_iota(jnp.int32, (SPEC_PAD, width), 0)
        spec = s_s[idx, main:total, 0:width]
        s_s[idx, main:total, 0:width] = jnp.where(row < n_spec, spec, -jnp.inf)
        top = jnp.max(s_s[idx, :, 0:width], axis=0, keepdims=True)
        norm = jnp.zeros((1, width), F32)
        for r in range(0, total, chunk):
            e = jnp.exp(s_s[idx, r:r + chunk, 0:width] - top)
            norm = norm + jnp.sum(e, axis=0, keepdims=True)
            s_s[idx, r:r + chunk, 0:width] = e
        inv = 1.0 / norm
        mix = jnp.zeros((1, width), F32)
        for r in range(0, total, chunk):
            prob = s_s[idx, r:r + chunk, 0:width] * inv
            p_s[r:r + chunk, out_col:out_col + width] = prob.astype(BF16)
            mix = mix + jnp.sum(prob * dp_s[idx, r:r + chunk, 0:width].astype(F32), axis=0, keepdims=True)
        for r in range(0, total, chunk):
            prob = s_s[idx, r:r + chunk, 0:width] * inv
            ds = prob * (dp_s[idx, r:r + chunk, 0:width].astype(F32) - mix)
            ds_s[r:r + chunk, out_col:out_col + width] = ds.astype(BF16)

    @pl.loop(0, main // QBLK)
    def _(blk):
        rows = pl.ds(pl.multiple_of(blk * QBLK, QBLK), QBLK)
        q_rows = q_s[rows, :]
        d_rows = da_s[rows, :]
        zero = jnp.zeros_like(q_rows)
        q_h = [jnp.where(head_mask(QBLK, h), q_rows, zero) for h in range(2)]
        d_h = [jnp.where(head_mask(QBLK, h), d_rows, zero) for h in range(2)]
        for h in range(2):
            scores(h, q_h[h], d_h[h], QBLK)
        for h in range(2):
            softmax_back(h, h * QBLK, QBLK)
        dv_s[...] += dot_nn(p_s[...], jnp.concatenate(d_h, axis=0))
        dk_s[...] += dot_nn(ds_s[...], jnp.concatenate(q_h, axis=0))
        for dst, lhs, probs in ((a_s, vt_s, p_s), (dq_s, kt_s, ds_s)):
            parts = [dot_nn(lhs[h * HEAD_DIM:(h + 1) * HEAD_DIM, 0:total], probs[:, h * QBLK:(h + 1) * QBLK])
                     for h in range(2)]
            both = jnp.concatenate(parts, axis=0)
            for c in range(0, QBLK, PAIR):
                dst[pl.ds(pl.multiple_of(blk * QBLK + c, PAIR), PAIR), :] = both[:, c:c + PAIR].T.astype(BF16)

    q_rows = q_s[main:total, :]
    d_rows = da_s[main:total, :]
    zero = jnp.zeros_like(q_rows)
    fill_rows = jnp.zeros((PAIR - 2 * SPEC_PAD, PAIR), BF16)
    q_both = jnp.concatenate([jnp.where(head_mask(SPEC_PAD, h), q_rows, zero) for h in range(2)] + [fill_rows], axis=0)
    d_both = jnp.concatenate([jnp.where(head_mask(SPEC_PAD, h), d_rows, zero) for h in range(2)] + [fill_rows], axis=0)
    scores(0, q_both, d_both, PAIR)
    softmax_back(0, 0, PAIR)
    dv_s[...] += dot_nn(p_s[:, 0:PAIR], d_both)
    dk_s[...] += dot_nn(ds_s[:, 0:PAIR], q_both)
    for dst, lhs, probs in ((a_s, vt_s, p_s), (dq_s, kt_s, ds_s)):
        both = dot_nn(lhs[:, 0:total], probs[:, 0:PAIR]).T
        dst[main:total, :] = jnp.where(head_mask(SPEC_PAD, 0), both[0:SPEC_PAD], both[SPEC_PAD:2 * SPEC_PAD]).astype(BF16)

    def emit(dst_loc, dst_rem, col, src):
        dst_loc[0:loc, col:col + PAIR] = src[0:loc, :].astype(BF16)
        dst_loc[loc:loc + SPEC_PAD, col:col + PAIR] = src[main:total, :].astype(BF16)
        dst_rem[:, col:col + PAIR] = src[loc:main, :].astype(BF16)

    emit(attn_loc, attn_rem, 0, a_s)
    emit(dqkv_loc, dqkv_rem, 0, dq_s)
    emit(dqkv_loc, dqkv_rem, PAIR, dk_s)
    emit(dqkv_loc, dqkv_rem, 2 * PAIR, dv_s)


def fused_attention(qkv_loc, qkv_rem, da_loc, da_rem, image, n_spec):
    rows_loc, rows_rem = qkv_loc.shape[1], qkv_rem.shape[0]
    pairs = da_rem.shape[1] // PAIR
    total = rows_loc + rows_rem
    flops = 2 * 6 * total * total * PAIR * pairs * 4
    return pl.pallas_call(
        functools.partial(attn_kernel, n_spec),
        grid=(pairs,),
        in_specs=[
            pl.BlockSpec((None, rows_loc, 3 * PAIR), lambda j: (image, 0, j)),
            pl.BlockSpec((rows_rem, 3 * PAIR), lambda j: (0, j)),
            pl.BlockSpec((None, rows_loc, PAIR), lambda j: (image, 0, j)),
            pl.BlockSpec((rows_rem, PAIR), lambda j: (0, j)),
        ],
        out_specs=[
            pl.BlockSpec((rows_loc, PAIR), lambda j: (0, j)),
            pl.BlockSpec((rows_rem, PAIR), lambda j: (0, j)),
            pl.BlockSpec((rows_loc, 3 * PAIR), lambda j: (0, j)),
            pl.BlockSpec((rows_rem, 3 * PAIR), lambda j: (0, j)),
        ],
        out_shape=[
            jax.ShapeDtypeStruct((rows_loc, pairs * PAIR), BF16),
            jax.ShapeDtypeStruct((rows_rem, pairs * PAIR), BF16),
            jax.ShapeDtypeStruct((rows_loc, 3 * pairs * PAIR), BF16),
            jax.ShapeDtypeStruct((rows_rem, 3 * pairs * PAIR), BF16),
        ],
        scratch_shapes=[pltpu.VMEM((total, PAIR), BF16)] * 4
        + [pltpu.VMEM((PAIR, total - SPEC_PAD + PAIR), BF16)] * 2
        + [pltpu.VMEM((2, total, QBLK), F32), pltpu.VMEM((2, total, QBLK), BF16)]
        + [pltpu.VMEM((total, 2 * QBLK), BF16)] * 2
        + [pltpu.VMEM((total, PAIR), F32)] * 2
        + [pltpu.VMEM((total, PAIR), BF16)] * 2,
        cost_estimate=pl.CostEstimate(flops=flops, bytes_accessed=8 * total * pairs * PAIR * 2,
                                      transcendentals=2 * pairs * total * total),
        name="fused_attention",
    )(qkv_loc, qkv_rem, da_loc, da_rem)


def norm_stats(x_rows):
    x_float = x_rows.astype(F32)
    centered = x_float - jnp.mean(x_float, axis=-1, keepdims=True)
    inv_std = lax.rsqrt(jnp.mean(centered * centered, axis=-1, keepdims=True) + LN_EPS)
    return centered * inv_std, inv_std


def norm_forward(x_rows, ln_scale, ln_bias):
    x_hat, _ = norm_stats(x_rows)
    return (x_hat * ln_scale + ln_bias).astype(BF16)


def matmul(a, b):
    return jnp.einsum('...d,de->...e', a, b, preferred_element_type=F32)


def matmul_t(a, b):
    return jnp.einsum('...e,de->...d', a, b, preferred_element_type=F32)


def token_dot(a, b):
    return jnp.einsum('td,te->de', a.reshape(-1, a.shape[-1]), b.reshape(-1, b.shape[-1]), preferred_element_type=F32)


def solution(mesh):
    group_size = mesh.shape['sp']
    partner = [(i, i ^ 1) for i in range(group_size)]
    across = [(i, i ^ 2) for i in range(group_size)]

    def swap(vals):
        return lax.ppermute(vals, 'sp', partner)

    def cross(vals):
        return lax.ppermute(vals, 'sp', across)

    def local_block(x_special, x_patch, dy_special, dy_patch, ln_scale, ln_bias, w_qkv, b_qkv, w_proj, b_proj, layer_scale):
        num_images, n_spec, d_model = x_special.shape
        patch = x_patch.shape[1]
        half = d_model // 2
        pairs = half // PAIR
        core = lax.axis_index('sp') % 2

        xd_own = jnp.stack([x_patch, dy_patch], axis=1)
        xd_across = [cross(xd_own[i]) for i in range(num_images)]
        xd_partner = swap(xd_own)
        xd_relay = [swap(vals) for vals in xd_across]

        pad = ((0, 0), (0, SPEC_PAD - n_spec), (0, 0))
        x_spec = jnp.pad(x_special, pad)
        dy_spec = jnp.pad(dy_special, pad)

        w_split = w_qkv.reshape(d_model, 3, 2, pairs, PAIR).transpose(2, 0, 3, 1, 4).reshape(2, d_model, 3 * half)
        b_split = b_qkv.reshape(3, 2, pairs, PAIR).transpose(1, 2, 0, 3).reshape(2, 3 * half)
        w_own = lax.dynamic_index_in_dim(w_split, core, 0, keepdims=False)
        w_par = lax.dynamic_index_in_dim(w_split, 1 - core, 0, keepdims=False)
        b_own = lax.dynamic_index_in_dim(b_split, core, 0, keepdims=False)
        wp_split = w_proj.reshape(2, half, d_model)
        wp_own = lax.dynamic_index_in_dim(wp_split, core, 0, keepdims=False)
        wp_par = lax.dynamic_index_in_dim(wp_split, 1 - core, 0, keepdims=False)

        def project(x_rows, dy_rows):
            normed = norm_forward(x_rows, ln_scale, ln_bias)
            qkv = (matmul(normed, w_own) + b_own).astype(BF16)
            d_proj = (dy_rows.astype(F32) * layer_scale).astype(BF16)
            d_attn = matmul_t(d_proj, wp_own).astype(BF16)
            return normed, qkv, d_attn

        x_loc = jnp.concatenate([x_patch, xd_partner[:, 0], x_spec], axis=1)
        dy_loc = jnp.concatenate([dy_patch, xd_partner[:, 1], dy_spec], axis=1)
        normed_loc, qkv_loc, da_loc = project(x_loc, dy_loc)

        attn_locs, dqkv_locs, got_attn, got_dqkv = [], [], [], []
        d_w = d_g = d_b = d_dy = None
        for i in range(num_images):
            x_rem = jnp.concatenate([xd_across[i][0], xd_relay[i][0]], axis=0)
            dy_rem = jnp.concatenate([xd_across[i][1], xd_relay[i][1]], axis=0)
            normed_rem, qkv_rem, da_rem = project(x_rem, dy_rem)
            attn_loc, attn_rem, dqkv_loc, dqkv_rem = fused_attention(qkv_loc, qkv_rem, da_loc, da_rem, i, n_spec)
            attn_locs.append(attn_loc)
            dqkv_locs.append(dqkv_loc)
            got_attn.append(swap(attn_loc[patch:]))
            got_dqkv.append(swap(dqkv_loc[patch:]))
            parts = (token_dot(normed_rem, dqkv_rem), token_dot(attn_rem, dy_rem),
                     jnp.sum(dqkv_rem, axis=0, dtype=F32), jnp.sum(dy_rem, axis=0, dtype=F32))
            if i == 0:
                d_w, d_g, d_b, d_dy = parts
            else:
                d_w, d_g, d_b, d_dy = (d_w + parts[0], d_g + parts[1], d_b + parts[2], d_dy + parts[3])

        attn_all = jnp.stack(attn_locs)
        dqkv_all = jnp.stack(dqkv_locs)
        d_w = d_w + token_dot(normed_loc, dqkv_all)
        d_g = d_g + token_dot(attn_all, dy_loc)
        d_b = d_b + jnp.sum(dqkv_all, axis=(0, 1), dtype=F32)
        d_dy = d_dy + jnp.sum(dy_loc, axis=(0, 1), dtype=F32)

        d_wp = d_g * layer_scale
        d_scale_part = jnp.sum(wp_own.astype(F32) * d_g, axis=0)
        d_w_got, d_wp_got = swap(d_w), swap(d_wp)
        small = jnp.concatenate([d_b, d_scale_part])
        small_got = swap(small)

        def mine(vals):
            return jnp.concatenate([vals[:, :patch], vals[:, 2 * patch:]], axis=1)

        x_own = jnp.concatenate([x_patch, x_spec], axis=1).astype(F32)
        dy_own = jnp.concatenate([dy_patch, dy_spec], axis=1).astype(F32)
        proj = matmul(mine(attn_all), wp_own) + matmul(jnp.stack(got_attn), wp_par) + b_proj
        out = (x_own + layer_scale * proj).astype(BF16)

        d_normed = (matmul_t(mine(dqkv_all), w_own) + matmul_t(jnp.stack(got_dqkv), w_par)).astype(BF16).astype(F32)
        x_hat, inv_std = norm_stats(x_own)
        grad_hat = d_normed * ln_scale
        d_rows = inv_std * (grad_hat - jnp.mean(grad_hat, axis=-1, keepdims=True)
                            - x_hat * jnp.mean(grad_hat * x_hat, axis=-1, keepdims=True))
        dx = (dy_own + d_rows).astype(BF16)

        scaled = d_normed * x_hat
        ln_patch = jnp.stack([jnp.sum(scaled[:, :patch], axis=(0, 1)), jnp.sum(d_normed[:, :patch], axis=(0, 1))])
        ln_spec = jnp.stack([jnp.sum(scaled[:, patch:], axis=(0, 1)), jnp.sum(d_normed[:, patch:], axis=(0, 1))])
        ln_patch = ln_patch + cross(ln_patch)
        ln_patch = ln_patch + swap(ln_patch)
        ln_grads = ln_patch + ln_spec

        def by_core(own, got, axis):
            first = core == 0
            return jnp.stack([jnp.where(first, own, got), jnp.where(first, got, own)], axis=axis)

        d_w_qkv = by_core(d_w, d_w_got, 0).reshape(2, d_model, pairs, 3, PAIR).transpose(1, 3, 0, 2, 4).reshape(d_model, 3 * d_model)
        d_b_qkv = by_core(d_b, small_got[:3 * half], 0).reshape(2, pairs, 3, PAIR).transpose(2, 0, 1, 3).reshape(3 * d_model)
        d_w_proj = by_core(d_wp, d_wp_got, 0).reshape(d_model, d_model)
        d_scale = d_scale_part + small_got[3 * half:] + b_proj * d_dy
        d_b_proj = layer_scale * d_dy
        return (out[:, patch:patch + n_spec], out[:, :patch], dx[:, patch:patch + n_spec], dx[:, :patch],
                ln_grads[0], ln_grads[1], d_w_qkv, d_b_qkv, d_w_proj, d_b_proj, d_scale)

    part_rows = P('dp')
    part_seq = P('dp', 'sp')
    replicated = P()
    return jax.shard_map(
        local_block, mesh=mesh,
        in_specs=(part_rows, part_seq, part_rows, part_seq, replicated, replicated, replicated, replicated, replicated, replicated, replicated),
        out_specs=(part_rows, part_seq, part_rows, part_seq, part_rows, part_rows, part_rows, part_rows, part_rows, part_rows, part_rows),
        check_vma=False)
```

```python
import functools

import jax
import jax.numpy as jnp
from jax import lax
from jax.experimental import pallas as pl
from jax.experimental.pallas import tpu as pltpu
from jax.sharding import PartitionSpec as P

HEAD_DIM = 64
PAIR = 2 * HEAD_DIM
LN_EPS = 1e-6
ATTN_SCALE = HEAD_DIM ** -0.5
SPEC_PAD = 16
QBLK = 256
F32 = jnp.float32
BF16 = jnp.bfloat16


def dot_nt(a, b):
    return lax.dot_general(a, b, (((1,), (1,)), ((), ())), preferred_element_type=F32)


def dot_nn(a, b):
    return lax.dot_general(a, b, (((1,), (0,)), ((), ())), preferred_element_type=F32)


def attn_kernel(n_spec, qkv_loc, qkv_rem, da_loc, da_rem, attn_loc, attn_rem, dqkv_loc, dqkv_rem,
                q_s, k_s, v_s, da_s, vt_s, kt_s, s_s, dp_s, p_s, ds_s, dv_s, dk_s):
    loc = qkv_loc.shape[0] - SPEC_PAD
    rem = qkv_rem.shape[0]
    main = loc + rem
    total = main + SPEC_PAD
    chunk = 80

    def fill(dst, src_loc, src_rem, col, scale):
        def put(start, vals):
            dst[start:start + vals.shape[0], :] = vals if scale is None else vals * jnp.asarray(scale, BF16)
        put(0, src_loc[0:loc, col:col + PAIR])
        put(loc, src_rem[:, col:col + PAIR])
        put(main, src_loc[loc:loc + SPEC_PAD, col:col + PAIR])

    fill(q_s, qkv_loc, qkv_rem, 0, ATTN_SCALE)
    fill(k_s, qkv_loc, qkv_rem, PAIR, None)
    fill(v_s, qkv_loc, qkv_rem, 2 * PAIR, None)
    fill(da_s, da_loc, da_rem, 0, None)

    def transpose_in():
        for dst, src, scale in ((vt_s, v_s, 1.0), (kt_s, k_s, ATTN_SCALE)):
            for row in range(0, main, PAIR):
                dst[:, row:row + PAIR] = (src[row:row + PAIR, :] * jnp.asarray(scale, BF16)).T
            tail = jnp.concatenate([src[main:total, :] * jnp.asarray(scale, BF16),
                                    jnp.zeros((PAIR - SPEC_PAD, PAIR), BF16)], axis=0)
            dst[:, main:main + PAIR] = tail.T

    def head_mask(rows, head):
        lane = lax.broadcasted_iota(jnp.int32, (rows, PAIR), 1)
        return (lane < HEAD_DIM) if head == 0 else (lane >= HEAD_DIM)

    def masked(rows_ref, start, rows):
        vals = rows_ref[start:start + rows, :]
        zero = jnp.zeros_like(vals)
        return [jnp.where(head_mask(rows, h), vals, zero) for h in range(2)]

    blocks = [None] + list(range(0, main, QBLK))

    def widths(t):
        return [(0, PAIR)] if blocks[t] is None else [(0, QBLK), (QBLK, QBLK)]

    def operands(t, rows_ref):
        if blocks[t] is None:
            parts = masked(rows_ref, main, SPEC_PAD)
            return [jnp.concatenate(parts + [jnp.zeros((PAIR - 2 * SPEC_PAD, PAIR), BF16)], axis=0)]
        return masked(rows_ref, blocks[t], QBLK)

    tops = {}

    def stage_scores(t):
        slot = t % 2
        tops[t] = []
        for (col, width), q_rows, d_rows in zip(widths(t), operands(t, q_s), operands(t, da_s)):
            s_val = dot_nt(k_s[...], q_rows)
            row = lax.broadcasted_iota(jnp.int32, (SPEC_PAD, width), 0)
            spec = jnp.where(row < n_spec, s_val[main:total], -jnp.inf)
            s_s[slot, 0:main, col:col + width] = s_val[0:main]
            s_s[slot, main:total, col:col + width] = spec
            tops[t].append(jnp.maximum(jnp.max(s_val[0:main], axis=0, keepdims=True), jnp.max(spec, axis=0, keepdims=True)))
            dp_s[slot, :, col:col + width] = dot_nt(v_s[...], d_rows).astype(BF16)

    def stage_softmax(t):
        slot = t % 2
        for (col, width), top in zip(widths(t), tops[t]):
            norm = jnp.zeros((8, width), F32)
            mix = jnp.zeros((8, width), F32)
            for r in range(0, total, chunk):
                e = jnp.exp(s_s[slot, r:r + chunk, col:col + width] - top)
                s_s[slot, r:r + chunk, col:col + width] = e
                ed = e * dp_s[slot, r:r + chunk, col:col + width].astype(F32)
                for g in range(0, chunk, 8):
                    norm = norm + e[g:g + 8]
                    mix = mix + ed[g:g + 8]
            inv = 1.0 / jnp.sum(norm, axis=0, keepdims=True)
            mix = jnp.sum(mix, axis=0, keepdims=True) * inv
            for r in range(0, total, chunk):
                prob = s_s[slot, r:r + chunk, col:col + width] * inv
                p_s[slot, r:r + chunk, col:col + width] = prob.astype(BF16)
                ds = prob * (dp_s[slot, r:r + chunk, col:col + width].astype(F32) - mix)
                ds_s[slot, r:r + chunk, col:col + width] = ds.astype(BF16)

    def emit(dst_loc, dst_rem, col, start, vals):
        rows = vals.shape[0]
        vals = vals.astype(BF16)
        if start >= main:
            dst_loc[loc:loc + SPEC_PAD, col:col + PAIR] = vals
        elif start < loc:
            dst_loc[start:start + rows, col:col + PAIR] = vals
        else:
            dst_rem[start - loc:start - loc + rows, col:col + PAIR] = vals

    def stage_outputs(t):
        slot = t % 2
        span = sum(width for _, width in widths(t))
        for acc, vals, rows_ref, col in ((dv_s, p_s, da_s, 2 * PAIR), (dk_s, ds_s, q_s, PAIR)):
            part = dot_nn(vals[slot, :, 0:span], jnp.concatenate(operands(t, rows_ref), axis=0))
            if t == 0:
                acc[...] = part
            elif t < len(blocks) - 1:
                acc[...] += part
            else:
                done = acc[...] + part
                emit(dqkv_loc, dqkv_rem, col, 0, done[0:loc])
                emit(dqkv_loc, dqkv_rem, col, loc, done[loc:main])
                emit(dqkv_loc, dqkv_rem, col, main, done[main:total])
        for outs, lhs, vals in (((attn_loc, attn_rem), vt_s, p_s), ((dqkv_loc, dqkv_rem), kt_s, ds_s)):
            if blocks[t] is None:
                both = dot_nn(lhs[:, 0:total], vals[slot, :, 0:PAIR]).T
                emit(*outs, 0, main, jnp.where(head_mask(SPEC_PAD, 0), both[0:SPEC_PAD], both[SPEC_PAD:2 * SPEC_PAD]))
            else:
                both = jnp.concatenate(
                    [dot_nn(lhs[h * HEAD_DIM:(h + 1) * HEAD_DIM, 0:total], vals[slot, :, h * QBLK:(h + 1) * QBLK])
                     for h in range(2)], axis=0)
                for c in range(0, QBLK, PAIR):
                    emit(*outs, 0, blocks[t] + c, both[:, c:c + PAIR].T)

    steps = len(blocks)
    stage_scores(0)
    transpose_in()
    for t in range(steps + 1):
        if t + 1 < steps:
            stage_scores(t + 1)
        if t >= 1:
            stage_outputs(t - 1)
        if t < steps:
            stage_softmax(t)


def fused_attention(qkv_loc, qkv_rem, da_loc, da_rem, image, n_spec):
    rows_loc, rows_rem = qkv_loc.shape[1], qkv_rem.shape[0]
    pairs = da_rem.shape[1] // PAIR
    total = rows_loc + rows_rem
    flops = 2 * 6 * total * total * PAIR * pairs * 4
    return pl.pallas_call(
        functools.partial(attn_kernel, n_spec),
        grid=(pairs,),
        in_specs=[
            pl.BlockSpec((None, rows_loc, 3 * PAIR), lambda j: (image, 0, j)),
            pl.BlockSpec((rows_rem, 3 * PAIR), lambda j: (0, j)),
            pl.BlockSpec((None, rows_loc, PAIR), lambda j: (image, 0, j)),
            pl.BlockSpec((rows_rem, PAIR), lambda j: (0, j)),
        ],
        out_specs=[
            pl.BlockSpec((rows_loc, PAIR), lambda j: (0, j)),
            pl.BlockSpec((rows_rem, PAIR), lambda j: (0, j)),
            pl.BlockSpec((rows_loc, 3 * PAIR), lambda j: (0, j)),
            pl.BlockSpec((rows_rem, 3 * PAIR), lambda j: (0, j)),
        ],
        out_shape=[
            jax.ShapeDtypeStruct((rows_loc, pairs * PAIR), BF16),
            jax.ShapeDtypeStruct((rows_rem, pairs * PAIR), BF16),
            jax.ShapeDtypeStruct((rows_loc, 3 * pairs * PAIR), BF16),
            jax.ShapeDtypeStruct((rows_rem, 3 * pairs * PAIR), BF16),
        ],
        scratch_shapes=[pltpu.VMEM((total, PAIR), BF16)] * 4
        + [pltpu.VMEM((PAIR, total - SPEC_PAD + PAIR), BF16)] * 2
        + [pltpu.VMEM((2, total, 2 * QBLK), F32)]
        + [pltpu.VMEM((2, total, 2 * QBLK), BF16)] * 3
        + [pltpu.VMEM((total, PAIR), F32)] * 2,
        cost_estimate=pl.CostEstimate(flops=flops, bytes_accessed=8 * total * pairs * PAIR * 2,
                                      transcendentals=2 * pairs * total * total),
        name="fused_attention",
    )(qkv_loc, qkv_rem, da_loc, da_rem)


def merge_kernel(core_ref, own_ref, got_ref, out_ref, *, half_of):
    use_own = half_of(pl.program_id(0)) == core_ref[0]

    @pl.when(use_own)
    def _():
        out_ref[...] = own_ref[...]

    @pl.when(jnp.logical_not(use_own))
    def _():
        out_ref[...] = got_ref[...]


def merge_columns(core, own, got):
    rows, cols = own.shape
    pairs = cols // (3 * PAIR)

    def half_of(g):
        return (g // pairs) % 2

    def source(half_wanted):
        def index(g, core_ref):
            third, half, pair = g // (2 * pairs), (g // pairs) % 2, g % pairs
            wanted = half == (core_ref[0] if half_wanted == 0 else 1 - core_ref[0])
            return (0, jnp.where(wanted, pair, jnp.where(half == 0, 0, pairs - 1)) * 3 + third)
        return index

    return pl.pallas_call(
        functools.partial(merge_kernel, half_of=half_of),
        grid_spec=pltpu.PrefetchScalarGridSpec(
            num_scalar_prefetch=1, grid=(6 * pairs,),
            in_specs=[pl.BlockSpec((rows, PAIR), source(0)), pl.BlockSpec((rows, PAIR), source(1))],
            out_specs=pl.BlockSpec((rows, PAIR), lambda g, core_ref: (0, g))),
        out_shape=jax.ShapeDtypeStruct((rows, 2 * cols), own.dtype),
        name="merge_columns",
    )(core, own, got)


def merge_rows(core, own, got):
    rows, cols = own.shape
    tile = PAIR
    count = rows // tile

    def half_of(g):
        return g // count

    def source(half_wanted):
        def index(g, core_ref):
            wanted = g // count == (core_ref[0] if half_wanted == 0 else 1 - core_ref[0])
            return (jnp.where(wanted, g % count, jnp.where(g // count == 0, 0, count - 1)), 0)
        return index

    return pl.pallas_call(
        functools.partial(merge_kernel, half_of=half_of),
        grid_spec=pltpu.PrefetchScalarGridSpec(
            num_scalar_prefetch=1, grid=(2 * count,),
            in_specs=[pl.BlockSpec((tile, cols), source(0)), pl.BlockSpec((tile, cols), source(1))],
            out_specs=pl.BlockSpec((tile, cols), lambda g, core_ref: (g, 0))),
        out_shape=jax.ShapeDtypeStruct((2 * rows, cols), own.dtype),
        name="merge_rows",
    )(core, own, got)


def norm_stats(x_rows):
    x_float = x_rows.astype(F32)
    centered = x_float - jnp.mean(x_float, axis=-1, keepdims=True)
    inv_std = lax.rsqrt(jnp.mean(centered * centered, axis=-1, keepdims=True) + LN_EPS)
    return centered * inv_std, inv_std


def norm_forward(x_rows, ln_scale, ln_bias):
    x_hat, _ = norm_stats(x_rows)
    return (x_hat * ln_scale + ln_bias).astype(BF16)


def matmul(a, b):
    return jnp.einsum('...d,de->...e', a, b, preferred_element_type=F32)


def matmul_t(a, b):
    return jnp.einsum('...e,de->...d', a, b, preferred_element_type=F32)


def token_dot(a, b):
    return jnp.einsum('td,te->de', a.reshape(-1, a.shape[-1]), b.reshape(-1, b.shape[-1]), preferred_element_type=F32)


def solution(mesh):
    group_size = mesh.shape['sp']
    partner = [(i, i ^ 1) for i in range(group_size)]
    opposite = [(i, i ^ 2) for i in range(group_size)]

    def swap(vals):
        return lax.ppermute(vals, 'sp', partner)

    def cross(vals):
        return lax.ppermute(vals, 'sp', opposite)

    def local_block(x_special, x_patch, dy_special, dy_patch, ln_scale, ln_bias, w_qkv, b_qkv, w_proj, b_proj, layer_scale):
        num_images, n_spec, d_model = x_special.shape
        patch = x_patch.shape[1]
        half = d_model // 2
        pairs = half // PAIR
        core = lax.axis_index('sp') % 2

        across = [(cross(x_patch[i]), cross(dy_patch[i])) for i in range(num_images)]
        x_partner, dy_partner = swap(x_patch), swap(dy_patch)

        pad = ((0, 0), (0, SPEC_PAD - n_spec), (0, 0))
        x_spec = jnp.pad(x_special, pad)
        dy_spec = jnp.pad(dy_special, pad)

        w_split = w_qkv.reshape(d_model, 3, 2, pairs, PAIR).transpose(2, 0, 3, 1, 4).reshape(2, d_model, 3 * half)
        b_split = b_qkv.reshape(3, 2, pairs, PAIR).transpose(1, 2, 0, 3).reshape(2, 3 * half)
        w_own = lax.dynamic_index_in_dim(w_split, core, 0, keepdims=False)
        w_par = lax.dynamic_index_in_dim(w_split, 1 - core, 0, keepdims=False)
        b_own = lax.dynamic_index_in_dim(b_split, core, 0, keepdims=False)
        wp_split = w_proj.reshape(2, half, d_model)
        wp_own = lax.dynamic_index_in_dim(wp_split, core, 0, keepdims=False)
        wp_par = lax.dynamic_index_in_dim(wp_split, 1 - core, 0, keepdims=False)

        def project(x_rows, dy_rows):
            normed = norm_forward(x_rows, ln_scale, ln_bias)
            qkv = (matmul(normed, w_own) + b_own).astype(BF16)
            d_proj = (dy_rows.astype(F32) * layer_scale).astype(BF16)
            d_attn = matmul_t(d_proj, wp_own).astype(BF16)
            return normed, qkv, d_attn

        x_loc = jnp.concatenate([x_patch, x_partner, x_spec], axis=1)
        dy_loc = jnp.concatenate([dy_patch, dy_partner, dy_spec], axis=1)
        normed_loc, qkv_loc, da_loc = project(x_loc, dy_loc)

        attn_locs, dqkv_locs, attn_rems, got_attn, got_dqkv = [], [], [], [], []
        relays = {}

        def gate(vals, image):
            if image < 0:
                return vals
            return lax.optimization_barrier((vals, attn_rems[image]))[0]

        def relay_image(image, after):
            across[image] = gate(across[image], after)
            relays[image] = (swap(across[image][0]), swap(across[image][1]))

        relay_image(0, -1)
        d_w = d_g = d_b = d_dy = None
        for i in range(num_images):
            near, relay = gate((across[i], relays[i]), i - 1)
            x_rem = jnp.concatenate([near[0], relay[0]], axis=0)
            dy_rem = jnp.concatenate([near[1], relay[1]], axis=0)
            normed_rem, qkv_rem, da_rem = project(x_rem, dy_rem)
            attn_loc, attn_rem, dqkv_loc, dqkv_rem = fused_attention(qkv_loc, qkv_rem, da_loc, da_rem, i, n_spec)
            attn_locs.append(attn_loc)
            attn_rems.append(attn_rem)
            for image in ((1, 2), (3,), (), ())[i]:
                relay_image(image, i)
            dqkv_locs.append(dqkv_loc)
            got_attn.append(swap(attn_loc[patch:]))
            got_dqkv.append(swap(dqkv_loc[patch:]))
            parts = (token_dot(normed_rem, dqkv_rem), token_dot(attn_rem, dy_rem),
                     jnp.sum(dqkv_rem, axis=0, dtype=F32), jnp.sum(dy_rem, axis=0, dtype=F32))
            if i == 0:
                d_w, d_g, d_b, d_dy = parts
            else:
                d_w, d_g, d_b, d_dy = (d_w + parts[0], d_g + parts[1], d_b + parts[2], d_dy + parts[3])

        attn_all = jnp.stack(attn_locs)
        dqkv_all = jnp.stack(dqkv_locs)
        d_w = d_w + token_dot(normed_loc, dqkv_all)
        d_g = d_g + token_dot(attn_all, dy_loc)
        d_b = d_b + jnp.sum(dqkv_all, axis=(0, 1), dtype=F32)
        d_dy = d_dy + jnp.sum(dy_loc, axis=(0, 1), dtype=F32)

        d_wp = d_g * layer_scale
        d_scale_part = jnp.sum(wp_own.astype(F32) * d_g, axis=0)
        d_w_got, d_wp_got = swap(d_w), swap(d_wp)
        small = jnp.concatenate([d_b, d_scale_part])
        small_got = swap(small)

        def mine(vals):
            return jnp.concatenate([vals[:, :patch], vals[:, 2 * patch:]], axis=1)

        x_own = jnp.concatenate([x_patch, x_spec], axis=1).astype(F32)
        dy_own = jnp.concatenate([dy_patch, dy_spec], axis=1).astype(F32)
        proj = matmul(mine(attn_all), wp_own) + matmul(jnp.stack(got_attn), wp_par) + b_proj
        out = (x_own + layer_scale * proj).astype(BF16)

        d_normed = (matmul_t(mine(dqkv_all), w_own) + matmul_t(jnp.stack(got_dqkv), w_par)).astype(BF16).astype(F32)
        x_hat, inv_std = norm_stats(x_own)
        grad_hat = d_normed * ln_scale
        d_rows = inv_std * (grad_hat - jnp.mean(grad_hat, axis=-1, keepdims=True)
                            - x_hat * jnp.mean(grad_hat * x_hat, axis=-1, keepdims=True))
        dx = (dy_own + d_rows).astype(BF16)

        scaled = d_normed * x_hat
        ln_patch = jnp.stack([jnp.sum(scaled[:, :patch], axis=(0, 1)), jnp.sum(d_normed[:, :patch], axis=(0, 1))])
        ln_spec = jnp.stack([jnp.sum(scaled[:, patch:], axis=(0, 1)), jnp.sum(d_normed[:, patch:], axis=(0, 1))])
        ln_patch = ln_patch + cross(ln_patch)
        ln_patch = ln_patch + swap(ln_patch)
        ln_grads = ln_patch + ln_spec

        core_arr = core.reshape(1).astype(jnp.int32)
        first = core == 0
        d_w_qkv = merge_columns(core_arr, d_w, d_w_got)
        d_w_proj = merge_rows(core_arr, d_wp, d_wp_got)
        b_both = jnp.stack([jnp.where(first, d_b, small_got[:3 * half]), jnp.where(first, small_got[:3 * half], d_b)])
        d_b_qkv = b_both.reshape(2, pairs, 3, PAIR).transpose(2, 0, 1, 3).reshape(3 * d_model)
        d_scale = d_scale_part + small_got[3 * half:] + b_proj * d_dy
        d_b_proj = layer_scale * d_dy
        return (out[:, patch:patch + n_spec], out[:, :patch], dx[:, patch:patch + n_spec], dx[:, :patch],
                ln_grads[0], ln_grads[1], d_w_qkv, d_b_qkv, d_w_proj, d_b_proj, d_scale)

    part_rows = P('dp')
    part_seq = P('dp', 'sp')
    replicated = P()
    return jax.shard_map(
        local_block, mesh=mesh,
        in_specs=(part_rows, part_seq, part_rows, part_seq, replicated, replicated, replicated, replicated, replicated, replicated, replicated),
        out_specs=(part_rows, part_seq, part_rows, part_seq, part_rows, part_rows, part_rows, part_rows, part_rows, part_rows, part_rows),
        check_vma=False)
```

```python
import functools

import jax
import jax.numpy as jnp
from jax import lax
from jax.experimental import pallas as pl
from jax.experimental.pallas import tpu as pltpu
from jax.sharding import PartitionSpec as P

HEAD_DIM = 64
PAIR = 2 * HEAD_DIM
LN_EPS = 1e-6
ATTN_SCALE = HEAD_DIM ** -0.5
SPEC_PAD = 16
QBLK = 256
F32 = jnp.float32
BF16 = jnp.bfloat16


def dot_nt(a, b):
    return lax.dot_general(a, b, (((1,), (1,)), ((), ())), preferred_element_type=F32)


def dot_nn(a, b):
    return lax.dot_general(a, b, (((1,), (0,)), ((), ())), preferred_element_type=F32)


def block_kernel(n_spec, first, *refs):
    (x_own, x_par, x_acr, x_rel, x_spc, dy_own, dy_par, dy_acr, dy_rel, dy_spc,
     ln_s, ln_b, l_scale, w_ref, b_ref, wp_ref) = refs[:16]
    refs = refs[16:]
    if first:
        acc_in = None
    else:
        acc_in, refs = refs[:5], refs[5:]
    attn_own, attn_par, dqkv_own, dqkv_par = refs[:4]
    acc_out, refs = refs[4:9], refs[9:]
    (norm_s, normt_s, dproj_s, q_s, k_s, v_s, da_s, vt_s, kt_s, s_s, dp_s, p_s, ds_s, dv_s, dk_s, at_s, dqkv_s) = refs
    patch = x_own.shape[-2]
    main = 4 * patch
    total = main + SPEC_PAD
    chunk = 80
    pair = pl.program_id(0)
    pieces = [(x_own, dy_own, 0, patch), (x_par, dy_par, patch, patch), (x_acr, dy_acr, 2 * patch, patch),
              (x_rel, dy_rel, 3 * patch, patch), (x_spc, dy_spc, main, SPEC_PAD)]

    @pl.when(pair == 0)
    def _():
        for x_ref, dy_ref, start, rows in pieces:
            step = min(rows, 64)

            @pl.loop(0, rows // step)
            def _(i):
                src = pl.ds(pl.multiple_of(i * step, step), step)
                dst = pl.ds(pl.multiple_of(start + i * step, step), step)
                x_float = x_ref[src, :].astype(F32)
                centered = x_float - jnp.mean(x_float, axis=-1, keepdims=True)
                inv_std = lax.rsqrt(jnp.mean(centered * centered, axis=-1, keepdims=True) + LN_EPS)
                norm_s[dst, :] = (centered * inv_std * ln_s[...] + ln_b[...]).astype(BF16)
                dproj_s[dst, :] = (dy_ref[src, :].astype(F32) * l_scale[...]).astype(BF16)

        width = norm_s.shape[1]

        @pl.loop(0, main // PAIR)
        def _(i):
            rows = pl.ds(pl.multiple_of(i * PAIR, PAIR), PAIR)
            for c in range(0, width, PAIR):
                normt_s[c:c + PAIR, rows] = norm_s[rows, c:c + PAIR].T

        for c in range(0, width, PAIR):
            tail = jnp.concatenate([norm_s[main:total, c:c + PAIR], jnp.zeros((PAIR - SPEC_PAD, PAIR), BF16)], axis=0)
            normt_s[c:c + PAIR, main:main + PAIR] = tail.T

        d_dy = jnp.zeros(acc_out[4].shape, F32)
        for _, dy_ref, _, rows in pieces:
            d_dy = d_dy + jnp.sum(dy_ref[...].astype(F32).reshape(rows // 8, 8, dy_ref.shape[-1]), axis=0)
        acc_out[4][...] = d_dy if first else acc_in[4][...] + d_dy

    scale = jnp.asarray(ATTN_SCALE, BF16)
    qkv = dot_nn(norm_s[...], w_ref[...]) + b_ref[...]
    q_s[...] = qkv[:, 0:PAIR].astype(BF16) * scale
    k_s[...] = qkv[:, PAIR:2 * PAIR].astype(BF16)
    v_s[...] = qkv[:, 2 * PAIR:3 * PAIR].astype(BF16)
    da_s[...] = dot_nt(dproj_s[...], wp_ref[...]).astype(BF16)

    def transpose_in():
        for dst, src, mult in ((vt_s, v_s, None), (kt_s, k_s, scale)):
            for row in range(0, main, PAIR):
                vals = src[row:row + PAIR, :]
                dst[:, row:row + PAIR] = (vals if mult is None else vals * mult).T
            vals = src[main:total, :]
            tail = jnp.concatenate([vals if mult is None else vals * mult,
                                    jnp.zeros((PAIR - SPEC_PAD, PAIR), BF16)], axis=0)
            dst[:, main:main + PAIR] = tail.T

    def head_mask(rows, head):
        lane = lax.broadcasted_iota(jnp.int32, (rows, PAIR), 1)
        return (lane < HEAD_DIM) if head == 0 else (lane >= HEAD_DIM)

    def masked(rows_ref, start, rows):
        vals = rows_ref[start:start + rows, :]
        zero = jnp.zeros_like(vals)
        return [jnp.where(head_mask(rows, h), vals, zero) for h in range(2)]

    blocks = [None] + list(range(0, main, QBLK))

    def widths(t):
        return [(0, PAIR)] if blocks[t] is None else [(0, QBLK), (QBLK, QBLK)]

    def operands(t, rows_ref):
        if blocks[t] is None:
            parts = masked(rows_ref, main, SPEC_PAD)
            return [jnp.concatenate(parts + [jnp.zeros((PAIR - 2 * SPEC_PAD, PAIR), BF16)], axis=0)]
        return masked(rows_ref, blocks[t], QBLK)

    tops = {}

    def stage_scores(t):
        slot = t % 2
        tops[t] = []
        for (col, width), q_rows, d_rows in zip(widths(t), operands(t, q_s), operands(t, da_s)):
            s_val = dot_nt(k_s[...], q_rows)
            row = lax.broadcasted_iota(jnp.int32, (SPEC_PAD, width), 0)
            spec = jnp.where(row < n_spec, s_val[main:total], -jnp.inf)
            s_s[slot, 0:main, col:col + width] = s_val[0:main]
            s_s[slot, main:total, col:col + width] = spec
            tops[t].append(jnp.maximum(jnp.max(s_val[0:main], axis=0, keepdims=True), jnp.max(spec, axis=0, keepdims=True)))
            dp_s[slot, :, col:col + width] = dot_nt(v_s[...], d_rows).astype(BF16)

    def stage_softmax(t):
        slot = t % 2
        for (col, width), top in zip(widths(t), tops[t]):
            norm = jnp.zeros((8, width), F32)
            mix = jnp.zeros((8, width), F32)
            for r in range(0, total, chunk):
                e = jnp.exp(s_s[slot, r:r + chunk, col:col + width] - top)
                s_s[slot, r:r + chunk, col:col + width] = e
                ed = e * dp_s[slot, r:r + chunk, col:col + width].astype(F32)
                for g in range(0, chunk, 8):
                    norm = norm + e[g:g + 8]
                    mix = mix + ed[g:g + 8]
            inv = 1.0 / jnp.sum(norm, axis=0, keepdims=True)
            mix = jnp.sum(mix, axis=0, keepdims=True) * inv
            for r in range(0, total, chunk):
                prob = s_s[slot, r:r + chunk, col:col + width] * inv
                p_s[slot, r:r + chunk, col:col + width] = prob.astype(BF16)
                ds = prob * (dp_s[slot, r:r + chunk, col:col + width].astype(F32) - mix)
                ds_s[slot, r:r + chunk, col:col + width] = ds.astype(BF16)

    def emit_attn(start, vals):
        if start >= main:
            attn_own[patch:patch + SPEC_PAD, :] = vals
            attn_par[patch:patch + SPEC_PAD, :] = vals
        elif start < patch:
            attn_own[start:start + vals.shape[0], :] = vals
        elif start < 2 * patch:
            attn_par[start - patch:start - patch + vals.shape[0], :] = vals

    def stage_outputs(t):
        slot = t % 2
        span = sum(width for _, width in widths(t))
        for acc, vals, rows_ref, col in ((dv_s, p_s, da_s, 2 * PAIR), (dk_s, ds_s, q_s, PAIR)):
            part = dot_nn(vals[slot, :, 0:span], jnp.concatenate(operands(t, rows_ref), axis=0))
            if t == 0:
                acc[...] = part
            elif t < len(blocks) - 1:
                acc[...] += part
            else:
                dqkv_s[:, col:col + PAIR] = (acc[...] + part).astype(BF16)
        for kind, lhs, vals in ((0, vt_s, p_s), (1, kt_s, ds_s)):
            if blocks[t] is None:
                both = dot_nn(lhs[:, 0:total], vals[slot, :, 0:PAIR]).T
                rows = jnp.where(head_mask(SPEC_PAD, 0), both[0:SPEC_PAD], both[SPEC_PAD:2 * SPEC_PAD]).astype(BF16)
                if kind == 0:
                    emit_attn(main, rows)
                    padded = jnp.concatenate([rows, jnp.zeros((PAIR - SPEC_PAD, PAIR), BF16)], axis=0)
                    at_s[:, main:main + PAIR] = padded.T
                else:
                    dqkv_s[main:total, 0:PAIR] = rows
                continue
            both = jnp.concatenate(
                [dot_nn(lhs[h * HEAD_DIM:(h + 1) * HEAD_DIM, 0:total], vals[slot, :, h * QBLK:(h + 1) * QBLK])
                 for h in range(2)], axis=0)
            if kind == 0:
                at_s[:, blocks[t]:blocks[t] + QBLK] = both.astype(BF16)
            if kind == 1 or blocks[t] < 2 * patch:
                for c in range(0, QBLK, PAIR):
                    rows = both[:, c:c + PAIR].T.astype(BF16)
                    if kind == 0:
                        emit_attn(blocks[t] + c, rows)
                    else:
                        dqkv_s[blocks[t] + c:blocks[t] + c + PAIR, 0:PAIR] = rows

    steps = len(blocks)
    stage_scores(0)
    transpose_in()
    for t in range(steps + 1):
        if t + 1 < steps:
            stage_scores(t + 1)
        if t >= 1:
            stage_outputs(t - 1)
        if t < steps:
            stage_softmax(t)

    dqkv_own[0:patch, :] = dqkv_s[0:patch, :]
    dqkv_own[patch:patch + SPEC_PAD, :] = dqkv_s[main:total, :]
    dqkv_par[0:patch, :] = dqkv_s[patch:2 * patch, :]
    dqkv_par[patch:patch + SPEC_PAD, :] = dqkv_s[main:total, :]
    d_b = jnp.sum(dqkv_s[...].astype(F32).reshape(total // 8, 8, 3 * PAIR), axis=0)
    acc_out[3][...] = d_b if first else acc_in[3][...] + d_b
    d_w = dot_nn(normt_s[:, 0:total], dqkv_s[...])
    acc_out[0][...] = (d_w if first else acc_in[0][...].reshape(d_w.shape) + d_w).reshape(acc_out[0].shape)
    d_g = dot_nn(at_s[:, main:main + SPEC_PAD], dy_spc[...])
    for _, dy_ref, start, rows in pieces[:4]:
        d_g = d_g + dot_nn(at_s[:, start:start + rows], dy_ref[...])
    acc_out[1][...] = d_g if first else acc_in[1][...] + d_g
    gls = jnp.sum((wp_ref[...].astype(F32) * acc_out[1][...]).reshape(PAIR // 8, 8, d_g.shape[1]), axis=0)

    @pl.when(pair == 0)
    def _():
        acc_out[2][...] = gls

    @pl.when(pair != 0)
    def _():
        acc_out[2][...] += gls


def fused_block(image, rows, accs, ln_scale, ln_bias, layer_scale, w_own, b_own, wp_own, n_spec):
    x_patch, x_par, x_acr, x_rel, x_spc, dy_patch, dy_par, dy_acr, dy_rel, dy_spc = rows
    patch, d_model = x_acr.shape
    pairs = wp_own.shape[0] // PAIR
    half = pairs * PAIR
    total = 4 * patch + SPEC_PAD
    first = accs is None

    def stacked(count):
        return pl.BlockSpec((None, count, d_model), lambda j: (image, 0, 0))

    whole = pl.BlockSpec((patch, d_model), lambda j: (0, 0))
    vec = pl.BlockSpec((1, d_model), lambda j: (0, 0))
    acc_specs = [
        pl.BlockSpec((d_model, 3 * PAIR), lambda j: (0, j)),
        pl.BlockSpec((PAIR, d_model), lambda j: (j, 0)),
        pl.BlockSpec((8, d_model), lambda j: (0, 0)),
        pl.BlockSpec((8, 3 * PAIR), lambda j: (0, j)),
        pl.BlockSpec((8, d_model), lambda j: (0, 0)),
    ]
    acc_shapes = [
        jax.ShapeDtypeStruct((d_model, 3 * half), F32),
        jax.ShapeDtypeStruct((half, d_model), F32),
        jax.ShapeDtypeStruct((8, d_model), F32),
        jax.ShapeDtypeStruct((8, 3 * half), F32),
        jax.ShapeDtypeStruct((8, d_model), F32),
    ]
    row_spec = [stacked(patch), stacked(patch), whole, whole, stacked(SPEC_PAD)]
    in_specs = row_spec * 2 + [vec] * 3 + [
        pl.BlockSpec((d_model, 3 * PAIR), lambda j: (0, j)),
        pl.BlockSpec((1, 3 * PAIR), lambda j: (0, j)),
        pl.BlockSpec((PAIR, d_model), lambda j: (j, 0)),
    ] + ([] if first else acc_specs)
    flops = 2 * 6 * total * total * PAIR * pairs * 4
    outs = pl.pallas_call(
        functools.partial(block_kernel, n_spec, first),
        grid=(pairs,),
        in_specs=in_specs,
        out_specs=[
            pl.BlockSpec((patch + SPEC_PAD, PAIR), lambda j: (0, j)),
            pl.BlockSpec((patch + SPEC_PAD, PAIR), lambda j: (0, j)),
            pl.BlockSpec((patch + SPEC_PAD, 3 * PAIR), lambda j: (0, j)),
            pl.BlockSpec((patch + SPEC_PAD, 3 * PAIR), lambda j: (0, j)),
        ] + acc_specs,
        out_shape=[jax.ShapeDtypeStruct((patch + SPEC_PAD, half), BF16)] * 2
        + [jax.ShapeDtypeStruct((patch + SPEC_PAD, 3 * half), BF16)] * 2 + acc_shapes,
        scratch_shapes=[pltpu.VMEM((total, d_model), BF16), pltpu.VMEM((d_model, total - SPEC_PAD + PAIR), BF16),
                        pltpu.VMEM((total, d_model), BF16)]
        + [pltpu.VMEM((total, PAIR), BF16)] * 4
        + [pltpu.VMEM((PAIR, total - SPEC_PAD + PAIR), BF16)] * 2
        + [pltpu.VMEM((2, total, 2 * QBLK), F32)]
        + [pltpu.VMEM((2, total, 2 * QBLK), BF16)] * 3
        + [pltpu.VMEM((total, PAIR), F32)] * 2
        + [pltpu.VMEM((PAIR, total - SPEC_PAD + PAIR), BF16), pltpu.VMEM((total, 3 * PAIR), BF16)],
        input_output_aliases={} if first else {16 + i: 4 + i for i in range(5)},
        cost_estimate=pl.CostEstimate(flops=flops, bytes_accessed=8 * total * half * 2,
                                      transcendentals=2 * pairs * total * total),
        compiler_params=pltpu.CompilerParams(vmem_limit_bytes=60 * 1024 * 1024),
        name="fused_block",
    )(x_patch, x_par, x_acr, x_rel, x_spc, dy_patch, dy_par, dy_acr, dy_rel, dy_spc,
      ln_scale, ln_bias, layer_scale, w_own, b_own, wp_own, *([] if first else accs))
    return outs[:4], outs[4:]


def merge_kernel(core_ref, w_own, w_got, g_own, g_got, w_out, g_out):
    pairs = w_own.shape[1] // (3 * PAIR)
    step = pl.program_id(0)
    count = pl.num_programs(0) // 2
    for half in range(2):
        @pl.when(core_ref[0] == half)
        def _():
            for third in range(3):
                for pair in range(pairs):
                    src = (pair * 3 + third) * PAIR
                    dst = (third * 2 * pairs + pair) * PAIR
                    w_out[:, dst + half * pairs * PAIR:dst + half * pairs * PAIR + PAIR] = w_own[:, src:src + PAIR]
                    w_out[:, dst + (1 - half) * pairs * PAIR:dst + (1 - half) * pairs * PAIR + PAIR] = w_got[:, src:src + PAIR]

    @pl.when(step // count == core_ref[0])
    def _():
        g_out[...] = g_own[...]

    @pl.when(step // count != core_ref[0])
    def _():
        g_out[...] = g_got[...]


def merge_grads(core, w_own, w_got, g_own, g_got):
    rows, cols = w_own.shape
    half, d_model = g_own.shape
    tile = PAIR
    count = half // tile
    return pl.pallas_call(
        merge_kernel,
        grid_spec=pltpu.PrefetchScalarGridSpec(
            num_scalar_prefetch=1, grid=(2 * count,),
            in_specs=[pl.BlockSpec((tile, cols), lambda g, c: (g, 0))] * 2
            + [pl.BlockSpec((tile, d_model), lambda g, c: (g % count, 0))] * 2,
            out_specs=[pl.BlockSpec((tile, 2 * cols), lambda g, c: (g, 0)),
                       pl.BlockSpec((tile, d_model), lambda g, c: (g, 0))]),
        out_shape=[jax.ShapeDtypeStruct((rows, 2 * cols), F32), jax.ShapeDtypeStruct((2 * half, d_model), F32)],
        name="merge_grads",
    )(core, w_own, w_got, g_own, g_got)


def norm_stats(x_rows):
    x_float = x_rows.astype(F32)
    centered = x_float - jnp.mean(x_float, axis=-1, keepdims=True)
    inv_std = lax.rsqrt(jnp.mean(centered * centered, axis=-1, keepdims=True) + LN_EPS)
    return centered * inv_std, inv_std


def norm_forward(x_rows, ln_scale, ln_bias):
    x_hat, _ = norm_stats(x_rows)
    return (x_hat * ln_scale + ln_bias).astype(BF16)


def matmul(a, b):
    return jnp.einsum('...d,de->...e', a, b, preferred_element_type=F32)


def matmul_t(a, b):
    return jnp.einsum('...e,de->...d', a, b, preferred_element_type=F32)


def token_dot(a, b):
    return jnp.einsum('td,te->de', a.reshape(-1, a.shape[-1]), b.reshape(-1, b.shape[-1]), preferred_element_type=F32)


def solution(mesh):
    group_size = mesh.shape['sp']
    partner = [(i, i ^ 1) for i in range(group_size)]
    opposite = [(i, i ^ 2) for i in range(group_size)]

    def swap(vals):
        return lax.ppermute(vals, 'sp', partner)

    def cross(vals):
        return lax.ppermute(vals, 'sp', opposite)

    def local_block(x_special, x_patch, dy_special, dy_patch, ln_scale, ln_bias, w_qkv, b_qkv, w_proj, b_proj, layer_scale):
        num_images, n_spec, d_model = x_special.shape
        patch = x_patch.shape[1]
        half = d_model // 2
        pairs = half // PAIR
        core = lax.axis_index('sp') % 2

        across = [(cross(x_patch[i]), cross(dy_patch[i])) for i in range(num_images)]
        x_partner, dy_partner = swap(x_patch), swap(dy_patch)

        pad = ((0, 0), (0, SPEC_PAD - n_spec), (0, 0))
        x_spec = jnp.pad(x_special, pad)
        dy_spec = jnp.pad(dy_special, pad)

        w_split = w_qkv.reshape(d_model, 3, 2, pairs, PAIR).transpose(2, 0, 3, 1, 4).reshape(2, d_model, 3 * half)
        b_split = b_qkv.reshape(3, 2, pairs, PAIR).transpose(1, 2, 0, 3).reshape(2, 3 * half)
        w_own = lax.dynamic_index_in_dim(w_split, core, 0, keepdims=False)
        w_par = lax.dynamic_index_in_dim(w_split, 1 - core, 0, keepdims=False)
        b_own = lax.dynamic_index_in_dim(b_split, core, 0, keepdims=False)
        wp_split = w_proj.reshape(2, half, d_model)
        wp_own = lax.dynamic_index_in_dim(wp_split, core, 0, keepdims=False)
        wp_par = lax.dynamic_index_in_dim(wp_split, 1 - core, 0, keepdims=False)

        attn_owns, dqkv_owns, got_attn, got_dqkv = [], [], [], []
        relays = {}
        accs = None

        def gate(vals, image):
            if image < 0:
                return vals
            return lax.optimization_barrier((vals, attn_owns[image]))[0]

        def relay_image(image, after):
            across[image] = gate(across[image], after)
            relays[image] = (swap(across[image][0]), swap(across[image][1]))

        relay_image(0, -1)
        for i in range(num_images):
            near, relay = gate((across[i], relays[i]), i - 1)
            rows = (x_patch, x_partner, near[0], relay[0], x_spec, dy_patch, dy_partner, near[1], relay[1], dy_spec)
            (attn_own, attn_par, dqkv_own, dqkv_par), accs = fused_block(
                i, rows, accs, ln_scale[None], ln_bias[None], layer_scale[None], w_own, b_own[None], wp_own, n_spec)
            attn_owns.append(attn_own)
            dqkv_owns.append(dqkv_own)
            for image in ((1, 2), (3,), (), ())[i]:
                relay_image(image, i)
            got_attn.append(swap(attn_par))
            got_dqkv.append(swap(dqkv_par))

        d_w, d_g, d_scale_part, d_b, d_dy = accs
        d_scale_part, d_b, d_dy = (jnp.sum(vals, axis=0) for vals in (d_scale_part, d_b, d_dy))
        d_wp = d_g * layer_scale
        d_w_got, d_wp_got = swap(d_w), swap(d_wp)
        small = jnp.concatenate([d_b, d_scale_part])
        small_got = swap(small)

        x_own = jnp.concatenate([x_patch, x_spec], axis=1).astype(F32)
        dy_own = jnp.concatenate([dy_patch, dy_spec], axis=1).astype(F32)
        proj = matmul(jnp.stack(attn_owns), wp_own) + matmul(jnp.stack(got_attn), wp_par) + b_proj
        out = (x_own + layer_scale * proj).astype(BF16)

        d_normed = (matmul_t(jnp.stack(dqkv_owns), w_own) + matmul_t(jnp.stack(got_dqkv), w_par)).astype(BF16).astype(F32)
        x_hat, inv_std = norm_stats(x_own)
        grad_hat = d_normed * ln_scale
        d_rows = inv_std * (grad_hat - jnp.mean(grad_hat, axis=-1, keepdims=True)
                            - x_hat * jnp.mean(grad_hat * x_hat, axis=-1, keepdims=True))
        dx = (dy_own + d_rows).astype(BF16)

        scaled = d_normed * x_hat
        ln_patch = jnp.stack([jnp.sum(scaled[:, :patch], axis=(0, 1)), jnp.sum(d_normed[:, :patch], axis=(0, 1))])
        ln_spec = jnp.stack([jnp.sum(scaled[:, patch:], axis=(0, 1)), jnp.sum(d_normed[:, patch:], axis=(0, 1))])
        ln_patch = ln_patch + cross(ln_patch)
        ln_patch = ln_patch + swap(ln_patch)
        ln_grads = ln_patch + ln_spec

        core_arr = core.reshape(1).astype(jnp.int32)
        first = core == 0
        d_w_qkv, d_w_proj = merge_grads(core_arr, d_w, d_w_got, d_wp, d_wp_got)
        b_both = jnp.stack([jnp.where(first, d_b, small_got[:3 * half]), jnp.where(first, small_got[:3 * half], d_b)])
        d_b_qkv = b_both.reshape(2, pairs, 3, PAIR).transpose(2, 0, 1, 3).reshape(3 * d_model)
        d_scale = d_scale_part + small_got[3 * half:] + b_proj * d_dy
        d_b_proj = layer_scale * d_dy
        return (out[:, patch:patch + n_spec], out[:, :patch], dx[:, patch:patch + n_spec], dx[:, :patch],
                ln_grads[0], ln_grads[1], d_w_qkv, d_b_qkv, d_w_proj, d_b_proj, d_scale)

    part_rows = P('dp')
    part_seq = P('dp', 'sp')
    replicated = P()
    return jax.shard_map(
        local_block, mesh=mesh,
        in_specs=(part_rows, part_seq, part_rows, part_seq, replicated, replicated, replicated, replicated, replicated, replicated, replicated),
        out_specs=(part_rows, part_seq, part_rows, part_seq, part_rows, part_rows, part_rows, part_rows, part_rows, part_rows, part_rows),
        check_vma=False)
```

```python
import functools

import jax
import jax.numpy as jnp
from jax import lax
from jax.experimental import pallas as pl
from jax.experimental.pallas import tpu as pltpu
from jax.sharding import PartitionSpec as P


HEAD_DIM = 64
PAIR = 2 * HEAD_DIM
LN_EPS = 1e-6
ATTN_SCALE = HEAD_DIM ** -0.5
SPEC_PAD = 16
QBLK = 256
F32 = jnp.float32
BF16 = jnp.bfloat16


def dot_nt(a, b):
    return lax.dot_general(a, b, (((1,), (1,)), ((), ())), preferred_element_type=F32)


def dot_nn(a, b):
    return lax.dot_general(a, b, (((1,), (0,)), ((), ())), preferred_element_type=F32)


def block_kernel(n_spec, first, core_ref, *refs):
    (x_own, x_par, x_acr, x_rel, x_spc, dy_own, dy_par, dy_acr, dy_rel, dy_spc,
     ln_s, ln_b, l_scale, wq_ref, wk_ref, wv_ref, bq_ref, bk_ref, bv_ref, wp_ref) = refs[:20]
    refs = refs[20:]
    if first:
        acc_in = None
    else:
        acc_in, refs = refs[:5], refs[5:]
    attn_own, attn_par, dqkv_own, dqkv_par = refs[:4]
    acc_out, refs = refs[4:9], refs[9:]
    (norm_s, normt_s, dproj_s, q_s, k_s, v_s, da_s, vt_s, kt_s, s_s, dp_s, p_s, ds_s, dv_s, dk_s, at_s, dqkv_s) = refs
    patch = x_own.shape[-2]
    main = 4 * patch
    total = main + SPEC_PAD
    chunk = 80
    pair = pl.program_id(0)
    pieces = [(x_own, dy_own, 0, patch), (x_par, dy_par, patch, patch), (x_acr, dy_acr, 2 * patch, patch),
              (x_rel, dy_rel, 3 * patch, patch), (x_spc, dy_spc, main, SPEC_PAD)]

    @pl.when(pair == 0)
    def _():
        for x_ref, dy_ref, start, rows in pieces:
            step = min(rows, 64)

            @pl.loop(0, rows // step)
            def _(i):
                src = pl.ds(pl.multiple_of(i * step, step), step)
                dst = pl.ds(pl.multiple_of(start + i * step, step), step)
                x_float = x_ref[src, :].astype(F32)
                centered = x_float - jnp.mean(x_float, axis=-1, keepdims=True)
                inv_std = lax.rsqrt(jnp.mean(centered * centered, axis=-1, keepdims=True) + LN_EPS)
                norm_s[dst, :] = (centered * inv_std * ln_s[...] + ln_b[...]).astype(BF16)
                dproj_s[dst, :] = (dy_ref[src, :].astype(F32) * l_scale[...]).astype(BF16)

        width = norm_s.shape[1]

        @pl.loop(0, main // PAIR)
        def _(i):
            rows = pl.ds(pl.multiple_of(i * PAIR, PAIR), PAIR)
            for c in range(0, width, PAIR):
                normt_s[c:c + PAIR, rows] = norm_s[rows, c:c + PAIR].T

        for c in range(0, width, PAIR):
            tail = jnp.concatenate([norm_s[main:total, c:c + PAIR], jnp.zeros((PAIR - SPEC_PAD, PAIR), BF16)], axis=0)
            normt_s[c:c + PAIR, main:main + PAIR] = tail.T

        d_dy = jnp.zeros(acc_out[4].shape, F32)
        for _, dy_ref, _, rows in pieces:
            d_dy = d_dy + jnp.sum(dy_ref[...].astype(F32).reshape(rows // 8, 8, dy_ref.shape[-1]), axis=0)
        acc_out[4][...] = d_dy if first else acc_in[4][...] + d_dy

    scale = jnp.asarray(ATTN_SCALE, BF16)
    w_pair = jnp.concatenate([wq_ref[...], wk_ref[...], wv_ref[...]], axis=1)
    qkv = dot_nn(norm_s[...], w_pair) + jnp.concatenate([bq_ref[...], bk_ref[...], bv_ref[...]], axis=1)
    q_s[...] = qkv[:, 0:PAIR].astype(BF16) * scale
    k_s[...] = qkv[:, PAIR:2 * PAIR].astype(BF16)
    v_s[...] = qkv[:, 2 * PAIR:3 * PAIR].astype(BF16)
    da_s[...] = dot_nt(dproj_s[...], wp_ref[...]).astype(BF16)

    def transpose_in():
        for dst, src, mult in ((vt_s, v_s, None), (kt_s, k_s, scale)):
            for row in range(0, main, PAIR):
                vals = src[row:row + PAIR, :]
                dst[:, row:row + PAIR] = (vals if mult is None else vals * mult).T
            vals = src[main:total, :]
            tail = jnp.concatenate([vals if mult is None else vals * mult,
                                    jnp.zeros((PAIR - SPEC_PAD, PAIR), BF16)], axis=0)
            dst[:, main:main + PAIR] = tail.T

    def head_mask(rows, head):
        lane = lax.broadcasted_iota(jnp.int32, (rows, PAIR), 1)
        return (lane < HEAD_DIM) if head == 0 else (lane >= HEAD_DIM)

    def masked(rows_ref, start, rows):
        vals = rows_ref[start:start + rows, :]
        zero = jnp.zeros_like(vals)
        return [jnp.where(head_mask(rows, h), vals, zero) for h in range(2)]

    blocks = [None] + list(range(0, main, QBLK))

    def widths(t):
        return [(0, PAIR)] if blocks[t] is None else [(0, QBLK), (QBLK, QBLK)]

    def operands(t, rows_ref):
        if blocks[t] is None:
            parts = masked(rows_ref, main, SPEC_PAD)
            return [jnp.concatenate(parts + [jnp.zeros((PAIR - 2 * SPEC_PAD, PAIR), BF16)], axis=0)]
        return masked(rows_ref, blocks[t], QBLK)

    tops = {}

    def stage_scores(t):
        slot = t % 2
        tops[t] = []
        for (col, width), q_rows, d_rows in zip(widths(t), operands(t, q_s), operands(t, da_s)):
            s_val = dot_nt(k_s[...], q_rows)
            row = lax.broadcasted_iota(jnp.int32, (SPEC_PAD, width), 0)
            spec = jnp.where(row < n_spec, s_val[main:total], -jnp.inf)
            s_s[slot, 0:main, col:col + width] = s_val[0:main]
            s_s[slot, main:total, col:col + width] = spec
            tops[t].append(jnp.maximum(jnp.max(s_val[0:main], axis=0, keepdims=True), jnp.max(spec, axis=0, keepdims=True)))
            dp_s[slot, :, col:col + width] = dot_nt(v_s[...], d_rows).astype(BF16)

    def stage_softmax(t):
        slot = t % 2
        for (col, width), top in zip(widths(t), tops[t]):
            norm = jnp.zeros((8, width), F32)
            mix = jnp.zeros((8, width), F32)
            for r in range(0, total, chunk):
                e = jnp.exp(s_s[slot, r:r + chunk, col:col + width] - top)
                s_s[slot, r:r + chunk, col:col + width] = e
                ed = e * dp_s[slot, r:r + chunk, col:col + width].astype(F32)
                for g in range(0, chunk, 8):
                    norm = norm + e[g:g + 8]
                    mix = mix + ed[g:g + 8]
            inv = 1.0 / jnp.sum(norm, axis=0, keepdims=True)
            mix = jnp.sum(mix, axis=0, keepdims=True) * inv
            for r in range(0, total, chunk):
                prob = s_s[slot, r:r + chunk, col:col + width] * inv
                p_s[slot, r:r + chunk, col:col + width] = prob.astype(BF16)
                ds = prob * (dp_s[slot, r:r + chunk, col:col + width].astype(F32) - mix)
                ds_s[slot, r:r + chunk, col:col + width] = ds.astype(BF16)

    def emit_attn(start, vals):
        if start >= main:
            attn_own[patch:patch + SPEC_PAD, :] = vals
            attn_par[patch:patch + SPEC_PAD, :] = vals
        elif start < patch:
            attn_own[start:start + vals.shape[0], :] = vals
        elif start < 2 * patch:
            attn_par[start - patch:start - patch + vals.shape[0], :] = vals

    def stage_outputs(t):
        slot = t % 2
        span = sum(width for _, width in widths(t))
        for acc, vals, rows_ref, col in ((dv_s, p_s, da_s, 2 * PAIR), (dk_s, ds_s, q_s, PAIR)):
            part = dot_nn(vals[slot, :, 0:span], jnp.concatenate(operands(t, rows_ref), axis=0))
            if t == 0:
                acc[...] = part
            elif t < len(blocks) - 1:
                acc[...] += part
            else:
                dqkv_s[:, col:col + PAIR] = (acc[...] + part).astype(BF16)
        for kind, lhs, vals in ((0, vt_s, p_s), (1, kt_s, ds_s)):
            if blocks[t] is None:
                both = dot_nn(lhs[:, 0:total], vals[slot, :, 0:PAIR]).T
                rows = jnp.where(head_mask(SPEC_PAD, 0), both[0:SPEC_PAD], both[SPEC_PAD:2 * SPEC_PAD]).astype(BF16)
                if kind == 0:
                    emit_attn(main, rows)
                    padded = jnp.concatenate([rows, jnp.zeros((PAIR - SPEC_PAD, PAIR), BF16)], axis=0)
                    at_s[:, main:main + PAIR] = padded.T
                else:
                    dqkv_s[main:total, 0:PAIR] = rows
                continue
            both = jnp.concatenate(
                [dot_nn(lhs[h * HEAD_DIM:(h + 1) * HEAD_DIM, 0:total], vals[slot, :, h * QBLK:(h + 1) * QBLK])
                 for h in range(2)], axis=0)
            if kind == 0:
                at_s[:, blocks[t]:blocks[t] + QBLK] = both.astype(BF16)
            if kind == 1 or blocks[t] < 2 * patch:
                for c in range(0, QBLK, PAIR):
                    rows = both[:, c:c + PAIR].T.astype(BF16)
                    if kind == 0:
                        emit_attn(blocks[t] + c, rows)
                    else:
                        dqkv_s[blocks[t] + c:blocks[t] + c + PAIR, 0:PAIR] = rows

    steps = len(blocks)
    stage_scores(0)
    transpose_in()
    for t in range(steps + 1):
        if t + 1 < steps:
            stage_scores(t + 1)
        if t >= 1:
            stage_outputs(t - 1)
        if t < steps:
            stage_softmax(t)

    dqkv_own[0:patch, :] = dqkv_s[0:patch, :]
    dqkv_own[patch:patch + SPEC_PAD, :] = dqkv_s[main:total, :]
    dqkv_par[0:patch, :] = dqkv_s[patch:2 * patch, :]
    dqkv_par[patch:patch + SPEC_PAD, :] = dqkv_s[main:total, :]
    d_b = jnp.sum(dqkv_s[...].astype(F32).reshape(total // 8, 8, 3 * PAIR), axis=0)
    acc_out[3][...] = d_b if first else acc_in[3][...] + d_b
    d_w = dot_nn(normt_s[:, 0:total], dqkv_s[...])
    acc_out[0][...] = (d_w if first else acc_in[0][...].reshape(d_w.shape) + d_w).reshape(acc_out[0].shape)
    d_g = dot_nn(at_s[:, main:main + SPEC_PAD], dy_spc[...])
    for _, dy_ref, start, rows in pieces[:4]:
        d_g = d_g + dot_nn(at_s[:, start:start + rows], dy_ref[...])
    acc_out[1][...] = d_g if first else acc_in[1][...] + d_g
    gls = jnp.sum((wp_ref[...].astype(F32) * acc_out[1][...]).reshape(PAIR // 8, 8, d_g.shape[1]), axis=0)

    @pl.when(pair == 0)
    def _():
        acc_out[2][...] = gls

    @pl.when(pair != 0)
    def _():
        acc_out[2][...] += gls


def fused_block(image, core, rows, accs, vectors, w_qkv, b_qkv, w_proj, n_spec):
    patch, d_model = rows[2].shape
    half = d_model // 2
    pairs = half // PAIR
    total = 4 * patch + SPEC_PAD
    first = accs is None

    def stacked(count):
        return pl.BlockSpec((None, count, d_model), lambda j, c: (image, 0, 0))

    def column(count, third):
        return pl.BlockSpec((count, PAIR), lambda j, c: (0, (2 * third + c[0]) * pairs + j))

    whole = pl.BlockSpec((patch, d_model), lambda j, c: (0, 0))
    vec = pl.BlockSpec((1, d_model), lambda j, c: (0, 0))
    acc_specs = [
        pl.BlockSpec((d_model, 3 * PAIR), lambda j, c: (0, j)),
        pl.BlockSpec((PAIR, d_model), lambda j, c: (j, 0)),
        pl.BlockSpec((8, d_model), lambda j, c: (0, 0)),
        pl.BlockSpec((8, 3 * PAIR), lambda j, c: (0, j)),
        pl.BlockSpec((8, d_model), lambda j, c: (0, 0)),
    ]
    acc_shapes = [
        jax.ShapeDtypeStruct((d_model, 3 * half), F32),
        jax.ShapeDtypeStruct((half, d_model), F32),
        jax.ShapeDtypeStruct((8, d_model), F32),
        jax.ShapeDtypeStruct((8, 3 * half), F32),
        jax.ShapeDtypeStruct((8, d_model), F32),
    ]
    row_spec = [stacked(patch), stacked(patch), whole, whole, stacked(SPEC_PAD)]
    in_specs = row_spec * 2 + [vec] * 3 + [column(d_model, t) for t in range(3)] + [column(1, t) for t in range(3)] + [
        pl.BlockSpec((PAIR, d_model), lambda j, c: (c[0] * pairs + j, 0)),
    ] + ([] if first else acc_specs)
    flops = 2 * 6 * total * total * PAIR * pairs * 4
    outs = pl.pallas_call(
        functools.partial(block_kernel, n_spec, first),
        grid_spec=pltpu.PrefetchScalarGridSpec(
            num_scalar_prefetch=1, grid=(pairs,),
            in_specs=in_specs,
            out_specs=[
                pl.BlockSpec((patch + SPEC_PAD, PAIR), lambda j, c: (0, j)),
                pl.BlockSpec((patch + SPEC_PAD, PAIR), lambda j, c: (0, j)),
                pl.BlockSpec((patch + SPEC_PAD, 3 * PAIR), lambda j, c: (0, j)),
                pl.BlockSpec((patch + SPEC_PAD, 3 * PAIR), lambda j, c: (0, j)),
            ] + acc_specs,
            scratch_shapes=[pltpu.VMEM((total, d_model), BF16), pltpu.VMEM((d_model, total - SPEC_PAD + PAIR), BF16),
                            pltpu.VMEM((total, d_model), BF16)]
            + [pltpu.VMEM((total, PAIR), BF16)] * 4
            + [pltpu.VMEM((PAIR, total - SPEC_PAD + PAIR), BF16)] * 2
            + [pltpu.VMEM((2, total, 2 * QBLK), F32)]
            + [pltpu.VMEM((2, total, 2 * QBLK), BF16)] * 3
            + [pltpu.VMEM((total, PAIR), F32)] * 2
            + [pltpu.VMEM((PAIR, total - SPEC_PAD + PAIR), BF16), pltpu.VMEM((total, 3 * PAIR), BF16)]),
        out_shape=[jax.ShapeDtypeStruct((patch + SPEC_PAD, half), BF16)] * 2
        + [jax.ShapeDtypeStruct((patch + SPEC_PAD, 3 * half), BF16)] * 2 + acc_shapes,
        input_output_aliases={} if first else {21 + i: 4 + i for i in range(5)},
        cost_estimate=pl.CostEstimate(flops=flops, bytes_accessed=8 * total * half * 2,
                                      transcendentals=2 * pairs * total * total),
        compiler_params=pltpu.CompilerParams(vmem_limit_bytes=60 * 1024 * 1024),
        name="fused_block",
    )(core, *rows, *vectors, w_qkv, w_qkv, w_qkv, b_qkv, b_qkv, b_qkv, w_proj, *([] if first else accs))
    return outs[:4], outs[4:]


def place_columns(dst, src, pairs, half):
    for third in range(3):
        for pair in range(pairs):
            col = ((2 * third + half) * pairs + pair) * PAIR
            at = (pair * 3 + third) * PAIR
            dst[:, col:col + PAIR] = src[:, at:at + PAIR]


def finish_kernel(images, core_ref, *refs):
    per_image, refs = refs[:4 * images], refs[4 * images:]
    (x_ref, xs_ref, dy_ref, dys_ref, w_ref, wp_ref, ln_s, l_scale, b_proj,
     out_ref, outs_ref, dx_ref, dxs_ref, sums_ref, at_s, dq_s) = refs
    image = pl.program_id(0)
    half_cols = per_image[0].shape[1]
    pairs = half_cols // PAIR
    patch = x_ref.shape[0]
    for k in range(images):
        attn_own, attn_got, dqkv_own, dqkv_got = per_image[4 * k:4 * k + 4]
        for half in range(2):
            @pl.when(jnp.logical_and(image == k, core_ref[0] == half))
            def _():
                at_s[:, half * half_cols:(half + 1) * half_cols] = attn_own[...]
                at_s[:, (1 - half) * half_cols:(2 - half) * half_cols] = attn_got[...]
                place_columns(dq_s, dqkv_own, pairs, half)
                place_columns(dq_s, dqkv_got, pairs, 1 - half)

    @pl.when(image == 0)
    def _():
        sums_ref[...] = jnp.zeros_like(sums_ref)

    proj = dot_nn(at_s[...], wp_ref[...]) + b_proj[...]
    d_norm = dot_nt(dq_s[...], w_ref[...]).astype(BF16).astype(F32)
    n_out = outs_ref.shape[0]
    for slot, x_in, dy_in, start, rows in ((0, x_ref, dy_ref, 0, patch), (1, xs_ref, dys_ref, patch, SPEC_PAD)):
        x_float = x_in[...].astype(F32)
        out = (x_float + l_scale[...] * proj[start:start + rows]).astype(BF16)
        centered = x_float - jnp.mean(x_float, axis=-1, keepdims=True)
        inv_std = lax.rsqrt(jnp.mean(centered * centered, axis=-1, keepdims=True) + LN_EPS)
        x_hat = centered * inv_std
        grad = d_norm[start:start + rows]
        grad_hat = grad * ln_s[...]
        d_rows = inv_std * (grad_hat - jnp.mean(grad_hat, axis=-1, keepdims=True)
                            - x_hat * jnp.mean(grad_hat * x_hat, axis=-1, keepdims=True))
        dx = (dy_in[...].astype(F32) + d_rows).astype(BF16)
        if slot == 0:
            out_ref[...] = out
            dx_ref[...] = dx
        else:
            outs_ref[...] = out[0:n_out]
            dxs_ref[...] = dx[0:n_out]
        width = grad.shape[1]
        sums_ref[2 * slot] += jnp.sum((grad * x_hat).reshape(rows // 8, 8, width), axis=0)
        sums_ref[2 * slot + 1] += jnp.sum(grad.reshape(rows // 8, 8, width), axis=0)


def finish(core, per_image, x_patch, x_spec, dy_patch, dy_spec, w_qkv, w_proj, ln_scale, layer_scale, b_proj, n_spec):
    images, patch, d_model = x_patch.shape
    rows = patch + SPEC_PAD

    def const(shape):
        return pl.BlockSpec(shape, lambda i, c: (0,) * len(shape))

    def by_image(count):
        return pl.BlockSpec((None, count, d_model), lambda i, c: (i, 0, 0))

    flat = [arr for group in per_image for arr in group]
    return pl.pallas_call(
        functools.partial(finish_kernel, images),
        grid_spec=pltpu.PrefetchScalarGridSpec(
            num_scalar_prefetch=1, grid=(images,),
            in_specs=[const(arr.shape) for arr in flat]
            + [by_image(patch), by_image(SPEC_PAD), by_image(patch), by_image(SPEC_PAD),
               const(w_qkv.shape), const(w_proj.shape), const((1, d_model)), const((1, d_model)), const((1, d_model))],
            out_specs=[by_image(patch), by_image(n_spec), by_image(patch), by_image(n_spec), const((4, 8, d_model))],
            scratch_shapes=[pltpu.VMEM((rows, d_model), BF16), pltpu.VMEM((rows, 3 * d_model), BF16)]),
        out_shape=[jax.ShapeDtypeStruct((images, patch, d_model), BF16), jax.ShapeDtypeStruct((images, n_spec, d_model), BF16),
                   jax.ShapeDtypeStruct((images, patch, d_model), BF16), jax.ShapeDtypeStruct((images, n_spec, d_model), BF16),
                   jax.ShapeDtypeStruct((4, 8, d_model), F32)],
        cost_estimate=pl.CostEstimate(flops=8 * images * rows * d_model * d_model, bytes_accessed=20 << 20, transcendentals=0),
        compiler_params=pltpu.CompilerParams(vmem_limit_bytes=56 * 1024 * 1024),
        name="finish",
    )(core, *flat, x_patch, x_spec, dy_patch, dy_spec, w_qkv, w_proj, ln_scale, layer_scale, b_proj)


def merge_kernel(core_ref, w_own, w_got, g_own, g_got, db_own, db_got, ds_own, ds_got, d_dy, l_scale, b_proj,
                 w_out, g_out, db_out, dbp_out, dls_out):
    pairs = w_own.shape[1] // (3 * PAIR)
    step = pl.program_id(0)
    count = pl.num_programs(0) // 2
    for half in range(2):
        @pl.when(core_ref[0] == half)
        def _():
            place_columns(w_out, w_own, pairs, half)
            place_columns(w_out, w_got, pairs, 1 - half)

    @pl.when(step // count == core_ref[0])
    def _():
        g_out[...] = g_own[...] * l_scale[...]

    @pl.when(step // count != core_ref[0])
    def _():
        g_out[...] = g_got[...] * l_scale[...]

    @pl.when(step == 0)
    def _():
        total_dy = jnp.sum(d_dy[...], axis=0, keepdims=True)
        dbp_out[...] = total_dy * l_scale[...]
        dls_out[...] = jnp.sum(ds_own[...] + ds_got[...], axis=0, keepdims=True) + b_proj[...] * total_dy
        own = jnp.sum(db_own[...], axis=0, keepdims=True)
        got = jnp.sum(db_got[...], axis=0, keepdims=True)
        for half in range(2):
            @pl.when(core_ref[0] == half)
            def _():
                place_columns(db_out, own, pairs, half)
                place_columns(db_out, got, pairs, 1 - half)


def merge_grads(core, w_own, w_got, g_own, g_got, db_own, db_got, ds_own, ds_got, d_dy, layer_scale, b_proj):
    rows, cols = w_own.shape
    half, d_model = g_own.shape
    tile = PAIR
    count = half // tile

    def const(shape):
        return pl.BlockSpec(shape, lambda g, c: (0,) * len(shape))

    small = (db_own, db_got, ds_own, ds_got, d_dy, layer_scale, b_proj)
    return pl.pallas_call(
        merge_kernel,
        grid_spec=pltpu.PrefetchScalarGridSpec(
            num_scalar_prefetch=1, grid=(2 * count,),
            in_specs=[pl.BlockSpec((tile, cols), lambda g, c: (g, 0))] * 2
            + [pl.BlockSpec((tile, d_model), lambda g, c: (g % count, 0))] * 2
            + [const(arr.shape) for arr in small],
            out_specs=[pl.BlockSpec((tile, 2 * cols), lambda g, c: (g, 0)),
                       pl.BlockSpec((tile, d_model), lambda g, c: (g, 0)),
                       const((1, 2 * cols)), const((1, d_model)), const((1, d_model))]),
        out_shape=[jax.ShapeDtypeStruct((rows, 2 * cols), F32), jax.ShapeDtypeStruct((2 * half, d_model), F32),
                   jax.ShapeDtypeStruct((1, 2 * cols), F32), jax.ShapeDtypeStruct((1, d_model), F32),
                   jax.ShapeDtypeStruct((1, d_model), F32)],
        cost_estimate=pl.CostEstimate(flops=rows * cols * 256, bytes_accessed=20 << 20, transcendentals=0),
        name="merge_grads",
    )(core, w_own, w_got, g_own, g_got, *small)


def solution(mesh):
    group_size = mesh.shape['sp']
    partner = [(i, i ^ 1) for i in range(group_size)]
    opposite = [(i, i ^ 2) for i in range(group_size)]

    def swap(vals):
        return lax.ppermute(vals, 'sp', partner)

    def cross(vals):
        return lax.ppermute(vals, 'sp', opposite)

    def run_block(x_special, x_patch, dy_special, dy_patch, ln_scale, ln_bias, w_qkv, b_qkv, w_proj, b_proj, layer_scale):
        num_images, n_spec, _ = x_special.shape
        core = (lax.axis_index('sp') % 2).reshape(1).astype(jnp.int32)

        across = [(cross(x_patch[i]), cross(dy_patch[i])) for i in range(num_images)]
        x_partner, dy_partner = swap(x_patch), swap(dy_patch)

        pad = ((0, 0), (0, SPEC_PAD - n_spec), (0, 0))
        x_spec = jnp.pad(x_special, pad)
        dy_spec = jnp.pad(dy_special, pad)
        ln_scale, ln_bias, layer_scale, b_proj, b_qkv = (v[None] for v in (ln_scale, ln_bias, layer_scale, b_proj, b_qkv))

        per_image = []
        relays = {}
        accs = None

        def gate(vals, image):
            if image < 0:
                return vals
            return lax.optimization_barrier((vals, per_image[image][0]))[0]

        def relay_image(image, after):
            across[image] = gate(across[image], after)
            relays[image] = (swap(across[image][0]), swap(across[image][1]))

        relay_image(0, -1)
        for i in range(num_images):
            near, relay = gate((across[i], relays[i]), i - 1)
            rows = (x_patch, x_partner, near[0], relay[0], x_spec, dy_patch, dy_partner, near[1], relay[1], dy_spec)
            (attn_own, attn_par, dqkv_own, dqkv_par), accs = fused_block(
                i, core, rows, accs, (ln_scale, ln_bias, layer_scale), w_qkv, b_qkv, w_proj, n_spec)
            per_image.append((attn_own, swap(attn_par), dqkv_own, swap(dqkv_par)))
            for image in range(i + 1, num_images):
                if image not in relays and (image <= i + 2):
                    relay_image(image, i)

        d_w, d_g, d_scale, d_b, d_dy = accs
        got = [swap(vals) for vals in (d_w, d_g, d_b, d_scale)]
        out_patch, out_special, dx_patch, dx_special, sums = finish(
            core, per_image, x_patch, x_spec, dy_patch, dy_spec, w_qkv, w_proj, ln_scale, layer_scale, b_proj, n_spec)
        sums = jnp.sum(sums, axis=1)
        ln_grads = sums[:2] + cross(sums[:2])
        ln_grads = ln_grads + swap(ln_grads) + sums[2:]
        d_w_qkv, d_w_proj, d_b_qkv, d_b_proj, d_layer_scale = merge_grads(
            core, d_w, got[0], d_g, got[1], d_b, got[2], d_scale, got[3], d_dy, layer_scale, b_proj)
        return (out_special, out_patch, dx_special, dx_patch, ln_grads[0], ln_grads[1],
                d_w_qkv, d_b_qkv[0], d_w_proj, d_b_proj[0], d_layer_scale[0])

    part_rows = P('dp')
    part_seq = P('dp', 'sp')
    replicated = P()
    return jax.shard_map(
        run_block, mesh=mesh,
        in_specs=(part_rows, part_seq, part_rows, part_seq, replicated, replicated, replicated, replicated, replicated, replicated, replicated),
        out_specs=(part_rows, part_seq, part_rows, part_seq, part_rows, part_rows, part_rows, part_rows, part_rows, part_rows, part_rows),
        check_vma=False)
```

```python
import functools

import jax
import jax.numpy as jnp
from jax import lax
from jax.experimental import pallas as pl
from jax.experimental.pallas import tpu as pltpu
from jax.sharding import PartitionSpec as P


HEAD_DIM = 64
PAIR = 2 * HEAD_DIM
LN_EPS = 1e-6
ATTN_SCALE = HEAD_DIM ** -0.5
SPEC_PAD = 16
QBLK = 256
F32 = jnp.float32
BF16 = jnp.bfloat16


def dot_nt(a, b):
    return lax.dot_general(a, b, (((1,), (1,)), ((), ())), preferred_element_type=F32)


def dot_nn(a, b):
    return lax.dot_general(a, b, (((1,), (0,)), ((), ())), preferred_element_type=F32)


def block_kernel(n_spec, first, core_ref, *refs):
    (x_own, x_par, x_acr, x_rel, x_spc, dy_own, dy_par, dy_acr, dy_rel, dy_spc,
     ln_s, ln_b, l_scale, wq_ref, wk_ref, wv_ref, bq_ref, bk_ref, bv_ref, wp_ref) = refs[:20]
    refs = refs[20:]
    if first:
        acc_in = None
    else:
        acc_in, refs = refs[:5], refs[5:]
    attn_own, attn_par, dqkv_own, dqkv_par = refs[:4]
    acc_out, refs = refs[4:9], refs[9:]
    (norm_s, normt_s, dproj_s, q_s, k_s, v_s, da_s, vt_s, kt_s, s_s, dp_s, p_s, ds_s, dv_s, dk_s, at_s, dqkv_s) = refs
    patch = x_own.shape[-2]
    main = 4 * patch
    total = main + SPEC_PAD
    chunk = 80
    pair = pl.program_id(0)
    pieces = [(x_own, dy_own, 0, patch), (x_par, dy_par, patch, patch), (x_acr, dy_acr, 2 * patch, patch),
              (x_rel, dy_rel, 3 * patch, patch), (x_spc, dy_spc, main, SPEC_PAD)]

    @pl.when(pair == 0)
    def _():
        for x_ref, dy_ref, start, rows in pieces:
            step = min(rows, 64)

            @pl.loop(0, rows // step)
            def _(i):
                src = pl.ds(pl.multiple_of(i * step, step), step)
                dst = pl.ds(pl.multiple_of(start + i * step, step), step)
                x_float = x_ref[src, :].astype(F32)
                centered = x_float - jnp.mean(x_float, axis=-1, keepdims=True)
                inv_std = lax.rsqrt(jnp.mean(centered * centered, axis=-1, keepdims=True) + LN_EPS)
                norm_s[dst, :] = (centered * inv_std * ln_s[...] + ln_b[...]).astype(BF16)
                dproj_s[dst, :] = (dy_ref[src, :].astype(F32) * l_scale[...]).astype(BF16)

        width = norm_s.shape[1]

        @pl.loop(0, main // PAIR)
        def _(i):
            rows = pl.ds(pl.multiple_of(i * PAIR, PAIR), PAIR)
            for c in range(0, width, PAIR):
                normt_s[c:c + PAIR, rows] = norm_s[rows, c:c + PAIR].T

        for c in range(0, width, PAIR):
            tail = jnp.concatenate([norm_s[main:total, c:c + PAIR], jnp.zeros((PAIR - SPEC_PAD, PAIR), BF16)], axis=0)
            normt_s[c:c + PAIR, main:main + PAIR] = tail.T

        d_dy = jnp.zeros(acc_out[4].shape, F32)
        for _, dy_ref, _, rows in pieces:
            d_dy = d_dy + jnp.sum(dy_ref[...].astype(F32).reshape(rows // 8, 8, dy_ref.shape[-1]), axis=0)
        acc_out[4][...] = d_dy if first else acc_in[4][...] + d_dy

    scale = jnp.asarray(ATTN_SCALE, BF16)
    w_pair = jnp.concatenate([wq_ref[...], wk_ref[...], wv_ref[...]], axis=1)
    qkv = dot_nn(norm_s[...], w_pair) + jnp.concatenate([bq_ref[...], bk_ref[...], bv_ref[...]], axis=1)
    q_s[...] = qkv[:, 0:PAIR].astype(BF16) * scale
    k_s[...] = qkv[:, PAIR:2 * PAIR].astype(BF16)
    v_s[...] = qkv[:, 2 * PAIR:3 * PAIR].astype(BF16)
    da_s[...] = dot_nt(dproj_s[...], wp_ref[...]).astype(BF16)

    def transpose_in():
        for dst, src, mult in ((vt_s, v_s, None), (kt_s, k_s, scale)):
            for row in range(0, main, PAIR):
                vals = src[row:row + PAIR, :]
                dst[:, row:row + PAIR] = (vals if mult is None else vals * mult).T
            vals = src[main:total, :]
            tail = jnp.concatenate([vals if mult is None else vals * mult,
                                    jnp.zeros((PAIR - SPEC_PAD, PAIR), BF16)], axis=0)
            dst[:, main:main + PAIR] = tail.T

    def head_mask(rows, head):
        lane = lax.broadcasted_iota(jnp.int32, (rows, PAIR), 1)
        return (lane < HEAD_DIM) if head == 0 else (lane >= HEAD_DIM)

    def masked(rows_ref, start, rows):
        vals = rows_ref[start:start + rows, :]
        zero = jnp.zeros_like(vals)
        return [jnp.where(head_mask(rows, h), vals, zero) for h in range(2)]

    blocks = [None] + list(range(0, main, QBLK))

    def widths(t):
        return [(0, PAIR)] if blocks[t] is None else [(0, QBLK), (QBLK, QBLK)]

    def operands(t, rows_ref):
        if blocks[t] is None:
            parts = masked(rows_ref, main, SPEC_PAD)
            return [jnp.concatenate(parts + [jnp.zeros((PAIR - 2 * SPEC_PAD, PAIR), BF16)], axis=0)]
        return masked(rows_ref, blocks[t], QBLK)

    tops = {}

    def stage_scores(t):
        slot = t % 2
        tops[t] = []
        for (col, width), q_rows in zip(widths(t), operands(t, q_s)):
            s_val = dot_nt(k_s[...], q_rows)
            row = lax.broadcasted_iota(jnp.int32, (SPEC_PAD, width), 0)
            spec = jnp.where(row < n_spec, s_val[main:total], -jnp.inf)
            s_s[slot, 0:main, col:col + width] = s_val[0:main]
            s_s[slot, main:total, col:col + width] = spec
            tops[t].append(jnp.maximum(jnp.max(s_val[0:main], axis=0, keepdims=True), jnp.max(spec, axis=0, keepdims=True)))
        for (col, width), d_rows in zip(widths(t), operands(t, da_s)):
            dp_s[slot, :, col:col + width] = dot_nt(v_s[...], d_rows).astype(BF16)

    def stage_softmax(t):
        slot = t % 2
        for (col, width), top in zip(widths(t), tops[t]):
            norm = jnp.zeros((8, width), F32)
            mix = jnp.zeros((8, width), F32)
            for r in range(0, total, chunk):
                e = jnp.exp(s_s[slot, r:r + chunk, col:col + width] - top)
                s_s[slot, r:r + chunk, col:col + width] = e
                ed = e * dp_s[slot, r:r + chunk, col:col + width].astype(F32)
                for g in range(0, chunk, 8):
                    norm = norm + e[g:g + 8]
                    mix = mix + ed[g:g + 8]
            inv = 1.0 / jnp.sum(norm, axis=0, keepdims=True)
            mix = jnp.sum(mix, axis=0, keepdims=True) * inv
            for r in range(0, total, chunk):
                prob = s_s[slot, r:r + chunk, col:col + width] * inv
                p_s[slot, r:r + chunk, col:col + width] = prob.astype(BF16)
                ds = prob * (dp_s[slot, r:r + chunk, col:col + width].astype(F32) - mix)
                ds_s[slot, r:r + chunk, col:col + width] = ds.astype(BF16)

    def emit_attn(start, vals):
        if start >= main:
            attn_own[patch:patch + SPEC_PAD, :] = vals
            attn_par[patch:patch + SPEC_PAD, :] = vals
        elif start < patch:
            attn_own[start:start + vals.shape[0], :] = vals
        elif start < 2 * patch:
            attn_par[start - patch:start - patch + vals.shape[0], :] = vals

    def stage_outputs(t):
        slot = t % 2
        span = sum(width for _, width in widths(t))
        for acc, vals, rows_ref, col in ((dv_s, p_s, da_s, 2 * PAIR), (dk_s, ds_s, q_s, PAIR)):
            part = dot_nn(vals[slot, :, 0:span], jnp.concatenate(operands(t, rows_ref), axis=0))
            if t == 0:
                acc[...] = part
            elif t < len(blocks) - 1:
                acc[...] += part
            else:
                dqkv_s[:, col:col + PAIR] = (acc[...] + part).astype(BF16)
        for kind, lhs, vals in ((0, vt_s, p_s), (1, kt_s, ds_s)):
            if blocks[t] is None:
                both = dot_nn(lhs[:, 0:total], vals[slot, :, 0:PAIR]).T
                rows = jnp.where(head_mask(SPEC_PAD, 0), both[0:SPEC_PAD], both[SPEC_PAD:2 * SPEC_PAD]).astype(BF16)
                if kind == 0:
                    emit_attn(main, rows)
                    padded = jnp.concatenate([rows, jnp.zeros((PAIR - SPEC_PAD, PAIR), BF16)], axis=0)
                    at_s[:, main:main + PAIR] = padded.T
                else:
                    dqkv_s[main:total, 0:PAIR] = rows
                continue
            both = jnp.concatenate(
                [dot_nn(lhs[h * HEAD_DIM:(h + 1) * HEAD_DIM, 0:total], vals[slot, :, h * QBLK:(h + 1) * QBLK])
                 for h in range(2)], axis=0)
            if kind == 0:
                at_s[:, blocks[t]:blocks[t] + QBLK] = both.astype(BF16)
            if kind == 1 or blocks[t] < 2 * patch:
                for c in range(0, QBLK, PAIR):
                    rows = both[:, c:c + PAIR].T.astype(BF16)
                    if kind == 0:
                        emit_attn(blocks[t] + c, rows)
                    else:
                        dqkv_s[blocks[t] + c:blocks[t] + c + PAIR, 0:PAIR] = rows

    steps = len(blocks)
    stage_scores(0)
    transpose_in()
    for t in range(steps + 1):
        if t + 1 < steps:
            stage_scores(t + 1)
        if t >= 1:
            stage_outputs(t - 1)
        if t < steps:
            stage_softmax(t)

    dqkv_own[0:patch, :] = dqkv_s[0:patch, :]
    dqkv_own[patch:patch + SPEC_PAD, :] = dqkv_s[main:total, :]
    dqkv_par[0:patch, :] = dqkv_s[patch:2 * patch, :]
    dqkv_par[patch:patch + SPEC_PAD, :] = dqkv_s[main:total, :]
    d_b = jnp.sum(dqkv_s[...].astype(F32).reshape(total // 8, 8, 3 * PAIR), axis=0)
    acc_out[3][...] = d_b if first else acc_in[3][...] + d_b
    d_w = dot_nn(normt_s[:, 0:total], dqkv_s[...])
    acc_out[0][...] = (d_w if first else acc_in[0][...].reshape(d_w.shape) + d_w).reshape(acc_out[0].shape)
    d_g = dot_nn(at_s[:, main:main + SPEC_PAD], dy_spc[...])
    for _, dy_ref, start, rows in pieces[:4]:
        d_g = d_g + dot_nn(at_s[:, start:start + rows], dy_ref[...])
    acc_out[1][...] = d_g if first else acc_in[1][...] + d_g
    gls = jnp.sum((wp_ref[...].astype(F32) * acc_out[1][...]).reshape(PAIR // 8, 8, d_g.shape[1]), axis=0)

    @pl.when(pair == 0)
    def _():
        acc_out[2][...] = gls

    @pl.when(pair != 0)
    def _():
        acc_out[2][...] += gls


def fused_block(image, core, rows, accs, vectors, w_qkv, b_qkv, w_proj, n_spec):
    patch, d_model = rows[2].shape
    half = d_model // 2
    pairs = half // PAIR
    total = 4 * patch + SPEC_PAD
    first = accs is None

    def stacked(count):
        return pl.BlockSpec((None, count, d_model), lambda j, c: (image, 0, 0))

    def column(count, third):
        return pl.BlockSpec((count, PAIR), lambda j, c: (0, (2 * third + c[0]) * pairs + j))

    whole = pl.BlockSpec((patch, d_model), lambda j, c: (0, 0))
    vec = pl.BlockSpec((1, d_model), lambda j, c: (0, 0))
    acc_specs = [
        pl.BlockSpec((d_model, 3 * PAIR), lambda j, c: (0, j)),
        pl.BlockSpec((PAIR, d_model), lambda j, c: (j, 0)),
        pl.BlockSpec((8, d_model), lambda j, c: (0, 0)),
        pl.BlockSpec((8, 3 * PAIR), lambda j, c: (0, j)),
        pl.BlockSpec((8, d_model), lambda j, c: (0, 0)),
    ]
    acc_shapes = [
        jax.ShapeDtypeStruct((d_model, 3 * half), F32),
        jax.ShapeDtypeStruct((half, d_model), F32),
        jax.ShapeDtypeStruct((8, d_model), F32),
        jax.ShapeDtypeStruct((8, 3 * half), F32),
        jax.ShapeDtypeStruct((8, d_model), F32),
    ]
    row_spec = [stacked(patch), stacked(patch), whole, whole, stacked(SPEC_PAD)]
    in_specs = row_spec * 2 + [vec] * 3 + [column(d_model, t) for t in range(3)] + [column(1, t) for t in range(3)] + [
        pl.BlockSpec((PAIR, d_model), lambda j, c: (c[0] * pairs + j, 0)),
    ] + ([] if first else acc_specs)
    flops = 2 * 6 * total * total * PAIR * pairs * 4
    outs = pl.pallas_call(
        functools.partial(block_kernel, n_spec, first),
        grid_spec=pltpu.PrefetchScalarGridSpec(
            num_scalar_prefetch=1, grid=(pairs,),
            in_specs=in_specs,
            out_specs=[
                pl.BlockSpec((patch + SPEC_PAD, PAIR), lambda j, c: (0, j)),
                pl.BlockSpec((patch + SPEC_PAD, PAIR), lambda j, c: (0, j)),
                pl.BlockSpec((patch + SPEC_PAD, 3 * PAIR), lambda j, c: (0, j)),
                pl.BlockSpec((patch + SPEC_PAD, 3 * PAIR), lambda j, c: (0, j)),
            ] + acc_specs,
            scratch_shapes=[pltpu.VMEM((total, d_model), BF16), pltpu.VMEM((d_model, total - SPEC_PAD + PAIR), BF16),
                            pltpu.VMEM((total, d_model), BF16)]
            + [pltpu.VMEM((total, PAIR), BF16)] * 4
            + [pltpu.VMEM((PAIR, total - SPEC_PAD + PAIR), BF16)] * 2
            + [pltpu.VMEM((2, total, 2 * QBLK), F32)]
            + [pltpu.VMEM((2, total, 2 * QBLK), BF16)] * 3
            + [pltpu.VMEM((total, PAIR), F32)] * 2
            + [pltpu.VMEM((PAIR, total - SPEC_PAD + PAIR), BF16), pltpu.VMEM((total, 3 * PAIR), BF16)]),
        out_shape=[jax.ShapeDtypeStruct((patch + SPEC_PAD, half), BF16)] * 2
        + [jax.ShapeDtypeStruct((patch + SPEC_PAD, 3 * half), BF16)] * 2 + acc_shapes,
        input_output_aliases={} if first else {21 + i: 4 + i for i in range(5)},
        cost_estimate=pl.CostEstimate(flops=flops, bytes_accessed=8 * total * half * 2,
                                      transcendentals=2 * pairs * total * total),
        compiler_params=pltpu.CompilerParams(vmem_limit_bytes=60 * 1024 * 1024),
        name="fused_block",
    )(core, *rows, *vectors, w_qkv, w_qkv, w_qkv, b_qkv, b_qkv, b_qkv, w_proj, *([] if first else accs))
    return outs[:4], outs[4:]


def place_columns(dst, src, pairs, half):
    for third in range(3):
        for pair in range(pairs):
            col = ((2 * third + half) * pairs + pair) * PAIR
            at = (pair * 3 + third) * PAIR
            dst[..., col:col + PAIR] = src[..., at:at + PAIR]


def finish_kernel(images, core_ref, *refs):
    per_image, refs = refs[:4 * images], refs[4 * images:]
    (x_ref, xs_ref, dy_ref, dys_ref, w_ref, wp_ref, ln_s, l_scale, b_proj,
     out_ref, outs_ref, dx_ref, dxs_ref, sums_ref, at_s, dq_s) = refs
    image = pl.program_id(0)
    half_cols = per_image[0].shape[1]
    pairs = half_cols // PAIR
    patch = x_ref.shape[0]
    for k in range(images):
        attn_own, attn_got, dqkv_own, dqkv_got = per_image[4 * k:4 * k + 4]
        for half in range(2):
            @pl.when(jnp.logical_and(image == k, core_ref[0] == half))
            def _():
                at_s[:, half * half_cols:(half + 1) * half_cols] = attn_own[...]
                at_s[:, (1 - half) * half_cols:(2 - half) * half_cols] = attn_got[...]
                place_columns(dq_s, dqkv_own, pairs, half)
                place_columns(dq_s, dqkv_got, pairs, 1 - half)

    @pl.when(image == 0)
    def _():
        sums_ref[...] = jnp.zeros_like(sums_ref)

    proj = dot_nn(at_s[...], wp_ref[...]) + b_proj[...]
    d_norm = dot_nt(dq_s[...], w_ref[...]).astype(BF16).astype(F32)
    n_out = outs_ref.shape[0]
    for slot, x_in, dy_in, start, rows in ((0, x_ref, dy_ref, 0, patch), (1, xs_ref, dys_ref, patch, SPEC_PAD)):
        x_float = x_in[...].astype(F32)
        out = (x_float + l_scale[...] * proj[start:start + rows]).astype(BF16)
        centered = x_float - jnp.mean(x_float, axis=-1, keepdims=True)
        inv_std = lax.rsqrt(jnp.mean(centered * centered, axis=-1, keepdims=True) + LN_EPS)
        x_hat = centered * inv_std
        grad = d_norm[start:start + rows]
        grad_hat = grad * ln_s[...]
        d_rows = inv_std * (grad_hat - jnp.mean(grad_hat, axis=-1, keepdims=True)
                            - x_hat * jnp.mean(grad_hat * x_hat, axis=-1, keepdims=True))
        dx = (dy_in[...].astype(F32) + d_rows).astype(BF16)
        if slot == 0:
            out_ref[...] = out
            dx_ref[...] = dx
        else:
            outs_ref[...] = out[0:n_out]
            dxs_ref[...] = dx[0:n_out]
        width = grad.shape[1]
        sums_ref[2 * slot] += jnp.sum((grad * x_hat).reshape(rows // 8, 8, width), axis=0)
        sums_ref[2 * slot + 1] += jnp.sum(grad.reshape(rows // 8, 8, width), axis=0)


def finish(core, per_image, x_patch, x_spec, dy_patch, dy_spec, w_qkv, w_proj, ln_scale, layer_scale, b_proj, n_spec):
    images, patch, d_model = x_patch.shape
    rows = patch + SPEC_PAD

    def const(shape):
        return pl.BlockSpec(shape, lambda i, c: (0,) * len(shape))

    def by_image(count):
        return pl.BlockSpec((None, count, d_model), lambda i, c: (i, 0, 0))

    flat = [arr for group in per_image for arr in group]
    return pl.pallas_call(
        functools.partial(finish_kernel, images),
        grid_spec=pltpu.PrefetchScalarGridSpec(
            num_scalar_prefetch=1, grid=(images,),
            in_specs=[const(arr.shape) for arr in flat]
            + [by_image(patch), by_image(SPEC_PAD), by_image(patch), by_image(SPEC_PAD),
               const(w_qkv.shape), const(w_proj.shape), const((1, d_model)), const((1, d_model)), const((1, d_model))],
            out_specs=[by_image(patch), by_image(n_spec), by_image(patch), by_image(n_spec), const((4, 8, d_model))],
            scratch_shapes=[pltpu.VMEM((rows, d_model), BF16), pltpu.VMEM((rows, 3 * d_model), BF16)]),
        out_shape=[jax.ShapeDtypeStruct((images, patch, d_model), BF16), jax.ShapeDtypeStruct((images, n_spec, d_model), BF16),
                   jax.ShapeDtypeStruct((images, patch, d_model), BF16), jax.ShapeDtypeStruct((images, n_spec, d_model), BF16),
                   jax.ShapeDtypeStruct((4, 8, d_model), F32)],
        cost_estimate=pl.CostEstimate(flops=8 * images * rows * d_model * d_model, bytes_accessed=20 << 20, transcendentals=0),
        compiler_params=pltpu.CompilerParams(vmem_limit_bytes=56 * 1024 * 1024),
        name="finish",
    )(core, *flat, x_patch, x_spec, dy_patch, dy_spec, w_qkv, w_proj, ln_scale, layer_scale, b_proj)


def merge_kernel(core_ref, w_own, w_got, g_own, g_got, db_own, db_got, ds_own, ds_got, d_dy, l_scale, b_proj,
                 w_out, g_out, db_out, dbp_out, dls_out):
    pairs = w_own.shape[1] // (3 * PAIR)
    step = pl.program_id(0)
    count = pl.num_programs(0) // 2
    for half in range(2):
        @pl.when(core_ref[0] == half)
        def _():
            place_columns(w_out, w_own, pairs, half)
            place_columns(w_out, w_got, pairs, 1 - half)

    @pl.when(step // count == core_ref[0])
    def _():
        g_out[...] = g_own[...] * l_scale[...]

    @pl.when(step // count != core_ref[0])
    def _():
        g_out[...] = g_got[...] * l_scale[...]

    @pl.when(step == 0)
    def _():
        total_dy = jnp.sum(d_dy[...], axis=0)
        dbp_out[...] = total_dy * l_scale[0]
        dls_out[...] = jnp.sum(ds_own[...] + ds_got[...], axis=0) + b_proj[0] * total_dy
        own = jnp.sum(db_own[...], axis=0)
        got = jnp.sum(db_got[...], axis=0)
        for half in range(2):
            @pl.when(core_ref[0] == half)
            def _():
                place_columns(db_out, own, pairs, half)
                place_columns(db_out, got, pairs, 1 - half)


def merge_grads(core, w_own, w_got, g_own, g_got, db_own, db_got, ds_own, ds_got, d_dy, layer_scale, b_proj):
    rows, cols = w_own.shape
    half, d_model = g_own.shape
    tile = PAIR
    count = half // tile

    def const(shape):
        return pl.BlockSpec(shape, lambda g, c: (0,) * len(shape))

    small = (db_own, db_got, ds_own, ds_got, d_dy, layer_scale, b_proj)
    return pl.pallas_call(
        merge_kernel,
        grid_spec=pltpu.PrefetchScalarGridSpec(
            num_scalar_prefetch=1, grid=(2 * count,),
            in_specs=[pl.BlockSpec((tile, cols), lambda g, c: (g, 0))] * 2
            + [pl.BlockSpec((tile, d_model), lambda g, c: (g % count, 0))] * 2
            + [const(arr.shape) for arr in small],
            out_specs=[pl.BlockSpec((tile, 2 * cols), lambda g, c: (g, 0)),
                       pl.BlockSpec((tile, d_model), lambda g, c: (g, 0)),
                       const((2 * cols,)), const((d_model,)), const((d_model,))]),
        out_shape=[jax.ShapeDtypeStruct((rows, 2 * cols), F32), jax.ShapeDtypeStruct((2 * half, d_model), F32),
                   jax.ShapeDtypeStruct((2 * cols,), F32), jax.ShapeDtypeStruct((d_model,), F32),
                   jax.ShapeDtypeStruct((d_model,), F32)],
        cost_estimate=pl.CostEstimate(flops=rows * cols * 256, bytes_accessed=20 << 20, transcendentals=0),
        name="merge_grads",
    )(core, w_own, w_got, g_own, g_got, *small)


def solution(mesh):
    group_size = mesh.shape['sp']
    partner = [(i, i ^ 1) for i in range(group_size)]
    opposite = [(i, i ^ 2) for i in range(group_size)]

    diagonal = [(i, i ^ 3) for i in range(group_size)]

    def swap(vals):
        return lax.ppermute(vals, 'sp', partner)

    def cross(vals):
        return lax.ppermute(vals, 'sp', opposite)

    def run_block(x_special, x_patch, dy_special, dy_patch, ln_scale, ln_bias, w_qkv, b_qkv, w_proj, b_proj, layer_scale):
        num_images, n_spec, _ = x_special.shape
        core = (lax.axis_index('sp') % 2).reshape(1).astype(jnp.int32)

        across = [(cross(x_patch[i]), cross(dy_patch[i])) for i in range(num_images)]
        x_partner, dy_partner = swap(x_patch), swap(dy_patch)

        pad = ((0, 0), (0, SPEC_PAD - n_spec), (0, 0))
        x_spec = jnp.pad(x_special, pad)
        dy_spec = jnp.pad(dy_special, pad)
        ln_scale, ln_bias, layer_scale, b_proj, b_qkv = (
            v.reshape(1, -1) for v in (ln_scale, ln_bias, layer_scale, b_proj, b_qkv))

        per_image = []
        relays = {}
        accs = None

        def gate(vals, image):
            if image < 0:
                return vals
            return lax.optimization_barrier((vals, per_image[image][0]))[0]

        def relay_image(image, after):
            across[image] = gate(across[image], after)
            relays[image] = (swap(across[image][0]), swap(across[image][1]))

        relay_image(0, -1)
        for i in range(num_images):
            near, relay = gate((across[i], relays[i]), i - 1)
            rows = (x_patch, x_partner, near[0], relay[0], x_spec, dy_patch, dy_partner, near[1], relay[1], dy_spec)
            (attn_own, attn_par, dqkv_own, dqkv_par), accs = fused_block(
                i, core, rows, accs, (ln_scale, ln_bias, layer_scale), w_qkv, b_qkv, w_proj, n_spec)
            per_image.append((attn_own, swap(attn_par), dqkv_own, swap(dqkv_par)))
            for image in range(i + 1, num_images):
                if image not in relays and (image <= i + 2):
                    relay_image(image, i)

        d_w, d_g, d_scale, d_b, d_dy = accs
        got = [swap(vals) for vals in (d_w, d_g, d_b, d_scale)]
        out_patch, out_special, dx_patch, dx_special, sums = finish(
            core, per_image, x_patch, x_spec, dy_patch, dy_spec, w_qkv, w_proj, ln_scale, layer_scale, b_proj, n_spec)
        sums = jnp.sum(sums, axis=1)
        near, far, diag = swap(sums[:2]), cross(sums[:2]), lax.ppermute(sums[:2], 'sp', diagonal)
        ln_grads = (sums[:2] + near) + (far + diag) + sums[2:]
        d_w_qkv, d_w_proj, d_b_qkv, d_b_proj, d_layer_scale = merge_grads(
            core, d_w, got[0], d_g, got[1], d_b, got[2], d_scale, got[3], d_dy, layer_scale, b_proj)
        return (out_special, out_patch, dx_special, dx_patch, ln_grads[0], ln_grads[1],
                d_w_qkv, d_b_qkv, d_w_proj, d_b_proj, d_layer_scale)

    part_rows = P('dp')
    part_seq = P('dp', 'sp')
    replicated = P()
    return jax.shard_map(
        run_block, mesh=mesh,
        in_specs=(part_rows, part_seq, part_rows, part_seq, replicated, replicated, replicated, replicated, replicated, replicated, replicated),
        out_specs=(part_rows, part_seq, part_rows, part_seq, part_rows, part_rows, part_rows, part_rows, part_rows, part_rows, part_rows),
        check_vma=False)
```

```python
import functools

import jax
import jax.numpy as jnp
from jax import lax
from jax.experimental import pallas as pl
from jax.experimental.pallas import tpu as pltpu
from jax.sharding import PartitionSpec as P


HEAD_DIM = 64
PAIR = 2 * HEAD_DIM
LN_EPS = 1e-6
ATTN_SCALE = HEAD_DIM ** -0.5
SPEC_PAD = 16
QBLK = 256
F32 = jnp.float32
BF16 = jnp.bfloat16


def dot_nt(a, b):
    return lax.dot_general(a, b, (((1,), (1,)), ((), ())), preferred_element_type=F32)


def dot_nn(a, b):
    return lax.dot_general(a, b, (((1,), (0,)), ((), ())), preferred_element_type=F32)


def block_kernel(n_spec, first, core_ref, *refs):
    (x_own, x_par, x_acr, x_rel, x_spc, dy_own, dy_par, dy_acr, dy_rel, dy_spc,
     ln_s, ln_b, l_scale, wq_ref, wk_ref, wv_ref, bq_ref, bk_ref, bv_ref, wp_ref) = refs[:20]
    refs = refs[20:]
    if first:
        acc_in = None
    else:
        acc_in, refs = refs[:5], refs[5:]
    attn_own, attn_par, dqkv_own, dqkv_par = refs[:4]
    acc_out, refs = refs[4:9], refs[9:]
    (norm_s, normt_s, dproj_s, q_s, k_s, v_s, da_s, vt_s, kt_s, s_s, dp_s, p_s, ds_s, dv_s, dk_s, at_s, dqkv_s) = refs
    patch = x_own.shape[-2]
    main = 4 * patch
    total = main + SPEC_PAD
    chunk = 80
    pair = pl.program_id(0)
    pieces = [(x_own, dy_own, 0, patch), (x_par, dy_par, patch, patch), (x_acr, dy_acr, 2 * patch, patch),
              (x_rel, dy_rel, 3 * patch, patch), (x_spc, dy_spc, main, SPEC_PAD)]

    @pl.when(pair == 0)
    def _():
        for x_ref, dy_ref, start, rows in pieces:
            step = min(rows, 64)

            @pl.loop(0, rows // step)
            def _(i):
                src = pl.ds(pl.multiple_of(i * step, step), step)
                dst = pl.ds(pl.multiple_of(start + i * step, step), step)
                x_float = x_ref[src, :].astype(F32)
                centered = x_float - jnp.mean(x_float, axis=-1, keepdims=True)
                inv_std = lax.rsqrt(jnp.mean(centered * centered, axis=-1, keepdims=True) + LN_EPS)
                norm_s[dst, :] = (centered * inv_std * ln_s[...] + ln_b[...]).astype(BF16)
                dproj_s[dst, :] = (dy_ref[src, :].astype(F32) * l_scale[...]).astype(BF16)

        width = norm_s.shape[1]

        @pl.loop(0, main // PAIR)
        def _(i):
            rows = pl.ds(pl.multiple_of(i * PAIR, PAIR), PAIR)
            for c in range(0, width, PAIR):
                normt_s[c:c + PAIR, rows] = norm_s[rows, c:c + PAIR].T

        for c in range(0, width, PAIR):
            tail = jnp.concatenate([norm_s[main:total, c:c + PAIR], jnp.zeros((PAIR - SPEC_PAD, PAIR), BF16)], axis=0)
            normt_s[c:c + PAIR, main:main + PAIR] = tail.T

        d_dy = jnp.zeros(acc_out[4].shape, F32)
        for _, dy_ref, _, rows in pieces:
            d_dy = d_dy + jnp.sum(dy_ref[...].astype(F32).reshape(rows // 8, 8, dy_ref.shape[-1]), axis=0)
        acc_out[4][...] = d_dy if first else acc_in[4][...] + d_dy

    scale = jnp.asarray(ATTN_SCALE, BF16)
    w_pair = jnp.concatenate([wq_ref[...], wk_ref[...], wv_ref[...]], axis=1)
    qkv = dot_nn(norm_s[...], w_pair) + jnp.concatenate([bq_ref[...], bk_ref[...], bv_ref[...]], axis=1)
    q_s[...] = qkv[:, 0:PAIR].astype(BF16) * scale
    k_s[...] = qkv[:, PAIR:2 * PAIR].astype(BF16)
    v_s[...] = qkv[:, 2 * PAIR:3 * PAIR].astype(BF16)
    da_s[...] = dot_nt(dproj_s[...], wp_ref[...]).astype(BF16)

    def transpose_in():
        for dst, src, mult in ((vt_s, v_s, None), (kt_s, k_s, scale)):
            for row in range(0, main, PAIR):
                vals = src[row:row + PAIR, :]
                dst[:, row:row + PAIR] = (vals if mult is None else vals * mult).T
            vals = src[main:total, :]
            tail = jnp.concatenate([vals if mult is None else vals * mult,
                                    jnp.zeros((PAIR - SPEC_PAD, PAIR), BF16)], axis=0)
            dst[:, main:main + PAIR] = tail.T

    def head_mask(rows, head):
        lane = lax.broadcasted_iota(jnp.int32, (rows, PAIR), 1)
        return (lane < HEAD_DIM) if head == 0 else (lane >= HEAD_DIM)

    def masked(rows_ref, start, rows):
        vals = rows_ref[start:start + rows, :]
        zero = jnp.zeros_like(vals)
        return [jnp.where(head_mask(rows, h), vals, zero) for h in range(2)]

    blocks = [None] + list(range(0, main, QBLK))

    def widths(t):
        return [(0, PAIR)] if blocks[t] is None else [(0, QBLK), (QBLK, QBLK)]

    def operands(t, rows_ref):
        if blocks[t] is None:
            parts = masked(rows_ref, main, SPEC_PAD)
            return [jnp.concatenate(parts + [jnp.zeros((PAIR - 2 * SPEC_PAD, PAIR), BF16)], axis=0)]
        return masked(rows_ref, blocks[t], QBLK)

    tops = {}

    def stage_scores(t):
        slot = t % 2
        tops[t] = []
        for (col, width), q_rows in zip(widths(t), operands(t, q_s)):
            s_val = dot_nt(k_s[...], q_rows)
            row = lax.broadcasted_iota(jnp.int32, (SPEC_PAD, width), 0)
            spec = jnp.where(row < n_spec, s_val[main:total], -jnp.inf)
            s_s[slot, 0:main, col:col + width] = s_val[0:main]
            s_s[slot, main:total, col:col + width] = spec
            tops[t].append(jnp.maximum(jnp.max(s_val[0:main], axis=0, keepdims=True), jnp.max(spec, axis=0, keepdims=True)))
        for (col, width), d_rows in zip(widths(t), operands(t, da_s)):
            dp_s[slot, :, col:col + width] = dot_nt(v_s[...], d_rows).astype(BF16)

    def stage_softmax(t):
        slot = t % 2
        for (col, width), top in zip(widths(t), tops[t]):
            norm = jnp.zeros((8, width), F32)
            mix = jnp.zeros((8, width), F32)
            for r in range(0, total, chunk):
                e = jnp.exp(s_s[slot, r:r + chunk, col:col + width] - top)
                s_s[slot, r:r + chunk, col:col + width] = e
                ed = e * dp_s[slot, r:r + chunk, col:col + width].astype(F32)
                for g in range(0, chunk, 8):
                    norm = norm + e[g:g + 8]
                    mix = mix + ed[g:g + 8]
            inv = 1.0 / jnp.sum(norm, axis=0, keepdims=True)
            mix = jnp.sum(mix, axis=0, keepdims=True) * inv
            for r in range(0, total, chunk):
                prob = s_s[slot, r:r + chunk, col:col + width] * inv
                p_s[slot, r:r + chunk, col:col + width] = prob.astype(BF16)
                ds = prob * (dp_s[slot, r:r + chunk, col:col + width].astype(F32) - mix)
                ds_s[slot, r:r + chunk, col:col + width] = ds.astype(BF16)

    def emit_attn(start, vals):
        if start >= main:
            attn_own[patch:patch + SPEC_PAD, :] = vals
            attn_par[patch:patch + SPEC_PAD, :] = vals
        elif start < patch:
            attn_own[start:start + vals.shape[0], :] = vals
        elif start < 2 * patch:
            attn_par[start - patch:start - patch + vals.shape[0], :] = vals

    def stage_outputs(t):
        slot = t % 2
        span = sum(width for _, width in widths(t))
        for acc, vals, rows_ref, col in ((dv_s, p_s, da_s, 2 * PAIR), (dk_s, ds_s, q_s, PAIR)):
            part = dot_nn(vals[slot, :, 0:span], jnp.concatenate(operands(t, rows_ref), axis=0))
            if t == 0:
                acc[...] = part
            elif t < len(blocks) - 1:
                acc[...] += part
            else:
                dqkv_s[:, col:col + PAIR] = (acc[...] + part).astype(BF16)
        for kind, lhs, vals in ((0, vt_s, p_s), (1, kt_s, ds_s)):
            if blocks[t] is None:
                both = dot_nn(lhs[:, 0:total], vals[slot, :, 0:PAIR]).T
                rows = jnp.where(head_mask(SPEC_PAD, 0), both[0:SPEC_PAD], both[SPEC_PAD:2 * SPEC_PAD]).astype(BF16)
                if kind == 0:
                    emit_attn(main, rows)
                    padded = jnp.concatenate([rows, jnp.zeros((PAIR - SPEC_PAD, PAIR), BF16)], axis=0)
                    at_s[:, main:main + PAIR] = padded.T
                else:
                    dqkv_s[main:total, 0:PAIR] = rows
                continue
            both = jnp.concatenate(
                [dot_nn(lhs[h * HEAD_DIM:(h + 1) * HEAD_DIM, 0:total], vals[slot, :, h * QBLK:(h + 1) * QBLK])
                 for h in range(2)], axis=0)
            if kind == 0:
                at_s[:, blocks[t]:blocks[t] + QBLK] = both.astype(BF16)
            if kind == 1 or blocks[t] < 2 * patch:
                for c in range(0, QBLK, PAIR):
                    rows = both[:, c:c + PAIR].T.astype(BF16)
                    if kind == 0:
                        emit_attn(blocks[t] + c, rows)
                    else:
                        dqkv_s[blocks[t] + c:blocks[t] + c + PAIR, 0:PAIR] = rows

    steps = len(blocks)
    stage_scores(0)
    transpose_in()
    for t in range(steps + 1):
        if t + 1 < steps:
            stage_scores(t + 1)
        if t >= 1:
            stage_outputs(t - 1)
        if t < steps:
            stage_softmax(t)

    dqkv_own[0:patch, :] = dqkv_s[0:patch, :]
    dqkv_own[patch:patch + SPEC_PAD, :] = dqkv_s[main:total, :]
    dqkv_par[0:patch, :] = dqkv_s[patch:2 * patch, :]
    dqkv_par[patch:patch + SPEC_PAD, :] = dqkv_s[main:total, :]
    d_b = jnp.sum(dqkv_s[...].astype(F32).reshape(total // 8, 8, 3 * PAIR), axis=0)
    acc_out[3][...] = d_b if first else acc_in[3][...] + d_b
    d_w = dot_nn(normt_s[:, 0:total], dqkv_s[...])
    acc_out[0][...] = (d_w if first else acc_in[0][...].reshape(d_w.shape) + d_w).reshape(acc_out[0].shape)
    d_g = dot_nn(at_s[:, main:main + SPEC_PAD], dy_spc[...])
    for _, dy_ref, start, rows in pieces[:4]:
        d_g = d_g + dot_nn(at_s[:, start:start + rows], dy_ref[...])
    acc_out[1][...] = d_g if first else acc_in[1][...] + d_g
    gls = jnp.sum((wp_ref[...].astype(F32) * acc_out[1][...]).reshape(PAIR // 8, 8, d_g.shape[1]), axis=0)

    @pl.when(pair == 0)
    def _():
        acc_out[2][...] = gls

    @pl.when(pair != 0)
    def _():
        acc_out[2][...] += gls


def fused_block(image, core, rows, accs, vectors, w_qkv, b_qkv, w_proj, n_spec):
    patch, d_model = rows[2].shape
    half = d_model // 2
    pairs = half // PAIR
    total = 4 * patch + SPEC_PAD
    first = accs is None

    def stacked(count):
        return pl.BlockSpec((None, count, d_model), lambda j, c: (image, 0, 0))

    def column(count, third):
        return pl.BlockSpec((count, PAIR), lambda j, c: (0, (2 * third + c[0]) * pairs + j))

    whole = pl.BlockSpec((patch, d_model), lambda j, c: (0, 0))
    vec = pl.BlockSpec((1, d_model), lambda j, c: (0, 0))
    acc_specs = [
        pl.BlockSpec((d_model, 3 * PAIR), lambda j, c: (0, j)),
        pl.BlockSpec((PAIR, d_model), lambda j, c: (j, 0)),
        pl.BlockSpec((8, d_model), lambda j, c: (0, 0)),
        pl.BlockSpec((8, 3 * PAIR), lambda j, c: (0, j)),
        pl.BlockSpec((8, d_model), lambda j, c: (0, 0)),
    ]
    acc_shapes = [
        jax.ShapeDtypeStruct((d_model, 3 * half), F32),
        jax.ShapeDtypeStruct((half, d_model), F32),
        jax.ShapeDtypeStruct((8, d_model), F32),
        jax.ShapeDtypeStruct((8, 3 * half), F32),
        jax.ShapeDtypeStruct((8, d_model), F32),
    ]
    row_spec = [stacked(patch), stacked(patch), whole, whole, stacked(SPEC_PAD)]
    in_specs = row_spec * 2 + [vec] * 3 + [column(d_model, t) for t in range(3)] + [column(1, t) for t in range(3)] + [
        pl.BlockSpec((PAIR, d_model), lambda j, c: (c[0] * pairs + j, 0)),
    ] + ([] if first else acc_specs)
    flops = 2 * 6 * total * total * PAIR * pairs * 4
    outs = pl.pallas_call(
        functools.partial(block_kernel, n_spec, first),
        grid_spec=pltpu.PrefetchScalarGridSpec(
            num_scalar_prefetch=1, grid=(pairs,),
            in_specs=in_specs,
            out_specs=[
                pl.BlockSpec((patch + SPEC_PAD, PAIR), lambda j, c: (0, j)),
                pl.BlockSpec((patch + SPEC_PAD, PAIR), lambda j, c: (0, j)),
                pl.BlockSpec((patch + SPEC_PAD, 3 * PAIR), lambda j, c: (0, j)),
                pl.BlockSpec((patch + SPEC_PAD, 3 * PAIR), lambda j, c: (0, j)),
            ] + acc_specs,
            scratch_shapes=[pltpu.VMEM((total, d_model), BF16), pltpu.VMEM((d_model, total - SPEC_PAD + PAIR), BF16),
                            pltpu.VMEM((total, d_model), BF16)]
            + [pltpu.VMEM((total, PAIR), BF16)] * 4
            + [pltpu.VMEM((PAIR, total - SPEC_PAD + PAIR), BF16)] * 2
            + [pltpu.VMEM((2, total, 2 * QBLK), F32)]
            + [pltpu.VMEM((2, total, 2 * QBLK), BF16)] * 3
            + [pltpu.VMEM((total, PAIR), F32)] * 2
            + [pltpu.VMEM((PAIR, total - SPEC_PAD + PAIR), BF16), pltpu.VMEM((total, 3 * PAIR), BF16)]),
        out_shape=[jax.ShapeDtypeStruct((patch + SPEC_PAD, half), BF16)] * 2
        + [jax.ShapeDtypeStruct((patch + SPEC_PAD, 3 * half), BF16)] * 2 + acc_shapes,
        input_output_aliases={} if first else {21 + i: 4 + i for i in range(5)},
        cost_estimate=pl.CostEstimate(flops=flops, bytes_accessed=8 * total * half * 2,
                                      transcendentals=2 * pairs * total * total),
        compiler_params=pltpu.CompilerParams(vmem_limit_bytes=40 * 1024 * 1024),
        name="fused_block",
    )(core, *rows, *vectors, w_qkv, w_qkv, w_qkv, b_qkv, b_qkv, b_qkv, w_proj, *([] if first else accs))
    return outs[:4], outs[4:]


def place_columns(dst, src, pairs, half):
    for third in range(3):
        for pair in range(pairs):
            col = ((2 * third + half) * pairs + pair) * PAIR
            at = (pair * 3 + third) * PAIR
            dst[..., col:col + PAIR] = src[..., at:at + PAIR]


def finish_kernel(images, core_ref, *refs):
    per_image, refs = refs[:4 * images], refs[4 * images:]
    (x_ref, xs_ref, dy_ref, dys_ref, w_ref, wp_ref, ln_s, l_scale, b_proj,
     out_ref, outs_ref, dx_ref, dxs_ref, sums_ref, at_s, dq_s, spec_s) = refs
    image = pl.program_id(0)
    half_cols = per_image[0].shape[1]
    pairs = half_cols // PAIR
    patch = x_ref.shape[0]
    for k in range(images):
        attn_own, attn_got, dqkv_own, dqkv_got = per_image[4 * k:4 * k + 4]
        for half in range(2):
            @pl.when(jnp.logical_and(image == k, core_ref[0] == half))
            def _():
                at_s[:, half * half_cols:(half + 1) * half_cols] = attn_own[...]
                at_s[:, (1 - half) * half_cols:(2 - half) * half_cols] = attn_got[...]
                place_columns(dq_s, dqkv_own, pairs, half)
                place_columns(dq_s, dqkv_got, pairs, 1 - half)

    @pl.when(image == 0)
    def _():
        sums_ref[...] = jnp.zeros_like(sums_ref)

    proj = dot_nn(at_s[...], wp_ref[...]) + b_proj[...]
    d_norm = dot_nt(dq_s[...], w_ref[...]).astype(BF16).astype(F32)
    n_out = outs_ref.shape[0]
    for slot, x_in, dy_in, start, rows in ((0, x_ref, dy_ref, 0, patch), (1, xs_ref, dys_ref, patch, SPEC_PAD)):
        x_float = x_in[...].astype(F32)
        out = x_float + l_scale[...] * proj[start:start + rows]
        centered = x_float - jnp.mean(x_float, axis=-1, keepdims=True)
        inv_std = lax.rsqrt(jnp.mean(centered * centered, axis=-1, keepdims=True) + LN_EPS)
        x_hat = centered * inv_std
        grad = d_norm[start:start + rows]
        grad_hat = grad * ln_s[...]
        d_rows = inv_std * (grad_hat - jnp.mean(grad_hat, axis=-1, keepdims=True)
                            - x_hat * jnp.mean(grad_hat * x_hat, axis=-1, keepdims=True))
        dx = dy_in[...].astype(F32) + d_rows
        if slot == 0:
            out_ref[...] = out.astype(BF16)
            dx_ref[...] = dx.astype(BF16)
        else:
            for k in range(images):
                @pl.when(image == k)
                def _():
                    for row in range(n_out):
                        spec_s[0, row, k:k + 1, :] = out[row:row + 1]
                        spec_s[1, row, k:k + 1, :] = dx[row:row + 1]

            @pl.when(image == images - 1)
            def _():
                outs_ref[...] = spec_s[0, :, 0:images, :].astype(BF16)
                dxs_ref[...] = spec_s[1, :, 0:images, :].astype(BF16)
        width = grad.shape[1]
        sums_ref[2 * slot] += jnp.sum((grad * x_hat).reshape(rows // 8, 8, width), axis=0)
        sums_ref[2 * slot + 1] += jnp.sum(grad.reshape(rows // 8, 8, width), axis=0)


def finish(core, per_image, x_patch, x_spec, dy_patch, dy_spec, w_qkv, w_proj, ln_scale, layer_scale, b_proj, n_spec):
    images, patch, d_model = x_patch.shape
    rows = patch + SPEC_PAD

    def const(shape):
        return pl.BlockSpec(shape, lambda i, c: (0,) * len(shape))

    def by_image(count):
        return pl.BlockSpec((None, count, d_model), lambda i, c: (i, 0, 0))

    flat = [arr for group in per_image for arr in group]
    return pl.pallas_call(
        functools.partial(finish_kernel, images),
        grid_spec=pltpu.PrefetchScalarGridSpec(
            num_scalar_prefetch=1, grid=(images,),
            in_specs=[const(arr.shape) for arr in flat]
            + [by_image(patch), by_image(SPEC_PAD), by_image(patch), by_image(SPEC_PAD),
               const(w_qkv.shape), const(w_proj.shape), const((1, d_model)), const((1, d_model)), const((1, d_model))],
            out_specs=[by_image(patch), const((n_spec, images, d_model)), by_image(patch), const((n_spec, images, d_model)),
                       const((4, 8, d_model))],
            scratch_shapes=[pltpu.VMEM((rows, d_model), BF16), pltpu.VMEM((rows, 3 * d_model), BF16),
                            pltpu.VMEM((2, n_spec, 8, d_model), F32)]),
        out_shape=[jax.ShapeDtypeStruct((images, patch, d_model), BF16), jax.ShapeDtypeStruct((n_spec, images, d_model), BF16),
                   jax.ShapeDtypeStruct((images, patch, d_model), BF16), jax.ShapeDtypeStruct((n_spec, images, d_model), BF16),
                   jax.ShapeDtypeStruct((4, 8, d_model), F32)],
        cost_estimate=pl.CostEstimate(flops=8 * images * rows * d_model * d_model, bytes_accessed=20 << 20, transcendentals=0),
        compiler_params=pltpu.CompilerParams(vmem_limit_bytes=34 * 1024 * 1024),
        name="finish",
    )(core, *flat, x_patch, x_spec, dy_patch, dy_spec, w_qkv, w_proj, ln_scale, layer_scale, b_proj)


def merge_kernel(core_ref, w_own, w_got, g_own, g_got, db_own, db_got, ds_own, ds_got, d_dy, l_scale, b_proj,
                 w_out, g_out, db_out, dbp_out, dls_out):
    pairs = w_own.shape[1] // (3 * PAIR)
    step = pl.program_id(0)
    count = pl.num_programs(0) // 2
    for half in range(2):
        @pl.when(core_ref[0] == half)
        def _():
            place_columns(w_out, w_own, pairs, half)
            place_columns(w_out, w_got, pairs, 1 - half)

    @pl.when(step // count == core_ref[0])
    def _():
        g_out[...] = g_own[...] * l_scale[...]

    @pl.when(step // count != core_ref[0])
    def _():
        g_out[...] = g_got[...] * l_scale[...]

    @pl.when(step == 0)
    def _():
        total_dy = jnp.sum(d_dy[...], axis=0)
        dbp_out[...] = total_dy * l_scale[0]
        dls_out[...] = jnp.sum(ds_own[...] + ds_got[...], axis=0) + b_proj[0] * total_dy
        own = jnp.sum(db_own[...], axis=0)
        got = jnp.sum(db_got[...], axis=0)
        for half in range(2):
            @pl.when(core_ref[0] == half)
            def _():
                place_columns(db_out, own, pairs, half)
                place_columns(db_out, got, pairs, 1 - half)


def merge_grads(core, w_own, w_got, g_own, g_got, db_own, db_got, ds_own, ds_got, d_dy, layer_scale, b_proj):
    rows, cols = w_own.shape
    half, d_model = g_own.shape
    tile = PAIR
    count = half // tile

    def const(shape):
        return pl.BlockSpec(shape, lambda g, c: (0,) * len(shape))

    def half_rows(other):
        def index(g, c):
            wanted = g // count == (c[0] if other == 0 else 1 - c[0])
            return (jnp.where(wanted, g % count, jnp.where(g < count, 0, count - 1)), 0)

        return index

    small = (db_own, db_got, ds_own, ds_got, d_dy, layer_scale, b_proj)
    return pl.pallas_call(
        merge_kernel,
        grid_spec=pltpu.PrefetchScalarGridSpec(
            num_scalar_prefetch=1, grid=(2 * count,),
            in_specs=[pl.BlockSpec((tile, cols), lambda g, c: (g, 0))] * 2
            + [pl.BlockSpec((tile, d_model), half_rows(0)), pl.BlockSpec((tile, d_model), half_rows(1))]
            + [const(arr.shape) for arr in small],
            out_specs=[pl.BlockSpec((tile, 2 * cols), lambda g, c: (g, 0)),
                       pl.BlockSpec((tile, d_model), lambda g, c: (g, 0)),
                       const((2 * cols,)), const((d_model,)), const((d_model,))]),
        out_shape=[jax.ShapeDtypeStruct((rows, 2 * cols), F32), jax.ShapeDtypeStruct((2 * half, d_model), F32),
                   jax.ShapeDtypeStruct((2 * cols,), F32), jax.ShapeDtypeStruct((d_model,), F32),
                   jax.ShapeDtypeStruct((d_model,), F32)],
        cost_estimate=pl.CostEstimate(flops=rows * cols * 256, bytes_accessed=20 << 20, transcendentals=0),
        name="merge_grads",
    )(core, w_own, w_got, g_own, g_got, *small)


def solution(mesh):
    group_size = mesh.shape['sp']
    partner = [(i, i ^ 1) for i in range(group_size)]
    opposite = [(i, i ^ 2) for i in range(group_size)]

    diagonal = [(i, i ^ 3) for i in range(group_size)]

    def swap(vals):
        return lax.ppermute(vals, 'sp', partner)

    def cross(vals):
        return lax.ppermute(vals, 'sp', opposite)

    def run_block(x_special, x_patch, dy_special, dy_patch, ln_scale, ln_bias, w_qkv, b_qkv, w_proj, b_proj, layer_scale):
        num_images, n_spec, _ = x_special.shape
        core = (lax.axis_index('sp') % 2).reshape(1).astype(jnp.int32)

        across = [(cross(x_patch[i]), cross(dy_patch[i])) for i in range(num_images)]
        x_partner, dy_partner = swap(x_patch), swap(dy_patch)

        pad = ((0, 0), (0, SPEC_PAD - n_spec), (0, 0))
        x_spec = jnp.pad(x_special, pad)
        dy_spec = jnp.pad(dy_special, pad)
        ln_scale, ln_bias, layer_scale, b_proj, b_qkv = (
            v.reshape(1, -1) for v in (ln_scale, ln_bias, layer_scale, b_proj, b_qkv))

        per_image = []
        relays = {}
        accs = None

        def gate(vals, image):
            if image < 0:
                return vals
            return lax.optimization_barrier((vals, per_image[image][0]))[0]

        def relay_image(image, after):
            across[image] = gate(across[image], after)
            relays[image] = (swap(across[image][0]), swap(across[image][1]))

        relay_image(0, -1)
        for i in range(num_images):
            near, relay = gate((across[i], relays[i]), i - 1)
            rows = (x_patch, x_partner, near[0], relay[0], x_spec, dy_patch, dy_partner, near[1], relay[1], dy_spec)
            (attn_own, attn_par, dqkv_own, dqkv_par), accs = fused_block(
                i, core, rows, accs, (ln_scale, ln_bias, layer_scale), w_qkv, b_qkv, w_proj, n_spec)
            per_image.append((attn_own, swap(attn_par), dqkv_own, swap(dqkv_par)))
            for image in range(i + 1, num_images):
                if image not in relays and (image <= i + 2):
                    relay_image(image, i)

        d_w, d_g, d_scale, d_b, d_dy = accs
        got = [swap(vals) for vals in (d_w, d_g, d_b, d_scale)]
        out_patch, out_special, dx_patch, dx_special, sums = finish(
            core, per_image, x_patch, x_spec, dy_patch, dy_spec, w_qkv, w_proj, ln_scale, layer_scale, b_proj, n_spec)
        sums = jnp.sum(sums, axis=1)
        near, far, diag = swap(sums[:2]), cross(sums[:2]), lax.ppermute(sums[:2], 'sp', diagonal)
        ln_grads = (sums[:2] + near) + (far + diag) + sums[2:]
        d_w_qkv, d_w_proj, d_b_qkv, d_b_proj, d_layer_scale = merge_grads(
            core, d_w, got[0], d_g, got[1], d_b, got[2], d_scale, got[3], d_dy, layer_scale, b_proj)
        return (out_special.transpose(1, 0, 2), out_patch, dx_special.transpose(1, 0, 2), dx_patch, ln_grads[0], ln_grads[1],
                d_w_qkv, d_b_qkv, d_w_proj, d_b_proj, d_layer_scale)

    part_rows = P('dp')
    part_seq = P('dp', 'sp')
    replicated = P()
    return jax.shard_map(
        run_block, mesh=mesh,
        in_specs=(part_rows, part_seq, part_rows, part_seq, replicated, replicated, replicated, replicated, replicated, replicated, replicated),
        out_specs=(part_rows, part_seq, part_rows, part_seq, part_rows, part_rows, part_rows, part_rows, part_rows, part_rows, part_rows),
        check_vma=False)
```

```python
import functools

import jax
import jax.numpy as jnp
from jax import lax
from jax.experimental import pallas as pl
from jax.experimental.pallas import tpu as pltpu
from jax.sharding import PartitionSpec as P


HEAD_DIM = 64
PAIR = 2 * HEAD_DIM
LN_EPS = 1e-6
ATTN_SCALE = HEAD_DIM ** -0.5
SPEC_PAD = 16
QBLK = 256
F32 = jnp.float32
BF16 = jnp.bfloat16


def dot_nt(a, b):
    return lax.dot_general(a, b, (((1,), (1,)), ((), ())), preferred_element_type=F32)


def dot_nn(a, b):
    return lax.dot_general(a, b, (((1,), (0,)), ((), ())), preferred_element_type=F32)


def block_kernel(n_spec, first, core_ref, *refs):
    (x_own, x_par, x_acr, x_rel, x_spc, dy_own, dy_par, dy_acr, dy_rel, dy_spc,
     ln_s, ln_b, l_scale, wq_ref, wk_ref, wv_ref, bq_ref, bk_ref, bv_ref, wp_ref) = refs[:20]
    refs = refs[20:]
    if first:
        acc_in = None
    else:
        acc_in, refs = refs[:5], refs[5:]
    attn_own, attn_par, dqkv_own, dqkv_par = refs[:4]
    acc_out, refs = refs[4:9], refs[9:]
    (norm_s, normt_s, dproj_s, q_s, k_s, v_s, da_s, vt_s, kt_s, s_s, dp_s, p_s, ds_s, dv_s, dk_s, at_s, dqkv_s,
     qkv_all, da_all, at_all) = refs
    patch = x_own.shape[-2]
    main = 4 * patch
    total = main + SPEC_PAD
    chunk = 80
    pair = pl.program_id(0)
    pieces = [(x_own, dy_own, 0, patch), (x_par, dy_par, patch, patch), (x_acr, dy_acr, 2 * patch, patch),
              (x_rel, dy_rel, 3 * patch, patch), (x_spc, dy_spc, main, SPEC_PAD)]

    @pl.when(pair == 0)
    def _():
        for x_ref, dy_ref, start, rows in pieces:
            step = min(rows, 64)

            @pl.loop(0, rows // step)
            def _(i):
                src = pl.ds(pl.multiple_of(i * step, step), step)
                dst = pl.ds(pl.multiple_of(start + i * step, step), step)
                x_float = x_ref[src, :].astype(F32)
                centered = x_float - jnp.mean(x_float, axis=-1, keepdims=True)
                inv_std = lax.rsqrt(jnp.mean(centered * centered, axis=-1, keepdims=True) + LN_EPS)
                norm_s[dst, :] = (centered * inv_std * ln_s[...] + ln_b[...]).astype(BF16)
                dproj_s[dst, :] = (dy_ref[src, :].astype(F32) * l_scale[...]).astype(BF16)

        width = norm_s.shape[1]

        @pl.loop(0, main // PAIR)
        def _(i):
            rows = pl.ds(pl.multiple_of(i * PAIR, PAIR), PAIR)
            for c in range(0, width, PAIR):
                normt_s[c:c + PAIR, rows] = norm_s[rows, c:c + PAIR].T

        for c in range(0, width, PAIR):
            tail = jnp.concatenate([norm_s[main:total, c:c + PAIR], jnp.zeros((PAIR - SPEC_PAD, PAIR), BF16)], axis=0)
            normt_s[c:c + PAIR, main:main + PAIR] = tail.T

        d_dy = jnp.zeros(acc_out[4].shape, F32)
        for _, dy_ref, _, rows in pieces:
            d_dy = d_dy + jnp.sum(dy_ref[...].astype(F32).reshape(rows // 8, 8, dy_ref.shape[-1]), axis=0)
        acc_out[4][...] = d_dy if first else acc_in[4][...] + d_dy

        w_all = jnp.concatenate([wq_ref[...], wk_ref[...], wv_ref[...]], axis=1)
        qkv = dot_nn(norm_s[...], w_all) + jnp.concatenate([bq_ref[...], bk_ref[...], bv_ref[...]], axis=1)
        qkv_all[...] = qkv.astype(BF16)
        da_all[...] = dot_nt(dproj_s[...], wp_ref[...]).astype(BF16)

    scale = jnp.asarray(ATTN_SCALE, BF16)
    half = da_all.shape[1]

    def pair_cols(base):
        return pl.ds(pl.multiple_of(base + pair * PAIR, PAIR), PAIR)

    q_s[...] = qkv_all[:, pair_cols(0)] * scale
    k_s[...] = qkv_all[:, pair_cols(half)]
    v_s[...] = qkv_all[:, pair_cols(2 * half)]
    da_s[...] = da_all[:, pair_cols(0)]

    def transpose_in():
        for dst, src, mult in ((vt_s, v_s, None), (kt_s, k_s, scale)):
            for row in range(0, main, PAIR):
                vals = src[row:row + PAIR, :]
                dst[:, row:row + PAIR] = (vals if mult is None else vals * mult).T
            vals = src[main:total, :]
            tail = jnp.concatenate([vals if mult is None else vals * mult,
                                    jnp.zeros((PAIR - SPEC_PAD, PAIR), BF16)], axis=0)
            dst[:, main:main + PAIR] = tail.T

    def head_mask(rows, head):
        lane = lax.broadcasted_iota(jnp.int32, (rows, PAIR), 1)
        return (lane < HEAD_DIM) if head == 0 else (lane >= HEAD_DIM)

    def masked(rows_ref, start, rows):
        vals = rows_ref[start:start + rows, :]
        zero = jnp.zeros_like(vals)
        return [jnp.where(head_mask(rows, h), vals, zero) for h in range(2)]

    blocks = [None] + list(range(0, main, QBLK))

    def widths(t):
        return [(0, PAIR)] if blocks[t] is None else [(0, QBLK), (QBLK, QBLK)]

    def operands(t, rows_ref):
        if blocks[t] is None:
            parts = masked(rows_ref, main, SPEC_PAD)
            return [jnp.concatenate(parts + [jnp.zeros((PAIR - 2 * SPEC_PAD, PAIR), BF16)], axis=0)]
        return masked(rows_ref, blocks[t], QBLK)

    tops = {}

    def stage_scores(t):
        slot = t % 2
        tops[t] = []
        for (col, width), q_rows in zip(widths(t), operands(t, q_s)):
            s_val = dot_nt(k_s[...], q_rows)
            row = lax.broadcasted_iota(jnp.int32, (SPEC_PAD, width), 0)
            spec = jnp.where(row < n_spec, s_val[main:total], -jnp.inf)
            s_s[slot, 0:main, col:col + width] = s_val[0:main]
            s_s[slot, main:total, col:col + width] = spec
            tops[t].append(jnp.maximum(jnp.max(s_val[0:main], axis=0, keepdims=True), jnp.max(spec, axis=0, keepdims=True)))
        for (col, width), d_rows in zip(widths(t), operands(t, da_s)):
            dp_s[slot, :, col:col + width] = dot_nt(v_s[...], d_rows).astype(BF16)

    def stage_softmax(t):
        slot = t % 2
        for (col, width), top in zip(widths(t), tops[t]):
            norm = jnp.zeros((8, width), F32)
            mix = jnp.zeros((8, width), F32)
            for r in range(0, total, chunk):
                e = jnp.exp(s_s[slot, r:r + chunk, col:col + width] - top)
                s_s[slot, r:r + chunk, col:col + width] = e
                ed = e * dp_s[slot, r:r + chunk, col:col + width].astype(F32)
                for g in range(0, chunk, 8):
                    norm = norm + e[g:g + 8]
                    mix = mix + ed[g:g + 8]
            inv = 1.0 / jnp.sum(norm, axis=0, keepdims=True)
            mix = jnp.sum(mix, axis=0, keepdims=True) * inv
            for r in range(0, total, chunk):
                prob = s_s[slot, r:r + chunk, col:col + width] * inv
                p_s[slot, r:r + chunk, col:col + width] = prob.astype(BF16)
                ds = prob * (dp_s[slot, r:r + chunk, col:col + width].astype(F32) - mix)
                ds_s[slot, r:r + chunk, col:col + width] = ds.astype(BF16)

    def emit_attn(start, vals):
        if start >= main:
            attn_own[patch:patch + SPEC_PAD, :] = vals
            attn_par[patch:patch + SPEC_PAD, :] = vals
        elif start < patch:
            attn_own[start:start + vals.shape[0], :] = vals
        elif start < 2 * patch:
            attn_par[start - patch:start - patch + vals.shape[0], :] = vals

    def stage_outputs(t):
        slot = t % 2
        span = sum(width for _, width in widths(t))
        for acc, vals, rows_ref, col in ((dv_s, p_s, da_s, 2 * PAIR), (dk_s, ds_s, q_s, PAIR)):
            part = dot_nn(vals[slot, :, 0:span], jnp.concatenate(operands(t, rows_ref), axis=0))
            if t == 0:
                acc[...] = part
            elif t < len(blocks) - 1:
                acc[...] += part
            else:
                dqkv_s[:, col:col + PAIR] = (acc[...] + part).astype(BF16)
        for kind, lhs, vals in ((0, vt_s, p_s), (1, kt_s, ds_s)):
            if blocks[t] is None:
                both = dot_nn(lhs[:, 0:total], vals[slot, :, 0:PAIR]).T
                rows = jnp.where(head_mask(SPEC_PAD, 0), both[0:SPEC_PAD], both[SPEC_PAD:2 * SPEC_PAD]).astype(BF16)
                if kind == 0:
                    emit_attn(main, rows)
                    padded = jnp.concatenate([rows, jnp.zeros((PAIR - SPEC_PAD, PAIR), BF16)], axis=0)
                    at_s[:, main:main + PAIR] = padded.T
                else:
                    dqkv_s[main:total, 0:PAIR] = rows
                continue
            both = jnp.concatenate(
                [dot_nn(lhs[h * HEAD_DIM:(h + 1) * HEAD_DIM, 0:total], vals[slot, :, h * QBLK:(h + 1) * QBLK])
                 for h in range(2)], axis=0)
            if kind == 0:
                at_s[:, blocks[t]:blocks[t] + QBLK] = both.astype(BF16)
            if kind == 1 or blocks[t] < 2 * patch:
                for c in range(0, QBLK, PAIR):
                    rows = both[:, c:c + PAIR].T.astype(BF16)
                    if kind == 0:
                        emit_attn(blocks[t] + c, rows)
                    else:
                        dqkv_s[blocks[t] + c:blocks[t] + c + PAIR, 0:PAIR] = rows

    steps = len(blocks)
    stage_scores(0)
    transpose_in()
    for t in range(steps + 1):
        if t + 1 < steps:
            stage_scores(t + 1)
        if t >= 1:
            stage_outputs(t - 1)
        if t < steps:
            stage_softmax(t)

    dqkv_own[0:patch, :] = dqkv_s[0:patch, :]
    dqkv_own[patch:patch + SPEC_PAD, :] = dqkv_s[main:total, :]
    dqkv_par[0:patch, :] = dqkv_s[patch:2 * patch, :]
    dqkv_par[patch:patch + SPEC_PAD, :] = dqkv_s[main:total, :]
    d_b = jnp.sum(dqkv_s[...].astype(F32).reshape(total // 8, 8, 3 * PAIR), axis=0)
    acc_out[3][...] = d_b if first else acc_in[3][...] + d_b
    d_w = dot_nn(normt_s[:, 0:total], dqkv_s[...])
    acc_out[0][...] = (d_w if first else acc_in[0][...].reshape(d_w.shape) + d_w).reshape(acc_out[0].shape)
    at_all[pair] = at_s[...]

    @pl.when(pair == pl.num_programs(0) - 1)
    def _():
        lhs = at_all[...].reshape(half, at_all.shape[2])
        d_g = dot_nn(lhs[:, main:main + SPEC_PAD], dy_spc[...])
        for _, dy_ref, start, rows in pieces[:4]:
            d_g = d_g + dot_nn(lhs[:, start:start + rows], dy_ref[...])
        d_g = d_g if first else acc_in[1][...] + d_g
        acc_out[1][...] = d_g
        acc_out[2][...] = jnp.sum((wp_ref[...].astype(F32) * d_g).reshape(half // 8, 8, d_g.shape[1]), axis=0)


def fused_block(image, core, rows, accs, vectors, w_qkv, b_qkv, w_proj, n_spec):
    patch, d_model = rows[2].shape
    half = d_model // 2
    pairs = half // PAIR
    total = 4 * patch + SPEC_PAD
    first = accs is None
    once = pl.Buffered(buffer_count=1)

    def stacked(count):
        return pl.BlockSpec((None, count, d_model), lambda j, c: (image, 0, 0), pipeline_mode=once)

    def column(count, third):
        return pl.BlockSpec((count, half), lambda j, c: (0, 2 * third + c[0]), pipeline_mode=once)

    whole = pl.BlockSpec((patch, d_model), lambda j, c: (0, 0), pipeline_mode=once)
    vec = pl.BlockSpec((1, d_model), lambda j, c: (0, 0))
    acc_specs = [
        pl.BlockSpec((d_model, 3 * PAIR), lambda j, c: (0, j)),
        pl.BlockSpec((half, d_model), lambda j, c: (0, 0), pipeline_mode=once),
        pl.BlockSpec((8, d_model), lambda j, c: (0, 0)),
        pl.BlockSpec((8, 3 * PAIR), lambda j, c: (0, j)),
        pl.BlockSpec((8, d_model), lambda j, c: (0, 0)),
    ]
    acc_shapes = [
        jax.ShapeDtypeStruct((d_model, 3 * half), F32),
        jax.ShapeDtypeStruct((half, d_model), F32),
        jax.ShapeDtypeStruct((8, d_model), F32),
        jax.ShapeDtypeStruct((8, 3 * half), F32),
        jax.ShapeDtypeStruct((8, d_model), F32),
    ]
    row_spec = [stacked(patch), stacked(patch), whole, whole, stacked(SPEC_PAD)]
    in_specs = row_spec * 2 + [vec] * 3 + [column(d_model, t) for t in range(3)] + [column(1, t) for t in range(3)] + [
        pl.BlockSpec((half, d_model), lambda j, c: (c[0], 0), pipeline_mode=once),
    ] + ([] if first else acc_specs)
    flops = 2 * 6 * total * total * PAIR * pairs * 4
    outs = pl.pallas_call(
        functools.partial(block_kernel, n_spec, first),
        grid_spec=pltpu.PrefetchScalarGridSpec(
            num_scalar_prefetch=1, grid=(pairs,),
            in_specs=in_specs,
            out_specs=[
                pl.BlockSpec((patch + SPEC_PAD, PAIR), lambda j, c: (0, j)),
                pl.BlockSpec((patch + SPEC_PAD, PAIR), lambda j, c: (0, j)),
                pl.BlockSpec((patch + SPEC_PAD, 3 * PAIR), lambda j, c: (0, j)),
                pl.BlockSpec((patch + SPEC_PAD, 3 * PAIR), lambda j, c: (0, j)),
            ] + acc_specs,
            scratch_shapes=[pltpu.VMEM((total, d_model), BF16), pltpu.VMEM((d_model, total - SPEC_PAD + PAIR), BF16),
                            pltpu.VMEM((total, d_model), BF16)]
            + [pltpu.VMEM((total, PAIR), BF16)] * 4
            + [pltpu.VMEM((PAIR, total - SPEC_PAD + PAIR), BF16)] * 2
            + [pltpu.VMEM((2, total, 2 * QBLK), F32)]
            + [pltpu.VMEM((2, total, 2 * QBLK), BF16)] * 3
            + [pltpu.VMEM((total, PAIR), F32)] * 2
            + [pltpu.VMEM((PAIR, total - SPEC_PAD + PAIR), BF16), pltpu.VMEM((total, 3 * PAIR), BF16)]
            + [pltpu.VMEM((total, 3 * half), BF16), pltpu.VMEM((total, half), BF16),
               pltpu.VMEM((pairs, PAIR, total - SPEC_PAD + PAIR), BF16)]),
        out_shape=[jax.ShapeDtypeStruct((patch + SPEC_PAD, half), BF16)] * 2
        + [jax.ShapeDtypeStruct((patch + SPEC_PAD, 3 * half), BF16)] * 2 + acc_shapes,
        input_output_aliases={} if first else {21 + i: 4 + i for i in range(5)},
        cost_estimate=pl.CostEstimate(flops=flops, bytes_accessed=8 * total * half * 2,
                                      transcendentals=2 * pairs * total * total),
        compiler_params=pltpu.CompilerParams(vmem_limit_bytes=40 * 1024 * 1024),
        name="fused_block",
    )(core, *rows, *vectors, w_qkv, w_qkv, w_qkv, b_qkv, b_qkv, b_qkv, w_proj, *([] if first else accs))
    return outs[:4], outs[4:]


def place_columns(dst, src, pairs, half):
    for third in range(3):
        for pair in range(pairs):
            col = ((2 * third + half) * pairs + pair) * PAIR
            at = (pair * 3 + third) * PAIR
            dst[..., col:col + PAIR] = src[..., at:at + PAIR]


def finish_kernel(images, core_ref, *refs):
    per_image, refs = refs[:4 * images], refs[4 * images:]
    (x_ref, xs_ref, dy_ref, dys_ref, w_ref, wp_ref, ln_s, l_scale, b_proj,
     out_ref, outs_ref, dx_ref, dxs_ref, sums_ref, at_s, dq_s, spec_s) = refs
    image = pl.program_id(0)
    half_cols = per_image[0].shape[1]
    pairs = half_cols // PAIR
    patch = x_ref.shape[0]
    for k in range(images):
        attn_own, attn_got, dqkv_own, dqkv_got = per_image[4 * k:4 * k + 4]
        for half in range(2):
            @pl.when(jnp.logical_and(image == k, core_ref[0] == half))
            def _():
                at_s[:, half * half_cols:(half + 1) * half_cols] = attn_own[...]
                at_s[:, (1 - half) * half_cols:(2 - half) * half_cols] = attn_got[...]
                place_columns(dq_s, dqkv_own, pairs, half)
                place_columns(dq_s, dqkv_got, pairs, 1 - half)

    @pl.when(image == 0)
    def _():
        sums_ref[...] = jnp.zeros_like(sums_ref)

    proj = dot_nn(at_s[...], wp_ref[...]) + b_proj[...]
    d_norm = dot_nt(dq_s[...], w_ref[...]).astype(BF16).astype(F32)
    n_out = outs_ref.shape[0]
    for slot, x_in, dy_in, start, rows in ((0, x_ref, dy_ref, 0, patch), (1, xs_ref, dys_ref, patch, SPEC_PAD)):
        x_float = x_in[...].astype(F32)
        out = x_float + l_scale[...] * proj[start:start + rows]
        centered = x_float - jnp.mean(x_float, axis=-1, keepdims=True)
        inv_std = lax.rsqrt(jnp.mean(centered * centered, axis=-1, keepdims=True) + LN_EPS)
        x_hat = centered * inv_std
        grad = d_norm[start:start + rows]
        grad_hat = grad * ln_s[...]
        d_rows = inv_std * (grad_hat - jnp.mean(grad_hat, axis=-1, keepdims=True)
                            - x_hat * jnp.mean(grad_hat * x_hat, axis=-1, keepdims=True))
        dx = dy_in[...].astype(F32) + d_rows
        if slot == 0:
            out_ref[...] = out.astype(BF16)
            dx_ref[...] = dx.astype(BF16)
        else:
            for k in range(images):
                @pl.when(image == k)
                def _():
                    for row in range(n_out):
                        spec_s[0, row, k:k + 1, :] = out[row:row + 1]
                        spec_s[1, row, k:k + 1, :] = dx[row:row + 1]

            @pl.when(image == images - 1)
            def _():
                outs_ref[...] = spec_s[0, :, 0:images, :].astype(BF16)
                dxs_ref[...] = spec_s[1, :, 0:images, :].astype(BF16)
        width = grad.shape[1]
        sums_ref[2 * slot] += jnp.sum((grad * x_hat).reshape(rows // 8, 8, width), axis=0)
        sums_ref[2 * slot + 1] += jnp.sum(grad.reshape(rows // 8, 8, width), axis=0)


def finish(core, per_image, x_patch, x_spec, dy_patch, dy_spec, w_qkv, w_proj, ln_scale, layer_scale, b_proj, n_spec):
    images, patch, d_model = x_patch.shape
    rows = patch + SPEC_PAD

    def const(shape):
        return pl.BlockSpec(shape, lambda i, c: (0,) * len(shape))

    def by_image(count):
        return pl.BlockSpec((None, count, d_model), lambda i, c: (i, 0, 0))

    flat = [arr for group in per_image for arr in group]
    return pl.pallas_call(
        functools.partial(finish_kernel, images),
        grid_spec=pltpu.PrefetchScalarGridSpec(
            num_scalar_prefetch=1, grid=(images,),
            in_specs=[const(arr.shape) for arr in flat]
            + [by_image(patch), by_image(SPEC_PAD), by_image(patch), by_image(SPEC_PAD),
               const(w_qkv.shape), const(w_proj.shape), const((1, d_model)), const((1, d_model)), const((1, d_model))],
            out_specs=[by_image(patch), const((n_spec, images, d_model)), by_image(patch), const((n_spec, images, d_model)),
                       const((4, 8, d_model))],
            scratch_shapes=[pltpu.VMEM((rows, d_model), BF16), pltpu.VMEM((rows, 3 * d_model), BF16),
                            pltpu.VMEM((2, n_spec, 8, d_model), F32)]),
        out_shape=[jax.ShapeDtypeStruct((images, patch, d_model), BF16), jax.ShapeDtypeStruct((n_spec, images, d_model), BF16),
                   jax.ShapeDtypeStruct((images, patch, d_model), BF16), jax.ShapeDtypeStruct((n_spec, images, d_model), BF16),
                   jax.ShapeDtypeStruct((4, 8, d_model), F32)],
        cost_estimate=pl.CostEstimate(flops=8 * images * rows * d_model * d_model, bytes_accessed=20 << 20, transcendentals=0),
        compiler_params=pltpu.CompilerParams(vmem_limit_bytes=34 * 1024 * 1024),
        name="finish",
    )(core, *flat, x_patch, x_spec, dy_patch, dy_spec, w_qkv, w_proj, ln_scale, layer_scale, b_proj)


def merge_kernel(core_ref, w_own, w_got, g_own, g_got, db_own, db_got, ds_own, ds_got, d_dy, l_scale, b_proj,
                 w_out, g_out, db_out, dbp_out, dls_out):
    pairs = w_own.shape[1] // (3 * PAIR)
    step = pl.program_id(0)
    count = pl.num_programs(0) // 2
    for half in range(2):
        @pl.when(core_ref[0] == half)
        def _():
            place_columns(w_out, w_own, pairs, half)
            place_columns(w_out, w_got, pairs, 1 - half)

    @pl.when(step // count == core_ref[0])
    def _():
        g_out[...] = g_own[...] * l_scale[...]

    @pl.when(step // count != core_ref[0])
    def _():
        g_out[...] = g_got[...] * l_scale[...]

    @pl.when(step == 0)
    def _():
        total_dy = jnp.sum(d_dy[...], axis=0)
        dbp_out[...] = total_dy * l_scale[0]
        dls_out[...] = jnp.sum(ds_own[...] + ds_got[...], axis=0) + b_proj[0] * total_dy
        own = jnp.sum(db_own[...], axis=0)
        got = jnp.sum(db_got[...], axis=0)
        for half in range(2):
            @pl.when(core_ref[0] == half)
            def _():
                place_columns(db_out, own, pairs, half)
                place_columns(db_out, got, pairs, 1 - half)


def merge_grads(core, w_own, w_got, g_own, g_got, db_own, db_got, ds_own, ds_got, d_dy, layer_scale, b_proj):
    rows, cols = w_own.shape
    half, d_model = g_own.shape
    tile = PAIR
    count = half // tile

    def const(shape):
        return pl.BlockSpec(shape, lambda g, c: (0,) * len(shape))

    def half_rows(other):
        def index(g, c):
            wanted = g // count == (c[0] if other == 0 else 1 - c[0])
            return (jnp.where(wanted, g % count, jnp.where(g < count, 0, count - 1)), 0)

        return index

    small = (db_own, db_got, ds_own, ds_got, d_dy, layer_scale, b_proj)
    return pl.pallas_call(
        merge_kernel,
        grid_spec=pltpu.PrefetchScalarGridSpec(
            num_scalar_prefetch=1, grid=(2 * count,),
            in_specs=[pl.BlockSpec((tile, cols), lambda g, c: (g, 0))] * 2
            + [pl.BlockSpec((tile, d_model), half_rows(0)), pl.BlockSpec((tile, d_model), half_rows(1))]
            + [const(arr.shape) for arr in small],
            out_specs=[pl.BlockSpec((tile, 2 * cols), lambda g, c: (g, 0)),
                       pl.BlockSpec((tile, d_model), lambda g, c: (g, 0)),
                       const((2 * cols,)), const((d_model,)), const((d_model,))]),
        out_shape=[jax.ShapeDtypeStruct((rows, 2 * cols), F32), jax.ShapeDtypeStruct((2 * half, d_model), F32),
                   jax.ShapeDtypeStruct((2 * cols,), F32), jax.ShapeDtypeStruct((d_model,), F32),
                   jax.ShapeDtypeStruct((d_model,), F32)],
        cost_estimate=pl.CostEstimate(flops=rows * cols * 256, bytes_accessed=20 << 20, transcendentals=0),
        name="merge_grads",
    )(core, w_own, w_got, g_own, g_got, *small)


def solution(mesh):
    group_size = mesh.shape['sp']
    partner = [(i, i ^ 1) for i in range(group_size)]
    opposite = [(i, i ^ 2) for i in range(group_size)]

    diagonal = [(i, i ^ 3) for i in range(group_size)]

    def swap(vals):
        return lax.ppermute(vals, 'sp', partner)

    def cross(vals):
        return lax.ppermute(vals, 'sp', opposite)

    def run_block(x_special, x_patch, dy_special, dy_patch, ln_scale, ln_bias, w_qkv, b_qkv, w_proj, b_proj, layer_scale):
        num_images, n_spec, _ = x_special.shape
        core = (lax.axis_index('sp') % 2).reshape(1).astype(jnp.int32)

        across = [(cross(x_patch[i]), cross(dy_patch[i])) for i in range(num_images)]
        x_partner, dy_partner = swap(x_patch), swap(dy_patch)

        pad = ((0, 0), (0, SPEC_PAD - n_spec), (0, 0))
        x_spec = jnp.pad(x_special, pad)
        dy_spec = jnp.pad(dy_special, pad)
        ln_scale, ln_bias, layer_scale, b_proj, b_qkv = (
            v.reshape(1, -1) for v in (ln_scale, ln_bias, layer_scale, b_proj, b_qkv))

        per_image = []
        relays = {}
        accs = None

        def gate(vals, image):
            if image < 0:
                return vals
            return lax.optimization_barrier((vals, per_image[image][0]))[0]

        def relay_image(image, after):
            across[image] = gate(across[image], after)
            relays[image] = (swap(across[image][0]), swap(across[image][1]))

        relay_image(0, -1)
        for i in range(num_images):
            near, relay = gate((across[i], relays[i]), i - 1)
            rows = (x_patch, x_partner, near[0], relay[0], x_spec, dy_patch, dy_partner, near[1], relay[1], dy_spec)
            (attn_own, attn_par, dqkv_own, dqkv_par), accs = fused_block(
                i, core, rows, accs, (ln_scale, ln_bias, layer_scale), w_qkv, b_qkv, w_proj, n_spec)
            per_image.append((attn_own, swap(attn_par), dqkv_own, swap(dqkv_par)))
            for image in range(i + 1, num_images):
                if image not in relays and (image <= i + 2):
                    relay_image(image, i)

        d_w, d_g, d_scale, d_b, d_dy = accs
        got = [swap(vals) for vals in (d_w, d_g, d_b, d_scale)]
        out_patch, out_special, dx_patch, dx_special, sums = finish(
            core, per_image, x_patch, x_spec, dy_patch, dy_spec, w_qkv, w_proj, ln_scale, layer_scale, b_proj, n_spec)
        sums = jnp.sum(sums, axis=1)
        near, far, diag = swap(sums[:2]), cross(sums[:2]), lax.ppermute(sums[:2], 'sp', diagonal)
        ln_grads = (sums[:2] + near) + (far + diag) + sums[2:]
        d_w_qkv, d_w_proj, d_b_qkv, d_b_proj, d_layer_scale = merge_grads(
            core, d_w, got[0], d_g, got[1], d_b, got[2], d_scale, got[3], d_dy, layer_scale, b_proj)
        return (out_special.transpose(1, 0, 2), out_patch, dx_special.transpose(1, 0, 2), dx_patch, ln_grads[0], ln_grads[1],
                d_w_qkv, d_b_qkv, d_w_proj, d_b_proj, d_layer_scale)

    part_rows = P('dp')
    part_seq = P('dp', 'sp')
    replicated = P()
    return jax.shard_map(
        run_block, mesh=mesh,
        in_specs=(part_rows, part_seq, part_rows, part_seq, replicated, replicated, replicated, replicated, replicated, replicated, replicated),
        out_specs=(part_rows, part_seq, part_rows, part_seq, part_rows, part_rows, part_rows, part_rows, part_rows, part_rows, part_rows),
        check_vma=False)
```

```python
import functools

import jax
import jax.numpy as jnp
from jax import lax
from jax.experimental import pallas as pl
from jax.experimental.pallas import tpu as pltpu
from jax.sharding import PartitionSpec as P


HEAD_DIM = 64
PAIR = 2 * HEAD_DIM
LN_EPS = 1e-6
ATTN_SCALE = HEAD_DIM ** -0.5
SPEC_PAD = 16
QBLK = 256
F32 = jnp.float32
BF16 = jnp.bfloat16


def dot_nt(a, b):
    return lax.dot_general(a, b, (((1,), (1,)), ((), ())), preferred_element_type=F32)


def dot_nn(a, b):
    return lax.dot_general(a, b, (((1,), (0,)), ((), ())), preferred_element_type=F32)


def block_kernel(n_spec, first, core_ref, *refs):
    (x_own, x_par, x_acr, x_rel, x_spc, dy_own, dy_par, dy_acr, dy_rel, dy_spc,
     ln_s, ln_b, l_scale, wq_ref, wk_ref, wv_ref, bq_ref, bk_ref, bv_ref, wp_ref) = refs[:20]
    refs = refs[20:]
    if first:
        acc_in = None
    else:
        acc_in, refs = refs[:5], refs[5:]
    attn_own, attn_par, dqkv_own, dqkv_par = refs[:4]
    acc_out, refs = refs[4:9], refs[9:]
    (norm_s, normt_s, dproj_s, q_s, k_s, v_s, da_s, vt_s, kt_s, s_s, dp_s, p_s, ds_s, dv_s, dk_s, at_s, dqkv_s,
     qkv_all, da_all, at_all) = refs
    patch = x_own.shape[-2]
    main = 4 * patch
    total = main + SPEC_PAD
    chunk = 80
    pair = pl.program_id(0)
    pieces = [(x_own, dy_own, 0, patch), (x_par, dy_par, patch, patch), (x_acr, dy_acr, 2 * patch, patch),
              (x_rel, dy_rel, 3 * patch, patch), (x_spc, dy_spc, main, SPEC_PAD)]

    @pl.when(pair == 0)
    def _():
        for x_ref, dy_ref, start, rows in pieces:
            step = min(rows, 64)

            @pl.loop(0, rows // step)
            def _(i):
                src = pl.ds(pl.multiple_of(i * step, step), step)
                dst = pl.ds(pl.multiple_of(start + i * step, step), step)
                x_float = x_ref[src, :].astype(F32)
                centered = x_float - jnp.mean(x_float, axis=-1, keepdims=True)
                inv_std = lax.rsqrt(jnp.mean(centered * centered, axis=-1, keepdims=True) + LN_EPS)
                norm_s[dst, :] = (centered * inv_std * ln_s[...] + ln_b[...]).astype(BF16)
                dproj_s[dst, :] = (dy_ref[src, :].astype(F32) * l_scale[...]).astype(BF16)

        width = norm_s.shape[1]

        @pl.loop(0, main // PAIR)
        def _(i):
            rows = pl.ds(pl.multiple_of(i * PAIR, PAIR), PAIR)
            for c in range(0, width, PAIR):
                normt_s[c:c + PAIR, rows] = norm_s[rows, c:c + PAIR].T

        for c in range(0, width, PAIR):
            tail = jnp.concatenate([norm_s[main:total, c:c + PAIR], jnp.zeros((PAIR - SPEC_PAD, PAIR), BF16)], axis=0)
            normt_s[c:c + PAIR, main:main + PAIR] = tail.T

        d_dy = jnp.zeros(acc_out[4].shape, F32)
        for _, dy_ref, _, rows in pieces:
            d_dy = d_dy + jnp.sum(dy_ref[...].astype(F32).reshape(rows // 8, 8, dy_ref.shape[-1]), axis=0)
        acc_out[4][...] = d_dy if first else acc_in[4][...] + d_dy

        w_all = jnp.concatenate([wq_ref[...], wk_ref[...], wv_ref[...]], axis=1)
        qkv = dot_nn(norm_s[...], w_all) + jnp.concatenate([bq_ref[...], bk_ref[...], bv_ref[...]], axis=1)
        qkv_all[...] = qkv.astype(BF16)
        da_all[...] = dot_nt(dproj_s[...], wp_ref[...]).astype(BF16)

    scale = jnp.asarray(ATTN_SCALE, BF16)
    half = da_all.shape[1]

    def pair_cols(base):
        return pl.ds(pl.multiple_of(base + pair * PAIR, PAIR), PAIR)

    q_s[...] = qkv_all[:, pair_cols(0)] * scale
    k_s[...] = qkv_all[:, pair_cols(half)]
    v_s[...] = qkv_all[:, pair_cols(2 * half)]
    da_s[...] = da_all[:, pair_cols(0)]

    def transpose_in():
        for dst, src, mult in ((vt_s, v_s, None), (kt_s, k_s, scale)):
            for row in range(0, main, PAIR):
                vals = src[row:row + PAIR, :]
                dst[:, row:row + PAIR] = (vals if mult is None else vals * mult).T
            vals = src[main:total, :]
            tail = jnp.concatenate([vals if mult is None else vals * mult,
                                    jnp.zeros((PAIR - SPEC_PAD, PAIR), BF16)], axis=0)
            dst[:, main:main + PAIR] = tail.T

    def head_mask(rows, head):
        lane = lax.broadcasted_iota(jnp.int32, (rows, PAIR), 1)
        return (lane < HEAD_DIM) if head == 0 else (lane >= HEAD_DIM)

    def masked(rows_ref, start, rows):
        vals = rows_ref[start:start + rows, :]
        zero = jnp.zeros_like(vals)
        return [jnp.where(head_mask(rows, h), vals, zero) for h in range(2)]

    blocks = [None] + list(range(0, main, QBLK))

    def widths(t):
        return [(0, PAIR)] if blocks[t] is None else [(0, QBLK), (QBLK, QBLK)]

    def operands(t, rows_ref):
        if blocks[t] is None:
            parts = masked(rows_ref, main, SPEC_PAD)
            return [jnp.concatenate(parts + [jnp.zeros((PAIR - 2 * SPEC_PAD, PAIR), BF16)], axis=0)]
        return masked(rows_ref, blocks[t], QBLK)

    tops = {}

    def stage_scores(t):
        slot = t % 2
        tops[t] = []
        for (col, width), q_rows in zip(widths(t), operands(t, q_s)):
            s_val = dot_nt(k_s[...], q_rows)
            row = lax.broadcasted_iota(jnp.int32, (SPEC_PAD, width), 0)
            spec = jnp.where(row < n_spec, s_val[main:total], -jnp.inf)
            s_s[slot, 0:main, col:col + width] = s_val[0:main]
            s_s[slot, main:total, col:col + width] = spec
            tops[t].append(jnp.maximum(jnp.max(s_val[0:main], axis=0, keepdims=True), jnp.max(spec, axis=0, keepdims=True)))
        for (col, width), d_rows in zip(widths(t), operands(t, da_s)):
            dp_s[slot, :, col:col + width] = dot_nt(v_s[...], d_rows).astype(BF16)

    def stage_softmax(t):
        slot = t % 2
        for (col, width), top in zip(widths(t), tops[t]):
            norm = jnp.zeros((8, width), F32)
            mix = jnp.zeros((8, width), F32)
            for r in range(0, total, chunk):
                e = jnp.exp(s_s[slot, r:r + chunk, col:col + width] - top)
                s_s[slot, r:r + chunk, col:col + width] = e
                ed = e * dp_s[slot, r:r + chunk, col:col + width].astype(F32)
                for g in range(0, chunk, 8):
                    norm = norm + e[g:g + 8]
                    mix = mix + ed[g:g + 8]
            inv = 1.0 / jnp.sum(norm, axis=0, keepdims=True)
            mix = jnp.sum(mix, axis=0, keepdims=True) * inv
            for r in range(0, total, chunk):
                prob = s_s[slot, r:r + chunk, col:col + width] * inv
                p_s[slot, r:r + chunk, col:col + width] = prob.astype(BF16)
                ds = prob * (dp_s[slot, r:r + chunk, col:col + width].astype(F32) - mix)
                ds_s[slot, r:r + chunk, col:col + width] = ds.astype(BF16)

    def emit_attn(start, vals):
        if start >= main:
            attn_own[patch:patch + SPEC_PAD, :] = vals
            attn_par[patch:patch + SPEC_PAD, :] = vals
        elif start < patch:
            attn_own[start:start + vals.shape[0], :] = vals
        elif start < 2 * patch:
            attn_par[start - patch:start - patch + vals.shape[0], :] = vals

    def stage_outputs(t):
        slot = t % 2
        span = sum(width for _, width in widths(t))
        for acc, vals, rows_ref, col in ((dv_s, p_s, da_s, 2 * PAIR), (dk_s, ds_s, q_s, PAIR)):
            part = dot_nn(vals[slot, :, 0:span], jnp.concatenate(operands(t, rows_ref), axis=0))
            if t == 0:
                acc[...] = part
            elif t < len(blocks) - 1:
                acc[...] += part
            else:
                dqkv_s[:, col:col + PAIR] = (acc[...] + part).astype(BF16)
        for kind, lhs, vals in ((0, vt_s, p_s), (1, kt_s, ds_s)):
            if blocks[t] is None:
                both = dot_nn(lhs[:, 0:total], vals[slot, :, 0:PAIR]).T
                rows = jnp.where(head_mask(SPEC_PAD, 0), both[0:SPEC_PAD], both[SPEC_PAD:2 * SPEC_PAD]).astype(BF16)
                if kind == 0:
                    emit_attn(main, rows)
                    padded = jnp.concatenate([rows, jnp.zeros((PAIR - SPEC_PAD, PAIR), BF16)], axis=0)
                    at_s[:, main:main + PAIR] = padded.T
                else:
                    dqkv_s[main:total, 0:PAIR] = rows
                continue
            both = jnp.concatenate(
                [dot_nn(lhs[h * HEAD_DIM:(h + 1) * HEAD_DIM, 0:total], vals[slot, :, h * QBLK:(h + 1) * QBLK])
                 for h in range(2)], axis=0)
            if kind == 0:
                at_s[:, blocks[t]:blocks[t] + QBLK] = both.astype(BF16)
            if kind == 1 or blocks[t] < 2 * patch:
                for c in range(0, QBLK, PAIR):
                    rows = both[:, c:c + PAIR].T.astype(BF16)
                    if kind == 0:
                        emit_attn(blocks[t] + c, rows)
                    else:
                        dqkv_s[blocks[t] + c:blocks[t] + c + PAIR, 0:PAIR] = rows

    steps = len(blocks)
    stage_scores(0)
    transpose_in()
    for t in range(steps + 1):
        if t + 1 < steps:
            stage_scores(t + 1)
        if t >= 1:
            stage_outputs(t - 1)
        if t < steps:
            stage_softmax(t)

    dqkv_own[0:patch, :] = dqkv_s[0:patch, :]
    dqkv_own[patch:patch + SPEC_PAD, :] = dqkv_s[main:total, :]
    dqkv_par[0:patch, :] = dqkv_s[patch:2 * patch, :]
    dqkv_par[patch:patch + SPEC_PAD, :] = dqkv_s[main:total, :]
    d_b = jnp.sum(dqkv_s[...].astype(F32).reshape(total // 8, 8, 3 * PAIR), axis=0)
    acc_out[3][...] = d_b if first else acc_in[3][...] + d_b
    d_w = dot_nn(normt_s[:, 0:total], dqkv_s[...])
    acc_out[0][...] = (d_w if first else acc_in[0][...].reshape(d_w.shape) + d_w).reshape(acc_out[0].shape)
    at_all[pair] = at_s[...]

    @pl.when(pair == pl.num_programs(0) - 1)
    def _():
        lhs = at_all[...].reshape(half, at_all.shape[2])
        d_g = dot_nn(lhs[:, main:main + SPEC_PAD], dy_spc[...])
        for _, dy_ref, start, rows in pieces[:4]:
            d_g = d_g + dot_nn(lhs[:, start:start + rows], dy_ref[...])
        d_g = d_g if first else acc_in[1][...] + d_g
        acc_out[1][...] = d_g
        acc_out[2][...] = jnp.sum((wp_ref[...].astype(F32) * d_g).reshape(half // 8, 8, d_g.shape[1]), axis=0)


def fused_block(image, core, rows, accs, vectors, w_qkv, b_qkv, w_proj, n_spec):
    patch, d_model = rows[2].shape
    half = d_model // 2
    pairs = half // PAIR
    total = 4 * patch + SPEC_PAD
    first = accs is None
    once = pl.Buffered(buffer_count=1)

    def stacked(count):
        return pl.BlockSpec((None, count, d_model), lambda j, c: (image, 0, 0), pipeline_mode=once)

    def column(count, third):
        return pl.BlockSpec((count, half), lambda j, c: (0, 2 * third + c[0]), pipeline_mode=once)

    whole = pl.BlockSpec((patch, d_model), lambda j, c: (0, 0), pipeline_mode=once)
    vec = pl.BlockSpec((1, d_model), lambda j, c: (0, 0))
    acc_specs = [
        pl.BlockSpec((d_model, 3 * PAIR), lambda j, c: (0, j)),
        pl.BlockSpec((half, d_model), lambda j, c: (0, 0), pipeline_mode=once),
        pl.BlockSpec((8, d_model), lambda j, c: (0, 0)),
        pl.BlockSpec((8, 3 * PAIR), lambda j, c: (0, j)),
        pl.BlockSpec((8, d_model), lambda j, c: (0, 0)),
    ]
    acc_shapes = [
        jax.ShapeDtypeStruct((d_model, 3 * half), F32),
        jax.ShapeDtypeStruct((half, d_model), F32),
        jax.ShapeDtypeStruct((8, d_model), F32),
        jax.ShapeDtypeStruct((8, 3 * half), F32),
        jax.ShapeDtypeStruct((8, d_model), F32),
    ]
    row_spec = [stacked(patch), stacked(patch), whole, whole, stacked(SPEC_PAD)]
    in_specs = row_spec * 2 + [vec] * 3 + [column(d_model, t) for t in range(3)] + [column(1, t) for t in range(3)] + [
        pl.BlockSpec((half, d_model), lambda j, c: (c[0], 0), pipeline_mode=once),
    ] + ([] if first else acc_specs)
    flops = 2 * 6 * total * total * PAIR * pairs * 4
    outs = pl.pallas_call(
        functools.partial(block_kernel, n_spec, first),
        grid_spec=pltpu.PrefetchScalarGridSpec(
            num_scalar_prefetch=1, grid=(pairs,),
            in_specs=in_specs,
            out_specs=[
                pl.BlockSpec((patch + SPEC_PAD, PAIR), lambda j, c: (0, j)),
                pl.BlockSpec((patch + SPEC_PAD, PAIR), lambda j, c: (0, j)),
                pl.BlockSpec((patch + SPEC_PAD, 3 * PAIR), lambda j, c: (0, j)),
                pl.BlockSpec((patch + SPEC_PAD, 3 * PAIR), lambda j, c: (0, j)),
            ] + acc_specs,
            scratch_shapes=[pltpu.VMEM((total, d_model), BF16), pltpu.VMEM((d_model, total - SPEC_PAD + PAIR), BF16),
                            pltpu.VMEM((total, d_model), BF16)]
            + [pltpu.VMEM((total, PAIR), BF16)] * 4
            + [pltpu.VMEM((PAIR, total - SPEC_PAD + PAIR), BF16)] * 2
            + [pltpu.VMEM((2, total, 2 * QBLK), F32)]
            + [pltpu.VMEM((2, total, 2 * QBLK), BF16)] * 3
            + [pltpu.VMEM((total, PAIR), F32)] * 2
            + [pltpu.VMEM((PAIR, total - SPEC_PAD + PAIR), BF16), pltpu.VMEM((total, 3 * PAIR), BF16)]
            + [pltpu.VMEM((total, 3 * half), BF16), pltpu.VMEM((total, half), BF16),
               pltpu.VMEM((pairs, PAIR, total - SPEC_PAD + PAIR), BF16)]),
        out_shape=[jax.ShapeDtypeStruct((patch + SPEC_PAD, half), BF16)] * 2
        + [jax.ShapeDtypeStruct((patch + SPEC_PAD, 3 * half), BF16)] * 2 + acc_shapes,
        input_output_aliases={} if first else {21 + i: 4 + i for i in range(5)},
        cost_estimate=pl.CostEstimate(flops=flops, bytes_accessed=8 * total * half * 2,
                                      transcendentals=2 * pairs * total * total),
        compiler_params=pltpu.CompilerParams(vmem_limit_bytes=40 * 1024 * 1024),
        name="fused_block",
    )(core, *rows, *vectors, w_qkv, w_qkv, w_qkv, b_qkv, b_qkv, b_qkv, w_proj, *([] if first else accs))
    return outs[:4], outs[4:]


def place_columns(dst, src, pairs, half):
    for third in range(3):
        for pair in range(pairs):
            col = ((2 * third + half) * pairs + pair) * PAIR
            at = (pair * 3 + third) * PAIR
            dst[..., col:col + PAIR] = src[..., at:at + PAIR]


def finish_kernel(images, core_ref, *refs):
    per_image, refs = refs[:4 * images], refs[4 * images:]
    (x_ref, xs_ref, dy_ref, dys_ref, w_ref, wp_ref, ln_s, l_scale, b_proj,
     out_ref, outs_ref, dx_ref, dxs_ref, sums_ref, at_s, dq_s, spec_s) = refs
    image = pl.program_id(0)
    half_cols = per_image[0].shape[1]
    pairs = half_cols // PAIR
    patch = x_ref.shape[0]
    for k in range(images):
        attn_own, attn_got, dqkv_own, dqkv_got = per_image[4 * k:4 * k + 4]
        for half in range(2):
            @pl.when(jnp.logical_and(image == k, core_ref[0] == half))
            def _():
                at_s[:, half * half_cols:(half + 1) * half_cols] = attn_own[...]
                at_s[:, (1 - half) * half_cols:(2 - half) * half_cols] = attn_got[...]
                place_columns(dq_s, dqkv_own, pairs, half)
                place_columns(dq_s, dqkv_got, pairs, 1 - half)

    @pl.when(image == 0)
    def _():
        sums_ref[...] = jnp.zeros_like(sums_ref)

    proj = dot_nn(at_s[...], wp_ref[...]) + b_proj[...]
    d_norm = dot_nt(dq_s[...], w_ref[...]).astype(BF16).astype(F32)
    n_out = outs_ref.shape[0]
    for slot, x_in, dy_in, start, rows in ((0, x_ref, dy_ref, 0, patch), (1, xs_ref, dys_ref, patch, SPEC_PAD)):
        x_float = x_in[...].astype(F32)
        out = x_float + l_scale[...] * proj[start:start + rows]
        centered = x_float - jnp.mean(x_float, axis=-1, keepdims=True)
        inv_std = lax.rsqrt(jnp.mean(centered * centered, axis=-1, keepdims=True) + LN_EPS)
        x_hat = centered * inv_std
        grad = d_norm[start:start + rows]
        grad_hat = grad * ln_s[...]
        d_rows = inv_std * (grad_hat - jnp.mean(grad_hat, axis=-1, keepdims=True)
                            - x_hat * jnp.mean(grad_hat * x_hat, axis=-1, keepdims=True))
        dx = dy_in[...].astype(F32) + d_rows
        if slot == 0:
            out_ref[...] = out.astype(BF16)
            dx_ref[...] = dx.astype(BF16)
        else:
            for k in range(images):
                @pl.when(image == k)
                def _():
                    for row in range(n_out):
                        spec_s[0, row, k:k + 1, :] = out[row:row + 1]
                        spec_s[1, row, k:k + 1, :] = dx[row:row + 1]

            @pl.when(image == images - 1)
            def _():
                outs_ref[...] = spec_s[0, :, 0:images, :].astype(BF16)
                dxs_ref[...] = spec_s[1, :, 0:images, :].astype(BF16)
        width = grad.shape[1]
        sums_ref[2 * slot] += jnp.sum((grad * x_hat).reshape(rows // 8, 8, width), axis=0)
        sums_ref[2 * slot + 1] += jnp.sum(grad.reshape(rows // 8, 8, width), axis=0)


def finish(core, per_image, x_patch, x_spec, dy_patch, dy_spec, w_qkv, w_proj, ln_scale, layer_scale, b_proj, n_spec):
    images, patch, d_model = x_patch.shape
    rows = patch + SPEC_PAD

    def const(shape):
        return pl.BlockSpec(shape, lambda i, c: (0,) * len(shape))

    def by_image(count):
        return pl.BlockSpec((None, count, d_model), lambda i, c: (i, 0, 0))

    flat = [arr for group in per_image for arr in group]
    return pl.pallas_call(
        functools.partial(finish_kernel, images),
        grid_spec=pltpu.PrefetchScalarGridSpec(
            num_scalar_prefetch=1, grid=(images,),
            in_specs=[const(arr.shape) for arr in flat]
            + [by_image(patch), by_image(SPEC_PAD), by_image(patch), by_image(SPEC_PAD),
               const(w_qkv.shape), const(w_proj.shape), const((1, d_model)), const((1, d_model)), const((1, d_model))],
            out_specs=[by_image(patch), const((n_spec, images, d_model)), by_image(patch), const((n_spec, images, d_model)),
                       const((4, 8, d_model))],
            scratch_shapes=[pltpu.VMEM((rows, d_model), BF16), pltpu.VMEM((rows, 3 * d_model), BF16),
                            pltpu.VMEM((2, n_spec, 8, d_model), F32)]),
        out_shape=[jax.ShapeDtypeStruct((images, patch, d_model), BF16), jax.ShapeDtypeStruct((n_spec, images, d_model), BF16),
                   jax.ShapeDtypeStruct((images, patch, d_model), BF16), jax.ShapeDtypeStruct((n_spec, images, d_model), BF16),
                   jax.ShapeDtypeStruct((4, 8, d_model), F32)],
        cost_estimate=pl.CostEstimate(flops=8 * images * rows * d_model * d_model, bytes_accessed=20 << 20, transcendentals=0),
        compiler_params=pltpu.CompilerParams(vmem_limit_bytes=34 * 1024 * 1024),
        name="finish",
    )(core, *flat, x_patch, x_spec, dy_patch, dy_spec, w_qkv, w_proj, ln_scale, layer_scale, b_proj)


def merge_kernel(core_ref, w_own, w_got, g_own, g_got, db_own, db_got, ds_own, ds_got, d_dy, l_scale, b_proj,
                 w_out, g_out, db_out, dbp_out, dls_out):
    pairs = w_own.shape[1] // (3 * PAIR)
    step = pl.program_id(0)
    count = pl.num_programs(0) // 2
    for half in range(2):
        @pl.when(core_ref[0] == half)
        def _():
            place_columns(w_out, w_own, pairs, half)
            place_columns(w_out, w_got, pairs, 1 - half)

    @pl.when(step // count == core_ref[0])
    def _():
        g_out[...] = g_own[...] * l_scale[...]

    @pl.when(step // count != core_ref[0])
    def _():
        g_out[...] = g_got[...] * l_scale[...]

    @pl.when(step == 0)
    def _():
        total_dy = jnp.sum(d_dy[...], axis=0)
        dbp_out[...] = total_dy * l_scale[0]
        dls_out[...] = jnp.sum(ds_own[...] + ds_got[...], axis=0) + b_proj[0] * total_dy
        own = jnp.sum(db_own[...], axis=0)
        got = jnp.sum(db_got[...], axis=0)
        for half in range(2):
            @pl.when(core_ref[0] == half)
            def _():
                place_columns(db_out, own, pairs, half)
                place_columns(db_out, got, pairs, 1 - half)


def merge_grads(core, w_own, w_got, g_own, g_got, db_own, db_got, ds_own, ds_got, d_dy, layer_scale, b_proj):
    rows, cols = w_own.shape
    half, d_model = g_own.shape
    tile = PAIR
    count = half // tile

    def const(shape):
        return pl.BlockSpec(shape, lambda g, c: (0,) * len(shape))

    def half_rows(other):
        def index(g, c):
            wanted = g // count == (c[0] if other == 0 else 1 - c[0])
            return (jnp.where(wanted, g % count, jnp.where(g < count, 0, count - 1)), 0)

        return index

    small = (db_own, db_got, ds_own, ds_got, d_dy, layer_scale, b_proj)
    return pl.pallas_call(
        merge_kernel,
        grid_spec=pltpu.PrefetchScalarGridSpec(
            num_scalar_prefetch=1, grid=(2 * count,),
            in_specs=[pl.BlockSpec((tile, cols), lambda g, c: (g, 0))] * 2
            + [pl.BlockSpec((tile, d_model), half_rows(0)), pl.BlockSpec((tile, d_model), half_rows(1))]
            + [const(arr.shape) for arr in small],
            out_specs=[pl.BlockSpec((tile, 2 * cols), lambda g, c: (g, 0)),
                       pl.BlockSpec((tile, d_model), lambda g, c: (g, 0)),
                       const((2 * cols,)), const((d_model,)), const((d_model,))]),
        out_shape=[jax.ShapeDtypeStruct((rows, 2 * cols), F32), jax.ShapeDtypeStruct((2 * half, d_model), F32),
                   jax.ShapeDtypeStruct((2 * cols,), F32), jax.ShapeDtypeStruct((d_model,), F32),
                   jax.ShapeDtypeStruct((d_model,), F32)],
        cost_estimate=pl.CostEstimate(flops=rows * cols * 256, bytes_accessed=20 << 20, transcendentals=0),
        name="merge_grads",
    )(core, w_own, w_got, g_own, g_got, *small)


def solution(mesh):
    group_size = mesh.shape['sp']
    partner = [(i, i ^ 1) for i in range(group_size)]
    opposite = [(i, i ^ 2) for i in range(group_size)]

    diagonal = [(i, i ^ 3) for i in range(group_size)]

    def swap(vals):
        return lax.ppermute(vals, 'sp', partner)

    def cross(vals):
        return lax.ppermute(vals, 'sp', opposite)

    def run_block(x_special, x_patch, dy_special, dy_patch, ln_scale, ln_bias, w_qkv, b_qkv, w_proj, b_proj, layer_scale):
        num_images, n_spec, _ = x_special.shape
        core = (lax.axis_index('sp') % 2).reshape(1).astype(jnp.int32)

        x_first, dy_first = x_patch[0], dy_patch[0]
        x_later, dy_later = lax.optimization_barrier((x_patch, dy_patch, x_first, dy_first))[:2]
        across = [(cross(x_first), cross(dy_first))]
        across += [(cross(x_later[i]), cross(dy_later[i])) for i in range(1, num_images)]
        x_partner, dy_partner = swap(x_patch), swap(dy_patch)

        pad = ((0, 0), (0, SPEC_PAD - n_spec), (0, 0))
        x_spec = jnp.pad(x_special, pad)
        dy_spec = jnp.pad(dy_special, pad)
        ln_scale, ln_bias, layer_scale, b_proj, b_qkv = (
            v.reshape(1, -1) for v in (ln_scale, ln_bias, layer_scale, b_proj, b_qkv))

        per_image = []
        relays = {}
        accs = None

        def gate(vals, image):
            if image < 0:
                return vals
            return lax.optimization_barrier((vals, per_image[image][0]))[0]

        def relay_image(image, after):
            across[image] = gate(across[image], after)
            relays[image] = (swap(across[image][0]), swap(across[image][1]))

        relay_image(0, -1)
        for i in range(num_images):
            near, relay = gate((across[i], relays[i]), i - 1)
            rows = (x_patch, x_partner, near[0], relay[0], x_spec, dy_patch, dy_partner, near[1], relay[1], dy_spec)
            (attn_own, attn_par, dqkv_own, dqkv_par), accs = fused_block(
                i, core, rows, accs, (ln_scale, ln_bias, layer_scale), w_qkv, b_qkv, w_proj, n_spec)
            per_image.append((attn_own, swap(attn_par), dqkv_own, swap(dqkv_par)))
            for image in range(i + 1, num_images):
                if image not in relays and (image <= i + 2):
                    relay_image(image, i)

        d_w, d_g, d_scale, d_b, d_dy = accs
        got = [swap(vals) for vals in (d_w, d_g, d_b, d_scale)]
        out_patch, out_special, dx_patch, dx_special, sums = finish(
            core, per_image, x_patch, x_spec, dy_patch, dy_spec, w_qkv, w_proj, ln_scale, layer_scale, b_proj, n_spec)
        sums = jnp.sum(sums, axis=1)
        near, far, diag = swap(sums[:2]), cross(sums[:2]), lax.ppermute(sums[:2], 'sp', diagonal)
        ln_grads = (sums[:2] + near) + (far + diag) + sums[2:]
        d_w_qkv, d_w_proj, d_b_qkv, d_b_proj, d_layer_scale = merge_grads(
            core, d_w, got[0], d_g, got[1], d_b, got[2], d_scale, got[3], d_dy, layer_scale, b_proj)
        return (out_special.transpose(1, 0, 2), out_patch, dx_special.transpose(1, 0, 2), dx_patch, ln_grads[0], ln_grads[1],
                d_w_qkv, d_b_qkv, d_w_proj, d_b_proj, d_layer_scale)

    part_rows = P('dp')
    part_seq = P('dp', 'sp')
    replicated = P()
    return jax.shard_map(
        run_block, mesh=mesh,
        in_specs=(part_rows, part_seq, part_rows, part_seq, replicated, replicated, replicated, replicated, replicated, replicated, replicated),
        out_specs=(part_rows, part_seq, part_rows, part_seq, part_rows, part_rows, part_rows, part_rows, part_rows, part_rows, part_rows),
        check_vma=False)
```

```python
import functools

import jax
import jax.numpy as jnp
from jax import lax
from jax.experimental import pallas as pl
from jax.experimental.pallas import tpu as pltpu
from jax.sharding import PartitionSpec as P


HEAD_DIM = 64
PAIR = 2 * HEAD_DIM
LN_EPS = 1e-6
ATTN_SCALE = HEAD_DIM ** -0.5
SPEC_PAD = 16
QBLK = 256
F32 = jnp.float32
BF16 = jnp.bfloat16


def dot_nt(a, b):
    return lax.dot_general(a, b, (((1,), (1,)), ((), ())), preferred_element_type=F32)


def dot_nn(a, b):
    return lax.dot_general(a, b, (((1,), (0,)), ((), ())), preferred_element_type=F32)


def block_kernel(n_spec, first, core_ref, *refs):
    (x_own, x_par, x_acr, x_rel, x_spc, dy_own, dy_par, dy_acr, dy_rel, dy_spc,
     ln_s, ln_b, l_scale, wq_ref, wk_ref, wv_ref, bq_ref, bk_ref, bv_ref, wp_ref) = refs[:20]
    refs = refs[20:]
    if first:
        acc_in = None
    else:
        acc_in, refs = refs[:5], refs[5:]
    attn_own, attn_par, dqkv_own, dqkv_par = refs[:4]
    acc_out, refs = refs[4:9], refs[9:]
    (norm_s, normt_s, dproj_s, q_s, k_s, v_s, da_s, vt_s, kt_s, s_s, dp_s, p_s, ds_s, dv_s, dk_s, at_s, dqkv_s,
     qkv_all, da_all, at_all) = refs
    patch = x_own.shape[-2]
    main = 4 * patch
    total = main + SPEC_PAD
    chunk = 80
    pair = pl.program_id(0)
    pieces = [(x_own, dy_own, 0, patch), (x_par, dy_par, patch, patch), (x_acr, dy_acr, 2 * patch, patch),
              (x_rel, dy_rel, 3 * patch, patch), (x_spc, dy_spc, main, SPEC_PAD)]

    @pl.when(pair == 0)
    def _():
        for x_ref, dy_ref, start, rows in pieces:
            step = min(rows, 64)

            @pl.loop(0, rows // step)
            def _(i):
                src = pl.ds(pl.multiple_of(i * step, step), step)
                dst = pl.ds(pl.multiple_of(start + i * step, step), step)
                x_float = x_ref[src, :].astype(F32)
                centered = x_float - jnp.mean(x_float, axis=-1, keepdims=True)
                inv_std = lax.rsqrt(jnp.mean(centered * centered, axis=-1, keepdims=True) + LN_EPS)
                norm_s[dst, :] = (centered * inv_std * ln_s[...] + ln_b[...]).astype(BF16)
                dproj_s[dst, :] = (dy_ref[src, :].astype(F32) * l_scale[...]).astype(BF16)

        width = norm_s.shape[1]

        @pl.loop(0, main // PAIR)
        def _(i):
            rows = pl.ds(pl.multiple_of(i * PAIR, PAIR), PAIR)
            for c in range(0, width, PAIR):
                normt_s[c:c + PAIR, rows] = norm_s[rows, c:c + PAIR].T

        for c in range(0, width, PAIR):
            tail = jnp.concatenate([norm_s[main:total, c:c + PAIR], jnp.zeros((PAIR - SPEC_PAD, PAIR), BF16)], axis=0)
            normt_s[c:c + PAIR, main:main + PAIR] = tail.T

        d_dy = jnp.zeros(acc_out[4].shape, F32)
        for _, dy_ref, _, rows in pieces:
            d_dy = d_dy + jnp.sum(dy_ref[...].astype(F32).reshape(rows // 8, 8, dy_ref.shape[-1]), axis=0)
        acc_out[4][...] = d_dy if first else acc_in[4][...] + d_dy

        w_all = jnp.concatenate([wq_ref[...], wk_ref[...], wv_ref[...]], axis=1)
        qkv = dot_nn(norm_s[...], w_all) + jnp.concatenate([bq_ref[...], bk_ref[...], bv_ref[...]], axis=1)
        qkv_all[...] = qkv.astype(BF16)
        da_all[...] = dot_nt(dproj_s[...], wp_ref[...]).astype(BF16)

    scale = jnp.asarray(ATTN_SCALE, BF16)
    half = da_all.shape[1]

    def pair_cols(base):
        return pl.ds(pl.multiple_of(base + pair * PAIR, PAIR), PAIR)

    q_s[...] = qkv_all[:, pair_cols(0)] * scale
    k_s[...] = qkv_all[:, pair_cols(half)]
    v_s[...] = qkv_all[:, pair_cols(2 * half)]
    da_s[...] = da_all[:, pair_cols(0)]

    def transpose_in():
        for dst, src, mult in ((vt_s, v_s, None), (kt_s, k_s, scale)):
            for row in range(0, main, PAIR):
                vals = src[row:row + PAIR, :]
                dst[:, row:row + PAIR] = (vals if mult is None else vals * mult).T
            vals = src[main:total, :]
            tail = jnp.concatenate([vals if mult is None else vals * mult,
                                    jnp.zeros((PAIR - SPEC_PAD, PAIR), BF16)], axis=0)
            dst[:, main:main + PAIR] = tail.T

    def head_mask(rows, head):
        lane = lax.broadcasted_iota(jnp.int32, (rows, PAIR), 1)
        return (lane < HEAD_DIM) if head == 0 else (lane >= HEAD_DIM)

    def masked(rows_ref, start, rows):
        vals = rows_ref[start:start + rows, :]
        zero = jnp.zeros_like(vals)
        return [jnp.where(head_mask(rows, h), vals, zero) for h in range(2)]

    blocks = [None] + list(range(0, main, QBLK))

    def widths(t):
        return [(0, PAIR)] if blocks[t] is None else [(0, QBLK), (QBLK, QBLK)]

    def operands(t, rows_ref):
        if blocks[t] is None:
            parts = masked(rows_ref, main, SPEC_PAD)
            return [jnp.concatenate(parts + [jnp.zeros((PAIR - 2 * SPEC_PAD, PAIR), BF16)], axis=0)]
        return masked(rows_ref, blocks[t], QBLK)

    tops = {}

    def stage_scores(t):
        slot = t % 2
        tops[t] = []
        for (col, width), q_rows in zip(widths(t), operands(t, q_s)):
            s_val = dot_nt(k_s[...], q_rows)
            row = lax.broadcasted_iota(jnp.int32, (SPEC_PAD, width), 0)
            spec = jnp.where(row < n_spec, s_val[main:total], -jnp.inf)
            s_s[slot, 0:main, col:col + width] = s_val[0:main]
            s_s[slot, main:total, col:col + width] = spec
            tops[t].append(jnp.maximum(jnp.max(s_val[0:main], axis=0, keepdims=True), jnp.max(spec, axis=0, keepdims=True)))
        for (col, width), d_rows in zip(widths(t), operands(t, da_s)):
            dp_s[slot, :, col:col + width] = dot_nt(v_s[...], d_rows).astype(BF16)

    def stage_softmax(t):
        slot = t % 2
        for (col, width), top in zip(widths(t), tops[t]):
            norm = jnp.zeros((8, width), F32)
            mix = jnp.zeros((8, width), F32)
            for r in range(0, total, chunk):
                e = jnp.exp(s_s[slot, r:r + chunk, col:col + width] - top)
                s_s[slot, r:r + chunk, col:col + width] = e
                ed = e * dp_s[slot, r:r + chunk, col:col + width].astype(F32)
                for g in range(0, chunk, 8):
                    norm = norm + e[g:g + 8]
                    mix = mix + ed[g:g + 8]
            inv = 1.0 / jnp.sum(norm, axis=0, keepdims=True)
            mix = jnp.sum(mix, axis=0, keepdims=True) * inv
            for r in range(0, total, chunk):
                prob = s_s[slot, r:r + chunk, col:col + width] * inv
                p_s[slot, r:r + chunk, col:col + width] = prob.astype(BF16)
                ds = prob * (dp_s[slot, r:r + chunk, col:col + width].astype(F32) - mix)
                ds_s[slot, r:r + chunk, col:col + width] = ds.astype(BF16)

    def emit_attn(start, vals):
        if start >= main:
            attn_own[patch:patch + SPEC_PAD, :] = vals
            attn_par[patch:patch + SPEC_PAD, :] = vals
        elif start < patch:
            attn_own[start:start + vals.shape[0], :] = vals
        elif start < 2 * patch:
            attn_par[start - patch:start - patch + vals.shape[0], :] = vals

    def stage_outputs(t):
        slot = t % 2
        span = sum(width for _, width in widths(t))
        for acc, vals, rows_ref, col in ((dv_s, p_s, da_s, 2 * PAIR),):
            part = dot_nn(vals[slot, :, 0:span], jnp.concatenate(operands(t, rows_ref), axis=0))
            if t == 0:
                acc[...] = part
            elif t < len(blocks) - 1:
                acc[...] += part
            else:
                dqkv_s[:, col:col + PAIR] = (acc[...] + part).astype(BF16)
        for kind, lhs, vals in ((0, vt_s, p_s),):
            if blocks[t] is None:
                both = dot_nn(lhs[:, 0:total], vals[slot, :, 0:PAIR]).T
                rows = jnp.where(head_mask(SPEC_PAD, 0), both[0:SPEC_PAD], both[SPEC_PAD:2 * SPEC_PAD]).astype(BF16)
                if kind == 0:
                    emit_attn(main, rows)
                    padded = jnp.concatenate([rows, jnp.zeros((PAIR - SPEC_PAD, PAIR), BF16)], axis=0)
                    at_s[:, main:main + PAIR] = padded.T
                else:
                    dqkv_s[main:total, 0:PAIR] = rows
                continue
            both = jnp.concatenate(
                [dot_nn(lhs[h * HEAD_DIM:(h + 1) * HEAD_DIM, 0:total], vals[slot, :, h * QBLK:(h + 1) * QBLK])
                 for h in range(2)], axis=0)
            if kind == 0:
                at_s[:, blocks[t]:blocks[t] + QBLK] = both.astype(BF16)
            if kind == 1 or blocks[t] < 2 * patch:
                for c in range(0, QBLK, PAIR):
                    rows = both[:, c:c + PAIR].T.astype(BF16)
                    if kind == 0:
                        emit_attn(blocks[t] + c, rows)
                    else:
                        dqkv_s[blocks[t] + c:blocks[t] + c + PAIR, 0:PAIR] = rows
        for acc, vals, rows_ref, col in ((dk_s, ds_s, q_s, PAIR),):
            part = dot_nn(vals[slot, :, 0:span], jnp.concatenate(operands(t, rows_ref), axis=0))
            if t == 0:
                acc[...] = part
            elif t < len(blocks) - 1:
                acc[...] += part
            else:
                dqkv_s[:, col:col + PAIR] = (acc[...] + part).astype(BF16)
        for kind, lhs, vals in ((1, kt_s, ds_s),):
            if blocks[t] is None:
                both = dot_nn(lhs[:, 0:total], vals[slot, :, 0:PAIR]).T
                rows = jnp.where(head_mask(SPEC_PAD, 0), both[0:SPEC_PAD], both[SPEC_PAD:2 * SPEC_PAD]).astype(BF16)
                if kind == 0:
                    emit_attn(main, rows)
                    padded = jnp.concatenate([rows, jnp.zeros((PAIR - SPEC_PAD, PAIR), BF16)], axis=0)
                    at_s[:, main:main + PAIR] = padded.T
                else:
                    dqkv_s[main:total, 0:PAIR] = rows
                continue
            both = jnp.concatenate(
                [dot_nn(lhs[h * HEAD_DIM:(h + 1) * HEAD_DIM, 0:total], vals[slot, :, h * QBLK:(h + 1) * QBLK])
                 for h in range(2)], axis=0)
            if kind == 0:
                at_s[:, blocks[t]:blocks[t] + QBLK] = both.astype(BF16)
            if kind == 1 or blocks[t] < 2 * patch:
                for c in range(0, QBLK, PAIR):
                    rows = both[:, c:c + PAIR].T.astype(BF16)
                    if kind == 0:
                        emit_attn(blocks[t] + c, rows)
                    else:
                        dqkv_s[blocks[t] + c:blocks[t] + c + PAIR, 0:PAIR] = rows

    steps = len(blocks)
    stage_scores(0)
    transpose_in()
    for t in range(steps + 1):
        if t + 1 < steps:
            stage_scores(t + 1)
        if t >= 1:
            stage_outputs(t - 1)
        if t < steps:
            stage_softmax(t)

    dqkv_own[0:patch, :] = dqkv_s[0:patch, :]
    dqkv_own[patch:patch + SPEC_PAD, :] = dqkv_s[main:total, :]
    dqkv_par[0:patch, :] = dqkv_s[patch:2 * patch, :]
    dqkv_par[patch:patch + SPEC_PAD, :] = dqkv_s[main:total, :]
    d_b = jnp.sum(dqkv_s[...].astype(F32).reshape(total // 8, 8, 3 * PAIR), axis=0)
    acc_out[3][...] = d_b if first else acc_in[3][...] + d_b
    d_w = dot_nn(normt_s[:, 0:total], dqkv_s[...])
    acc_out[0][...] = (d_w if first else acc_in[0][...].reshape(d_w.shape) + d_w).reshape(acc_out[0].shape)
    at_all[pair] = at_s[...]

    @pl.when(pair == pl.num_programs(0) - 1)
    def _():
        lhs = at_all[...].reshape(half, at_all.shape[2])
        d_g = dot_nn(lhs[:, main:main + SPEC_PAD], dy_spc[...])
        for _, dy_ref, start, rows in pieces[:4]:
            d_g = d_g + dot_nn(lhs[:, start:start + rows], dy_ref[...])
        d_g = d_g if first else acc_in[1][...] + d_g
        acc_out[1][...] = d_g
        acc_out[2][...] = jnp.sum((wp_ref[...].astype(F32) * d_g).reshape(half // 8, 8, d_g.shape[1]), axis=0)


def fused_block(image, core, rows, accs, vectors, w_qkv, b_qkv, w_proj, n_spec):
    patch, d_model = rows[2].shape
    half = d_model // 2
    pairs = half // PAIR
    total = 4 * patch + SPEC_PAD
    first = accs is None
    once = pl.Buffered(buffer_count=1)

    def stacked(count):
        return pl.BlockSpec((None, count, d_model), lambda j, c: (image, 0, 0), pipeline_mode=once)

    def column(count, third):
        return pl.BlockSpec((count, half), lambda j, c: (0, 2 * third + c[0]), pipeline_mode=once)

    whole = pl.BlockSpec((patch, d_model), lambda j, c: (0, 0), pipeline_mode=once)
    vec = pl.BlockSpec((1, d_model), lambda j, c: (0, 0))
    acc_specs = [
        pl.BlockSpec((d_model, 3 * PAIR), lambda j, c: (0, j)),
        pl.BlockSpec((half, d_model), lambda j, c: (0, 0), pipeline_mode=once),
        pl.BlockSpec((8, d_model), lambda j, c: (0, 0)),
        pl.BlockSpec((8, 3 * PAIR), lambda j, c: (0, j)),
        pl.BlockSpec((8, d_model), lambda j, c: (0, 0)),
    ]
    acc_shapes = [
        jax.ShapeDtypeStruct((d_model, 3 * half), F32),
        jax.ShapeDtypeStruct((half, d_model), F32),
        jax.ShapeDtypeStruct((8, d_model), F32),
        jax.ShapeDtypeStruct((8, 3 * half), F32),
        jax.ShapeDtypeStruct((8, d_model), F32),
    ]
    row_spec = [stacked(patch), stacked(patch), whole, whole, stacked(SPEC_PAD)]
    in_specs = row_spec * 2 + [vec] * 3 + [column(d_model, t) for t in range(3)] + [column(1, t) for t in range(3)] + [
        pl.BlockSpec((half, d_model), lambda j, c: (c[0], 0), pipeline_mode=once),
    ] + ([] if first else acc_specs)
    flops = 2 * 6 * total * total * PAIR * pairs * 4
    outs = pl.pallas_call(
        functools.partial(block_kernel, n_spec, first),
        grid_spec=pltpu.PrefetchScalarGridSpec(
            num_scalar_prefetch=1, grid=(pairs,),
            in_specs=in_specs,
            out_specs=[
                pl.BlockSpec((patch + SPEC_PAD, PAIR), lambda j, c: (0, j)),
                pl.BlockSpec((patch + SPEC_PAD, PAIR), lambda j, c: (0, j)),
                pl.BlockSpec((patch + SPEC_PAD, 3 * PAIR), lambda j, c: (0, j)),
                pl.BlockSpec((patch + SPEC_PAD, 3 * PAIR), lambda j, c: (0, j)),
            ] + acc_specs,
            scratch_shapes=[pltpu.VMEM((total, d_model), BF16), pltpu.VMEM((d_model, total - SPEC_PAD + PAIR), BF16),
                            pltpu.VMEM((total, d_model), BF16)]
            + [pltpu.VMEM((total, PAIR), BF16)] * 4
            + [pltpu.VMEM((PAIR, total - SPEC_PAD + PAIR), BF16)] * 2
            + [pltpu.VMEM((2, total, 2 * QBLK), F32)]
            + [pltpu.VMEM((2, total, 2 * QBLK), BF16)] * 3
            + [pltpu.VMEM((total, PAIR), F32)] * 2
            + [pltpu.VMEM((PAIR, total - SPEC_PAD + PAIR), BF16), pltpu.VMEM((total, 3 * PAIR), BF16)]
            + [pltpu.VMEM((total, 3 * half), BF16), pltpu.VMEM((total, half), BF16),
               pltpu.VMEM((pairs, PAIR, total - SPEC_PAD + PAIR), BF16)]),
        out_shape=[jax.ShapeDtypeStruct((patch + SPEC_PAD, half), BF16)] * 2
        + [jax.ShapeDtypeStruct((patch + SPEC_PAD, 3 * half), BF16)] * 2 + acc_shapes,
        input_output_aliases={} if first else {21 + i: 4 + i for i in range(5)},
        cost_estimate=pl.CostEstimate(flops=flops, bytes_accessed=8 * total * half * 2,
                                      transcendentals=2 * pairs * total * total),
        compiler_params=pltpu.CompilerParams(vmem_limit_bytes=38 * 1024 * 1024),
        name="fused_block",
    )(core, *rows, *vectors, w_qkv, w_qkv, w_qkv, b_qkv, b_qkv, b_qkv, w_proj, *([] if first else accs))
    return outs[:4], outs[4:]


def place_columns(dst, src, pairs, half):
    for third in range(3):
        for pair in range(pairs):
            col = ((2 * third + half) * pairs + pair) * PAIR
            at = (pair * 3 + third) * PAIR
            dst[..., col:col + PAIR] = src[..., at:at + PAIR]


def finish_kernel(images, core_ref, *refs):
    per_image, refs = refs[:4 * images], refs[4 * images:]
    (x_ref, xs_ref, dy_ref, dys_ref, w_ref, wp_ref, ln_s, l_scale, b_proj,
     out_ref, outs_ref, dx_ref, dxs_ref, sums_ref, at_s, dq_s, spec_s) = refs
    image = pl.program_id(0)
    half_cols = per_image[0].shape[1]
    pairs = half_cols // PAIR
    patch = x_ref.shape[0]
    for k in range(images):
        attn_own, attn_got, dqkv_own, dqkv_got = per_image[4 * k:4 * k + 4]
        for half in range(2):
            @pl.when(jnp.logical_and(image == k, core_ref[0] == half))
            def _():
                at_s[:, half * half_cols:(half + 1) * half_cols] = attn_own[...]
                at_s[:, (1 - half) * half_cols:(2 - half) * half_cols] = attn_got[...]
                place_columns(dq_s, dqkv_own, pairs, half)
                place_columns(dq_s, dqkv_got, pairs, 1 - half)

    @pl.when(image == 0)
    def _():
        sums_ref[...] = jnp.zeros_like(sums_ref)

    proj = dot_nn(at_s[...], wp_ref[...]) + b_proj[...]
    d_norm = dot_nt(dq_s[...], w_ref[...]).astype(BF16).astype(F32)
    n_out = outs_ref.shape[0]
    for slot, x_in, dy_in, start, rows in ((0, x_ref, dy_ref, 0, patch), (1, xs_ref, dys_ref, patch, SPEC_PAD)):
        x_float = x_in[...].astype(F32)
        out = x_float + l_scale[...] * proj[start:start + rows]
        centered = x_float - jnp.mean(x_float, axis=-1, keepdims=True)
        inv_std = lax.rsqrt(jnp.mean(centered * centered, axis=-1, keepdims=True) + LN_EPS)
        x_hat = centered * inv_std
        grad = d_norm[start:start + rows]
        grad_hat = grad * ln_s[...]
        d_rows = inv_std * (grad_hat - jnp.mean(grad_hat, axis=-1, keepdims=True)
                            - x_hat * jnp.mean(grad_hat * x_hat, axis=-1, keepdims=True))
        dx = dy_in[...].astype(F32) + d_rows
        if slot == 0:
            out_ref[...] = out.astype(BF16)
            dx_ref[...] = dx.astype(BF16)
        else:
            for k in range(images):
                @pl.when(image == k)
                def _():
                    for row in range(n_out):
                        spec_s[0, row, k:k + 1, :] = out[row:row + 1]
                        spec_s[1, row, k:k + 1, :] = dx[row:row + 1]

            @pl.when(image == images - 1)
            def _():
                outs_ref[...] = spec_s[0, :, 0:images, :].astype(BF16)
                dxs_ref[...] = spec_s[1, :, 0:images, :].astype(BF16)
        width = grad.shape[1]
        sums_ref[2 * slot] += jnp.sum((grad * x_hat).reshape(rows // 8, 8, width), axis=0)
        sums_ref[2 * slot + 1] += jnp.sum(grad.reshape(rows // 8, 8, width), axis=0)


def finish(core, per_image, x_patch, x_spec, dy_patch, dy_spec, w_qkv, w_proj, ln_scale, layer_scale, b_proj, n_spec):
    images, patch, d_model = x_patch.shape
    rows = patch + SPEC_PAD

    def const(shape):
        return pl.BlockSpec(shape, lambda i, c: (0,) * len(shape))

    def by_image(count):
        return pl.BlockSpec((None, count, d_model), lambda i, c: (i, 0, 0))

    flat = [arr for group in per_image for arr in group]
    return pl.pallas_call(
        functools.partial(finish_kernel, images),
        grid_spec=pltpu.PrefetchScalarGridSpec(
            num_scalar_prefetch=1, grid=(images,),
            in_specs=[const(arr.shape) for arr in flat]
            + [by_image(patch), by_image(SPEC_PAD), by_image(patch), by_image(SPEC_PAD),
               const(w_qkv.shape), const(w_proj.shape), const((1, d_model)), const((1, d_model)), const((1, d_model))],
            out_specs=[by_image(patch), const((n_spec, images, d_model)), by_image(patch), const((n_spec, images, d_model)),
                       const((4, 8, d_model))],
            scratch_shapes=[pltpu.VMEM((rows, d_model), BF16), pltpu.VMEM((rows, 3 * d_model), BF16),
                            pltpu.VMEM((2, n_spec, 8, d_model), F32)]),
        out_shape=[jax.ShapeDtypeStruct((images, patch, d_model), BF16), jax.ShapeDtypeStruct((n_spec, images, d_model), BF16),
                   jax.ShapeDtypeStruct((images, patch, d_model), BF16), jax.ShapeDtypeStruct((n_spec, images, d_model), BF16),
                   jax.ShapeDtypeStruct((4, 8, d_model), F32)],
        cost_estimate=pl.CostEstimate(flops=8 * images * rows * d_model * d_model, bytes_accessed=20 << 20, transcendentals=0),
        compiler_params=pltpu.CompilerParams(vmem_limit_bytes=34 * 1024 * 1024),
        name="finish",
    )(core, *flat, x_patch, x_spec, dy_patch, dy_spec, w_qkv, w_proj, ln_scale, layer_scale, b_proj)


def merge_kernel(core_ref, w_own, w_got, g_own, g_got, db_own, db_got, ds_own, ds_got, d_dy, l_scale, b_proj,
                 w_out, g_out, db_out, dbp_out, dls_out):
    pairs = w_own.shape[1] // (3 * PAIR)
    step = pl.program_id(0)
    count = pl.num_programs(0) // 2
    for half in range(2):
        @pl.when(core_ref[0] == half)
        def _():
            place_columns(w_out, w_own, pairs, half)
            place_columns(w_out, w_got, pairs, 1 - half)

    @pl.when(step // count == core_ref[0])
    def _():
        g_out[...] = g_own[...] * l_scale[...]

    @pl.when(step // count != core_ref[0])
    def _():
        g_out[...] = g_got[...] * l_scale[...]

    @pl.when(step == 0)
    def _():
        total_dy = jnp.sum(d_dy[...], axis=0)
        dbp_out[...] = total_dy * l_scale[0]
        dls_out[...] = jnp.sum(ds_own[...] + ds_got[...], axis=0) + b_proj[0] * total_dy
        own = jnp.sum(db_own[...], axis=0)
        got = jnp.sum(db_got[...], axis=0)
        for half in range(2):
            @pl.when(core_ref[0] == half)
            def _():
                place_columns(db_out, own, pairs, half)
                place_columns(db_out, got, pairs, 1 - half)


def merge_grads(core, w_own, w_got, g_own, g_got, db_own, db_got, ds_own, ds_got, d_dy, layer_scale, b_proj):
    rows, cols = w_own.shape
    half, d_model = g_own.shape
    tile = PAIR
    count = half // tile

    def const(shape):
        return pl.BlockSpec(shape, lambda g, c: (0,) * len(shape))

    def half_rows(other):
        def index(g, c):
            wanted = g // count == (c[0] if other == 0 else 1 - c[0])
            return (jnp.where(wanted, g % count, jnp.where(g < count, 0, count - 1)), 0)

        return index

    small = (db_own, db_got, ds_own, ds_got, d_dy, layer_scale, b_proj)
    return pl.pallas_call(
        merge_kernel,
        grid_spec=pltpu.PrefetchScalarGridSpec(
            num_scalar_prefetch=1, grid=(2 * count,),
            in_specs=[pl.BlockSpec((tile, cols), lambda g, c: (g, 0))] * 2
            + [pl.BlockSpec((tile, d_model), half_rows(0)), pl.BlockSpec((tile, d_model), half_rows(1))]
            + [const(arr.shape) for arr in small],
            out_specs=[pl.BlockSpec((tile, 2 * cols), lambda g, c: (g, 0)),
                       pl.BlockSpec((tile, d_model), lambda g, c: (g, 0)),
                       const((2 * cols,)), const((d_model,)), const((d_model,))]),
        out_shape=[jax.ShapeDtypeStruct((rows, 2 * cols), F32), jax.ShapeDtypeStruct((2 * half, d_model), F32),
                   jax.ShapeDtypeStruct((2 * cols,), F32), jax.ShapeDtypeStruct((d_model,), F32),
                   jax.ShapeDtypeStruct((d_model,), F32)],
        cost_estimate=pl.CostEstimate(flops=rows * cols * 256, bytes_accessed=20 << 20, transcendentals=0),
        name="merge_grads",
    )(core, w_own, w_got, g_own, g_got, *small)


def solution(mesh):
    group_size = mesh.shape['sp']
    partner = [(i, i ^ 1) for i in range(group_size)]
    opposite = [(i, i ^ 2) for i in range(group_size)]

    diagonal = [(i, i ^ 3) for i in range(group_size)]

    def swap(vals):
        return lax.ppermute(vals, 'sp', partner)

    def cross(vals):
        return lax.ppermute(vals, 'sp', opposite)

    def run_block(x_special, x_patch, dy_special, dy_patch, ln_scale, ln_bias, w_qkv, b_qkv, w_proj, b_proj, layer_scale):
        num_images, n_spec, _ = x_special.shape
        core = (lax.axis_index('sp') % 2).reshape(1).astype(jnp.int32)

        x_first, dy_first = x_patch[0], dy_patch[0]
        x_later, dy_later = lax.optimization_barrier((x_patch, dy_patch, x_first, dy_first))[:2]
        across = [(cross(x_first), cross(dy_first))]
        across += [(cross(x_later[i]), cross(dy_later[i])) for i in range(1, num_images)]
        x_partner, dy_partner = swap(x_patch), swap(dy_patch)

        pad = ((0, 0), (0, SPEC_PAD - n_spec), (0, 0))
        x_spec = jnp.pad(x_special, pad)
        dy_spec = jnp.pad(dy_special, pad)
        ln_scale, ln_bias, layer_scale, b_proj, b_qkv = (
            v.reshape(1, -1) for v in (ln_scale, ln_bias, layer_scale, b_proj, b_qkv))

        per_image = []
        relays = {}
        accs = None

        def gate(vals, image):
            if image < 0:
                return vals
            return lax.optimization_barrier((vals, per_image[image][0]))[0]

        def relay_image(image, after):
            across[image] = gate(across[image], after)
            relays[image] = (swap(across[image][0]), swap(across[image][1]))

        relay_image(0, -1)
        for i in range(num_images):
            near, relay = gate((across[i], relays[i]), i - 1)
            rows = (x_patch, x_partner, near[0], relay[0], x_spec, dy_patch, dy_partner, near[1], relay[1], dy_spec)
            (attn_own, attn_par, dqkv_own, dqkv_par), accs = fused_block(
                i, core, rows, accs, (ln_scale, ln_bias, layer_scale), w_qkv, b_qkv, w_proj, n_spec)
            per_image.append((attn_own, swap(attn_par), dqkv_own, swap(dqkv_par)))
            for image in range(i + 1, num_images):
                if image not in relays and (image <= i + 2):
                    relay_image(image, i)

        d_w, d_g, d_scale, d_b, d_dy = accs
        got = [swap(vals) for vals in (d_w, d_g, d_b, d_scale)]
        out_patch, out_special, dx_patch, dx_special, sums = finish(
            core, per_image, x_patch, x_spec, dy_patch, dy_spec, w_qkv, w_proj, ln_scale, layer_scale, b_proj, n_spec)
        sums = jnp.sum(sums, axis=1)
        near, far, diag = swap(sums[:2]), cross(sums[:2]), lax.ppermute(sums[:2], 'sp', diagonal)
        ln_grads = (sums[:2] + near) + (far + diag) + sums[2:]
        d_w_qkv, d_w_proj, d_b_qkv, d_b_proj, d_layer_scale = merge_grads(
            core, d_w, got[0], d_g, got[1], d_b, got[2], d_scale, got[3], d_dy, layer_scale, b_proj)
        return (out_special.transpose(1, 0, 2), out_patch, dx_special.transpose(1, 0, 2), dx_patch, ln_grads[0], ln_grads[1],
                d_w_qkv, d_b_qkv, d_w_proj, d_b_proj, d_layer_scale)

    part_rows = P('dp')
    part_seq = P('dp', 'sp')
    replicated = P()
    return jax.shard_map(
        run_block, mesh=mesh,
        in_specs=(part_rows, part_seq, part_rows, part_seq, replicated, replicated, replicated, replicated, replicated, replicated, replicated),
        out_specs=(part_rows, part_seq, part_rows, part_seq, part_rows, part_rows, part_rows, part_rows, part_rows, part_rows, part_rows),
        check_vma=False)
```
